32 devices in a mesh: data: 32 (over z, y, x, core).
Axes of the slice: x: 2, y: 2, z: 4, core: 2. Of those that a mesh axis runs over, the one named last changes fastest.
Arguments:
- view_one: bfloat16 [2048, 256], P('data')
- view_two: bfloat16 [2048, 256], P('data')
- protos: bfloat16 [8192, 256], replicated
- valid_mask: int32 [2048], P('data')
Outputs:
- output 1: float32 [2048, 8192], P('data')
- output 2: float32 [2048, 8192], P('data')
- output 3: float32 [], replicated
- output 4: float32 [2048, 256], P('data')
- output 5: float32 [2048, 256], P('data')
- output 6: float32 [8192, 256], replicated
All inputs are finite; a program needn't handle non-finite values.
Results may differ from the reference program's by a relative error of at most 0.001.
Values are sent between devices in bfloat16 or wider.
A program may use at most 1 GiB of HBM per device.

```python
import jax
import jax.numpy as jnp

ROWS_DEV = 64
GROUPS = 32
PROTOS = 8192
EMBED_DIM = 256
SINK_ITERS = 3
SINK_EPS = 0.05
SOFT_TEMP = 0.1


def unit_rows(matrix):
    return matrix / jnp.sqrt(jnp.sum(matrix * matrix, axis=1, keepdims=True))


def draw_mask(draw_key):
    count_key, order_key = jax.random.split(draw_key)
    counts = jax.random.randint(count_key, (GROUPS,), 1, ROWS_DEV + 1)
    counts = counts.at[0].set(ROWS_DEV).at[1].set(1)
    order_scores = jax.random.randint(order_key, (GROUPS, ROWS_DEV), 0, 1 << 20) * ROWS_DEV + jnp.arange(ROWS_DEV, dtype=jnp.int32)[None, :]
    row_ranks = jnp.argsort(jnp.argsort(order_scores, axis=1), axis=1)
    return (row_ranks < counts[:, None]).astype(jnp.int32).reshape(-1)


def draw_picks(draw_key):
    band_width = max(2 * PROTOS // GROUPS, 1)
    starts = jnp.arange(GROUPS, dtype=jnp.int32)[:, None] * (PROTOS // GROUPS)
    offsets = jax.random.randint(draw_key, (GROUPS, ROWS_DEV), 0, band_width)
    return ((starts + offsets) % PROTOS).reshape(-1)


def draw_view(draw_key, protos, pick_ids):
    noise_rows = jax.random.normal(draw_key, (GROUPS * ROWS_DEV, EMBED_DIM), jnp.float32) * EMBED_DIM ** -0.5
    return unit_rows(0.6 * protos[pick_ids] + 0.8 * noise_rows)


def setup_inputs(seed: int = 0) -> dict:
    root_key = jax.random.key(seed)
    proto_key, pick_key, one_key, two_key, mask_key = jax.random.split(root_key, 5)
    protos = unit_rows(jax.random.normal(proto_key, (PROTOS, EMBED_DIM), jnp.float32))
    pick_ids = draw_picks(pick_key)
    return {
        "view_one": draw_view(one_key, protos, pick_ids).astype(jnp.bfloat16),
        "view_two": draw_view(two_key, protos, pick_ids).astype(jnp.bfloat16),
        "protos": protos.astype(jnp.bfloat16),
        "valid_mask": draw_mask(mask_key),
    }


def sinkhorn_codes(scores, weights, valid_count):
    transport = jnp.exp(scores / SINK_EPS) * weights
    for sweep_idx in range(SINK_ITERS):
        col_sum = jnp.sum(transport, axis=0, keepdims=True)
        transport = transport / (PROTOS * col_sum)
        row_sum = jnp.sum(transport, axis=1, keepdims=True) + (1.0 - weights)
        transport = transport / (valid_count * row_sum)
    return transport * valid_count


def reference(view_one, view_two, protos, valid_mask):
    weights = valid_mask.astype(jnp.float32)[:, None]
    valid_count = jnp.sum(weights)
    score_one = jnp.dot(view_one, protos.T, preferred_element_type=jnp.float32)
    score_two = jnp.dot(view_two, protos.T, preferred_element_type=jnp.float32)
    codes_one = sinkhorn_codes(score_one, weights, valid_count)
    codes_two = sinkhorn_codes(score_two, weights, valid_count)
    logp_one = jax.nn.log_softmax(score_one / SOFT_TEMP, axis=1)
    logp_two = jax.nn.log_softmax(score_two / SOFT_TEMP, axis=1)
    loss_value = -(jnp.sum(codes_two * logp_one) + jnp.sum(codes_one * logp_two)) / (2.0 * valid_count)
    grad_scale = weights / (2.0 * valid_count * SOFT_TEMP)
    grad_one = ((jnp.exp(logp_one) - codes_two) * grad_scale).astype(jnp.bfloat16)
    grad_two = ((jnp.exp(logp_two) - codes_one) * grad_scale).astype(jnp.bfloat16)
    dz_one = jnp.dot(grad_one, protos, preferred_element_type=jnp.float32)
    dz_two = jnp.dot(grad_two, protos, preferred_element_type=jnp.float32)
    d_protos = (jnp.dot(grad_one.T, view_one, preferred_element_type=jnp.float32)
                + jnp.dot(grad_two.T, view_two, preferred_element_type=jnp.float32))
    return codes_one, codes_two, loss_value, dz_one, dz_two, d_protos
```

```python
import jax
import jax.numpy as jnp
from jax import lax
from jax.experimental import pallas as pl
from jax.experimental.pallas import tpu as pltpu
from jax.sharding import PartitionSpec as P

MESH = pl.DeviceIdType.MESH
F32 = jnp.float32
BF16 = jnp.bfloat16

ROWS = 64
DEVS = 32
PLANE = 8
SAMPLES = ROWS * DEVS
PROTOS = 8192
DIM = 256
COLS = PROTOS // PLANE
ITERS = 3
INV_T = 10.0
SLAB = 2 * ROWS + 16
UNIT = 64
UNITS = COLS // UNIT
DIRECT = 11
NT = (((1,), (1,)), ((), ()))


def kernel(v1_hbm, v2_hbm, mk_hbm, c_hbm,
           q1_ref, q2_ref, loss_ref, dz1_ref, dz2_ref, dc_ref,
           zc, call, e_ref, vbc, mden, uden, ub, rbuf, vall, lbuf, lzbuf, colv,
           lsem, z_send, z_recv, ar_send, ar_recv, v_send, v_recv,
           l_send, l_recv, lz_send, lz_recv,
           d_recv, dcore_recv, d_sf, d_ss, d_sc, d_fs, d_sz):
    me = lax.axis_index("data")
    z = me // PLANE
    j = me % PLANE
    c = j % 2
    x = (j // 2) % 2
    y = j // 4
    jx = j + 2 - 4 * x
    jy = j + 4 - 8 * y
    jd = (6 - 2 * (j // 2)) + c
    jf = jx + c * (jy - jx)
    js = jy + c * (jx - jy)
    core = me + 1 - 2 * c
    first = z * PLANE + jf
    second = z * PLANE + js
    par = z % 2
    zpart = me + PLANE - 2 * PLANE * par

    barrier = pltpu.get_barrier_semaphore()
    for t in range(1, PLANE):
        pl.semaphore_signal(barrier, inc=1, device_id=(z * PLANE + (j + t) % PLANE,), device_id_type=MESH)
    for t in range(1, 4):
        pl.semaphore_signal(barrier, inc=1, device_id=(((z + t) % 4) * PLANE + j,), device_id_type=MESH)

    own = [
        pltpu.make_async_copy(v1_hbm, zc.at[me, pl.ds(0, ROWS), :], lsem.at[0]),
        pltpu.make_async_copy(v2_hbm, zc.at[me, pl.ds(ROWS, ROWS), :], lsem.at[1]),
        pltpu.make_async_copy(mk_hbm, zc.at[me, pl.ds(2 * ROWS, 16), :], lsem.at[2]),
    ]
    for cp in own:
        cp.start()
    c_copy = pltpu.make_async_copy(c_hbm, call, lsem.at[3])
    c_copy.start()
    for cp in own:
        cp.wait()
    pl.semaphore_wait(barrier, PLANE - 1 + 3)

    def remote(src, dst, ssem, rsem, dev):
        return pltpu.make_async_remote_copy(src_ref=src, dst_ref=dst, send_sem=ssem, recv_sem=rsem,
                                            device_id=(dev,), device_id_type=MESH)

    pending = []

    def z_copy(i, dev):
        cp = remote(zc.at[i], zc.at[i], z_send.at[len(pending)], z_recv.at[i], dev)
        pending.append(cp)
        cp.start()

    def z_wait(i):
        remote(zc.at[i], zc.at[i], z_send.at[0], z_recv.at[i], me).wait_recv()

    def rel(t):
        return ((z + t) % 4) * PLANE

    z_copy(me, first)
    z_copy(me, second)
    for t in range(1, 4):
        z_copy(me, rel(t) + j)
    z_copy(me, core)

    def take_f(t):
        z_wait(rel(t) + jf)
        z_copy(rel(t) + jf, second)
        z_copy(rel(t) + jf, core)

    def take_s(t):
        z_wait(rel(t) + js)
        z_copy(rel(t) + js, core)
        z_wait(rel(t) + jd)
        z_copy(rel(t) + jd, core)

    def take_core(t):
        for q in range(4):
            z_wait(rel(t) + 2 * q + 1 - c)

    take_f(0)
    for t in range(1, 4):
        z_wait(rel(t) + j)
        z_copy(rel(t) + j, first)
        z_copy(rel(t) + j, second)
        z_copy(rel(t) + j, core)
    take_s(0)
    for t in range(1, 4):
        take_f(t)
    take_s(1)
    c_copy.wait()

    def scores(t):
        p = (z + t) % 4
        for v in range(2):
            zb = zc[pl.ds(p * PLANE, PLANE), v * ROWS:(v + 1) * ROWS, :].reshape(PLANE * ROWS, DIM)

            def body(kb, acc, v=v, zb=zb):
                cs = call[pl.ds(pl.multiple_of(j * COLS + kb * 128, 128), 128), :]
                s = lax.dot_general(cs, zb, NT, preferred_element_type=F32)
                e = jnp.exp(s * INV_T)
                e_ref[v, pl.ds(pl.multiple_of(kb * 128, 128), 128), pl.ds(pl.multiple_of(p * 512, 512), 512)] = e
                return acc + jnp.sum(e.reshape(16, 8, 512), axis=0)

            acc = lax.fori_loop(0, COLS // 128, body, jnp.zeros((8, 512), F32))
            tot = jnp.sum(acc, axis=0, keepdims=True)
            for b in range(4):
                rbuf[0, j, pl.ds(v * 16 + p * 4 + b, 1), :] = tot[:, b * 128:(b + 1) * 128]

    take_core(0)
    scores(0)
    take_s(2)
    take_core(1)
    scores(1)
    take_s(3)
    take_core(2)
    scores(2)
    take_core(3)
    scores(3)

    def ar_copies(ph):
        return [remote(rbuf.at[ph, j], rbuf.at[ph, j], ar_send.at[ph, t - 1], ar_recv.at[ph, j],
                       z * PLANE + (j + t) % PLANE) for t in range(1, PLANE)]

    def ar_wait(ph):
        for t in range(1, PLANE):
            o = (j + t) % PLANE
            remote(rbuf.at[ph, o], rbuf.at[ph, o], ar_send.at[ph, 0], ar_recv.at[ph, o], me).wait_recv()

    def ar_sum(ph):
        tot = rbuf[ph, 0]
        for o in range(1, PLANE):
            tot = tot + rbuf[ph, o]
        return tot

    for cp in ar_copies(0):
        cp.start()

    lane = lax.broadcasted_iota(jnp.int32, (1, 128), 1)
    for b in range(16):
        even = zc[2 * b, 2 * ROWS:2 * ROWS + 16, 0:128].astype(F32)[0:1]
        odd = zc[2 * b + 1, 2 * ROWS:2 * ROWS + 16, 0:128].astype(F32)[0:1]
        mrow = jnp.where(lane < ROWS, even, odd)
        mden[pl.ds(b, 1), :] = mrow
        mden[pl.ds(16 + b, 1), :] = mrow
    valid = jnp.sum(jnp.sum(mden[0:16, :], axis=0, keepdims=True), axis=1, keepdims=True)

    def spread(dense, slot):
        uden[...] = dense
        for v in range(2):
            for b in range(16):
                ub[slot, v, :, b * 128:(b + 1) * 128] = jnp.broadcast_to(uden[pl.ds(v * 16 + b, 1), :], (8, 128))

    spread(mden[...], 0)

    KB = 32

    def sweep(ph):
        for v in range(2):
            u = ub[0, v]

            def rows(kb):
                w = e_ref[v, pl.ds(pl.multiple_of(kb * KB, KB), KB), :]
                return (w * w).reshape(KB // 8, 8, SAMPLES)

            def body(kb, carry):
                acc, vprev = carry
                wu = rows(kb) * u[None]
                part = wu[:, :, 0:128]
                for b in range(1, 16):
                    part = part + wu[:, :, b * 128:(b + 1) * 128]
                col = jnp.sum(part.reshape(KB, 128), axis=1, keepdims=True)
                vnew = jnp.broadcast_to(1.0 / (PROTOS * col), (KB, 128))
                vbc[v, pl.ds(pl.multiple_of(kb * KB, KB), KB), :] = vnew
                old = rows(jnp.maximum(kb - 1, 0))
                vb = jnp.concatenate([vprev.reshape(KB // 8, 8, 128)] * 16, axis=2)
                acc = acc + jnp.sum(old * vb, axis=0)
                return acc, vnew

            acc, vlast = lax.fori_loop(0, COLS // KB, body, (jnp.zeros((8, SAMPLES), F32), jnp.zeros((KB, 128), F32)))
            vb = jnp.concatenate([vlast.reshape(KB // 8, 8, 128)] * 16, axis=2)
            acc = acc + jnp.sum(rows(COLS // KB - 1) * vb, axis=0)
            tot = jnp.sum(acc, axis=0, keepdims=True)
            for b in range(16):
                rbuf[ph, j, pl.ds(v * 16 + b, 1), :] = tot[:, b * 128:(b + 1) * 128]

    v_copies = []
    u3 = None
    for it in range(ITERS):
        ph = it + 1
        sweep(ph)
        for cp in ar_copies(ph):
            cp.start()
        if it == 0:
            ar_wait(0)
        if it == ITERS - 1:
            diag = (lax.broadcasted_iota(jnp.int32, (128, 128), 0) == lax.broadcasted_iota(jnp.int32, (128, 128), 1))
            for v in range(2):
                for b in range(COLS // 128):
                    blk = vbc[v, b * 128:(b + 1) * 128, :]
                    vall[j, pl.ds(v, 1), b * 128:(b + 1) * 128] = jnp.sum(jnp.where(diag, blk, 0.0), axis=0, keepdims=True)
            v_copies = [remote(vall.at[j], vall.at[j], v_send.at[t - 1], v_recv.at[j],
                               z * PLANE + (j + t) % PLANE) for t in range(1, PLANE)]
            for cp in v_copies:
                cp.start()
        ar_wait(ph)
        u3 = mden[...] / (valid * ar_sum(ph))
        if it < ITERS - 1:
            spread(u3, 0)

    gam = mden[...] / (valid * 0.2)
    soft = ar_sum(0)
    mu = valid * u3
    sub = lax.broadcasted_iota(jnp.int32, (ROWS, 128), 0)
    pick = lax.broadcasted_iota(jnp.int32, (ROWS, 128), 1) == sub + ROWS * (me % 2)

    def own_rows(dense, slot):
        uden[...] = dense
        for v in range(2):
            row = uden[pl.ds(v * 16 + me // 2, 1), :]
            val = jnp.sum(jnp.where(pick, jnp.broadcast_to(row, (ROWS, 128)), 0.0), axis=1, keepdims=True)
            colv[slot, v] = jnp.broadcast_to(val, (ROWS, 128))

    spread(mu * gam, 0)
    spread(gam / soft, 1)

    def unit_of(w):
        return w + par * (UNITS - 1 - 2 * w)

    def unit_ref(q, u):
        return dc_ref.at[pl.ds(pl.multiple_of(q * COLS + u * UNIT, UNIT), UNIT), :]

    def d_copy(q, u, ssem, rsem, dev):
        return remote(unit_ref(q, u), unit_ref(q, u), ssem, rsem, dev)

    def d_core(q, s, u):
        return d_copy(q, u, d_sc.at[s, u], dcore_recv.at[q // 2, u], core)

    def d_wait(q, s, u):
        d_copy(q, u, d_sf.at[0], d_recv.at[s, u], me).wait_recv()

    def own_block(b):
        blk = b + par * (COLS // 128 - 1 - 2 * b)
        k0 = pl.multiple_of(blk * 128, 128)

        def body(i, acc):
            n0 = pl.multiple_of(i * 256, 256)
            e1 = e_ref[0, pl.ds(k0, 128), pl.ds(n0, 256)].reshape(16, 8, 256)
            e2 = e_ref[1, pl.ds(k0, 128), pl.ds(n0, 256)].reshape(16, 8, 256)
            va = jnp.concatenate([vbc[0, pl.ds(k0, 128), :]] * 2, axis=1).reshape(16, 8, 256)
            vb = jnp.concatenate([vbc[1, pl.ds(k0, 128), :]] * 2, axis=1).reshape(16, 8, 256)
            g1 = e1 * ub[1, 0, :, pl.ds(n0, 256)][None] - (e2 * e2 * vb) * ub[0, 1, :, pl.ds(n0, 256)][None]
            g2 = e2 * ub[1, 1, :, pl.ds(n0, 256)][None] - (e1 * e1 * va) * ub[0, 0, :, pl.ds(n0, 256)][None]
            z1 = zc[pl.ds(i * 4, 4), 0:ROWS, :].reshape(256, DIM)
            z2 = zc[pl.ds(i * 4, 4), ROWS:2 * ROWS, :].reshape(256, DIM)
            acc = acc + jnp.dot(g1.reshape(128, 256).astype(BF16), z1, preferred_element_type=F32)
            return acc + jnp.dot(g2.reshape(128, 256).astype(BF16), z2, preferred_element_type=F32)

        acc = lax.fori_loop(0, SAMPLES // 256, body, jnp.zeros((128, DIM), F32))
        dc_ref[pl.ds(pl.multiple_of(j * COLS + blk * 128, 128), 128), :] = acc

    def direct(w):
        u = unit_of(w)
        d_copy(j, u, d_sf.at[u], d_recv.at[0, u], first).start()
        d_copy(j, u, d_ss.at[u], d_recv.at[1, u], second).start()
        d_core(j, 0, u).start()

    def only_core(w):
        d_core(j, 0, unit_of(w)).start()

    @pl.loop(0, DIRECT // 2)
    def _(b):
        own_block(b)
        direct(2 * b)
        direct(2 * b + 1)

    own_block(DIRECT // 2)
    direct(DIRECT - 1)
    only_core(DIRECT)

    @pl.loop(DIRECT // 2 + 1, UNITS // 2)
    def _(b):
        own_block(b)
        only_core(2 * b)
        only_core(2 * b + 1)

    own_rows(mu, 0)
    own_rows(gam, 1)
    own_rows(soft, 2)
    for t in range(1, PLANE):
        o = (j + t) % PLANE
        remote(vall.at[o], vall.at[o], v_send.at[0], v_recv.at[o], me).wait_recv()

    mu1, mu2 = colv[0, 0][:, 0:1], colv[0, 1][:, 0:1]
    gm = colv[1, 0][:, 0:1]
    p1, p2 = colv[2, 0][:, 0:1], colv[2, 1][:, 0:1]
    ip1, ip2 = 1.0 / p1, 1.0 / p2
    lp1, lp2 = jnp.log(p1), jnp.log(p2)
    zown = zc[me, 0:2 * ROWS, :]

    def row_body(i, carry):
        dz, lacc = carry
        k0 = pl.multiple_of(i * 256, 256)
        l0 = pl.multiple_of((i % 4) * 256, 256)
        cb = call[pl.ds(k0, 256), :]
        s = lax.dot_general(zown, cb, NT, preferred_element_type=F32) * INV_T
        e = jnp.exp(s)
        e1, e2 = e[0:ROWS], e[ROWS:]
        q1 = (e1 * e1) * mu1 * vall[i // 4, 0:1, pl.ds(l0, 256)]
        q2 = (e2 * e2) * mu2 * vall[i // 4, 1:2, pl.ds(l0, 256)]
        q1_ref[:, pl.ds(k0, 256)] = q1
        q2_ref[:, pl.ds(k0, 256)] = q2
        lsum = q2 * (s[0:ROWS] - lp1) + q1 * (s[ROWS:] - lp2)
        lacc = lacc + jnp.sum(lsum.reshape(ROWS // 8, 8, 256), axis=0)
        g = jnp.concatenate([(e1 * ip1 - q2) * gm, (e2 * ip2 - q1) * gm], axis=0).astype(BF16)
        return dz + jnp.dot(g, cb, preferred_element_type=F32), lacc

    dz, lacc = lax.fori_loop(0, PROTOS // 256, row_body, (jnp.zeros((2 * ROWS, DIM), F32), jnp.zeros((8, 256), F32)))
    dz1_ref[...] = dz[0:ROWS]
    dz2_ref[...] = dz[ROWS:]
    lpart = jnp.sum(jnp.sum(lacc, axis=0, keepdims=True), axis=1, keepdims=True)
    lbuf[j] = jnp.broadcast_to(lpart, (8, 128))
    l_copies = [remote(lbuf.at[j], lbuf.at[j], l_send.at[t - 1], l_recv.at[j],
                       z * PLANE + (j + t) % PLANE) for t in range(1, PLANE)]
    for cp in l_copies:
        cp.start()

    LAG = 3

    def take_d(w, fwd):
        u = unit_of(w)
        d_wait(jd, 2, u)
        if fwd:
            d_copy(jd, u, d_sz.at[2, u], d_recv.at[2, u], zpart).start()
        d_core(jd, 3, u).start()

    for w in range(DIRECT + LAG):
        if w < DIRECT:
            u = unit_of(w)
            d_wait(jf, 0, u)
            d_copy(jf, u, d_fs.at[u], d_recv.at[2, u], second).start()
            if w < UNITS - DIRECT:
                d_copy(jf, u, d_sz.at[0, u], d_recv.at[0, u], zpart).start()
            d_core(jf, 1, u).start()
            d_wait(js, 1, u)
            if w < UNITS - DIRECT:
                d_copy(js, u, d_sz.at[1, u], d_recv.at[1, u], zpart).start()
            d_core(js, 2, u).start()
        if w >= LAG:
            take_d(w - LAG, w - LAG < UNITS - DIRECT)

    for t in range(1, PLANE):
        o = (j + t) % PLANE
        remote(lbuf.at[o], lbuf.at[o], l_send.at[0], l_recv.at[o], me).wait_recv()
    lsum = lbuf[0]
    for o in range(1, PLANE):
        lsum = lsum + lbuf[o]
    lzbuf[z] = lsum
    lz_copies = [remote(lzbuf.at[z], lzbuf.at[z], lz_send.at[t - 1], lz_recv.at[z],
                        ((z + t) % 4) * PLANE + j) for t in range(1, 4)]
    for cp in lz_copies:
        cp.start()

    for w in range(DIRECT, UNITS):
        u = unit_of(w)
        for s, q in ((0, jf), (1, js), (2, jd)):
            d_wait(q, s, u)
            d_core(q, s + 1, u).start()

    for t in range(1, 4):
        o = (z + t) % 4
        remote(lzbuf.at[o], lzbuf.at[o], lz_send.at[0], lz_recv.at[o], me).wait_recv()
    loss_ref[...] = -(((lzbuf[0] + lzbuf[1]) + lzbuf[2]) + lzbuf[3]) / (2.0 * valid)

    @pl.loop(0, UNITS)
    def _(u):
        for q in range(4):
            d_copy(2 * q + 1 - c, u, d_sf.at[0], dcore_recv.at[q, u], me).wait_recv()

    for cp in pending + v_copies + l_copies + lz_copies:
        cp.wait_send()
    for ph in range(ITERS + 1):
        for cp in ar_copies(ph):
            cp.wait_send()
    for w in range(UNITS):
        u = unit_of(w)
        for s in range(4):
            d_copy(j, u, d_sc.at[s, u], dcore_recv.at[0, u], core).wait_send()
        if w < DIRECT:
            d_copy(j, u, d_sf.at[u], d_recv.at[0, u], first).wait_send()
            d_copy(j, u, d_ss.at[u], d_recv.at[1, u], second).wait_send()
            d_copy(jf, u, d_fs.at[u], d_recv.at[2, u], second).wait_send()
        if w < UNITS - DIRECT:
            for s in range(3):
                d_copy(j, u, d_sz.at[s, u], d_recv.at[s, u], zpart).wait_send()


def solution(mesh):
    def local_step(view_one, view_two, protos, valid_mask):
        m = valid_mask.astype(BF16)
        mk = jnp.broadcast_to(jnp.tile(m, 4)[None], (16, DIM))
        dma = pltpu.SemaphoreType.DMA
        outs = pl.pallas_call(
            kernel,
            out_shape=[
                pltpu.VMEM((ROWS, PROTOS), F32),
                pltpu.VMEM((ROWS, PROTOS), F32),
                pltpu.VMEM((8, 128), F32),
                pltpu.VMEM((ROWS, DIM), F32),
                pltpu.VMEM((ROWS, DIM), F32),
                pltpu.VMEM((PROTOS, DIM), F32),
            ],
            in_specs=[pl.BlockSpec(memory_space=pl.ANY)] * 4,
            out_specs=[pl.BlockSpec(memory_space=pltpu.VMEM)] * 6,
            scratch_shapes=[
                pltpu.VMEM((DEVS, SLAB, DIM), BF16),
                pltpu.VMEM((PROTOS, DIM), BF16),
                pltpu.VMEM((2, COLS, SAMPLES), F32),
                pltpu.VMEM((2, COLS, 128), F32),
                pltpu.VMEM((32, 128), F32),
                pltpu.VMEM((32, 128), F32),
                pltpu.VMEM((2, 2, 8, SAMPLES), F32),
                pltpu.VMEM((ITERS + 1, PLANE, 32, 128), F32),
                pltpu.VMEM((PLANE, 2, COLS), F32),
                pltpu.VMEM((PLANE, 8, 128), F32),
                pltpu.VMEM((4, 8, 128), F32),
                pltpu.VMEM((3, 2, ROWS, 128), F32),
                dma((4,)), dma((31,)), dma((DEVS,)),
                dma((ITERS + 1, PLANE - 1)), dma((ITERS + 1, PLANE)),
                dma((PLANE - 1,)), dma((PLANE,)),
                dma((PLANE - 1,)), dma((PLANE,)), dma((3,)), dma((4,)),
                dma((3, UNITS)), dma((4, UNITS)), dma((UNITS,)), dma((UNITS,)), dma((4, UNITS)),
                dma((UNITS,)), dma((3, UNITS)),
            ],
            compiler_params=pltpu.CompilerParams(
                collective_id=0, has_side_effects=True, vmem_limit_bytes=44 << 20),
        )(view_one, view_two, mk, protos)
        q1, q2, loss, dz1, dz2, dc = outs
        return q1, q2, loss[0, 0], dz1, dz2, dc

    return jax.shard_map(
        local_step,
        mesh=mesh,
        in_specs=(P("data", None), P("data", None), P(None, None), P("data")),
        out_specs=(P("data", None), P("data", None), P(), P("data", None), P("data", None), P(None, None)),
        check_vma=False,
    )
```

```python
import jax
import jax.numpy as jnp
from jax import lax
from jax.experimental import pallas as pl
from jax.experimental.pallas import tpu as pltpu
from jax.sharding import PartitionSpec as P

MESH = pl.DeviceIdType.MESH
F32 = jnp.float32
BF16 = jnp.bfloat16

ROWS = 64
DEVS = 32
PLANE = 8
SAMPLES = ROWS * DEVS
MB = 256
PROTOS = 8192
DIM = 256
COLS = PROTOS // PLANE
ITERS = 3
INV_T = 10.0
SLAB = 2 * ROWS
UNIT = 64
UNITS = COLS // UNIT
DIRECT = 11
LOG2E = 1.4426950408889634
NT = (((1,), (1,)), ((), ()))


def kernel(v1_hbm, v2_hbm, mk_hbm, c_hbm,
           q1_ref, q2_ref, loss_ref, dz1_ref, dz2_ref, dc_ref,
           zc, mi, mbuf, call, e_ref, a_ref, vbc, mden, uden, ub, rbuf, vall, lbuf, lzbuf, colv,
           lsem, z_send, z_recv, m_send, m_recv, ar_send, ar_recv, v_send, v_recv,
           l_send, l_recv, lz_send, lz_recv,
           d_recv, dcore_recv, d_sf, d_ss, d_sc, d_fs, d_sz):
    me = lax.axis_index("data")
    z = me // PLANE
    j = me % PLANE
    c = j % 2
    x = (j // 2) % 2
    y = j // 4
    jx = j + 2 - 4 * x
    jy = j + 4 - 8 * y
    jd = (6 - 2 * (j // 2)) + c
    jf = jx + c * (jy - jx)
    js = jy + c * (jx - jy)
    core = me + 1 - 2 * c
    first = z * PLANE + jf
    second = z * PLANE + js
    par = z % 2
    zpart = me + PLANE - 2 * PLANE * par

    barrier = pltpu.get_barrier_semaphore()
    for t in range(1, PLANE):
        pl.semaphore_signal(barrier, inc=1, device_id=(z * PLANE + (j + t) % PLANE,), device_id_type=MESH)
    for t in range(1, 4):
        pl.semaphore_signal(barrier, inc=1, device_id=(((z + t) % 4) * PLANE + j,), device_id_type=MESH)

    own = [
        pltpu.make_async_copy(v1_hbm, zc.at[me, pl.ds(0, ROWS), :], lsem.at[0]),
        pltpu.make_async_copy(v2_hbm, zc.at[me, pl.ds(ROWS, ROWS), :], lsem.at[1]),
        pltpu.make_async_copy(mk_hbm, mi, lsem.at[2]),
    ]
    for cp in own:
        cp.start()
    c_copy = pltpu.make_async_copy(c_hbm, call, lsem.at[3])
    c_copy.start()
    for cp in own:
        cp.wait()
    mrow = mi[...].astype(F32)
    mbuf[me] = jnp.concatenate([mrow, mrow], axis=1)
    pl.semaphore_wait(barrier, PLANE - 1 + 3)

    def remote(src, dst, ssem, rsem, dev):
        return pltpu.make_async_remote_copy(src_ref=src, dst_ref=dst, send_sem=ssem, recv_sem=rsem,
                                            device_id=(dev,), device_id_type=MESH)

    pending = []

    def z_copy(i, dev):
        k = len(pending) // 2
        for cp in (remote(zc.at[i], zc.at[i], z_send.at[k], z_recv.at[i], dev),
                   remote(mbuf.at[i], mbuf.at[i], m_send.at[k], m_recv.at[i], dev)):
            pending.append(cp)
            cp.start()

    def z_wait(i):
        remote(zc.at[i], zc.at[i], z_send.at[0], z_recv.at[i], me).wait_recv()
        remote(mbuf.at[i], mbuf.at[i], m_send.at[0], m_recv.at[i], me).wait_recv()

    def rel(t):
        return ((z + t) % 4) * PLANE

    z_copy(me, first)
    z_copy(me, second)
    for t in range(1, 4):
        z_copy(me, rel(t) + j)
    z_copy(me, core)

    def take_f(t):
        z_wait(rel(t) + jf)
        z_copy(rel(t) + jf, second)
        z_copy(rel(t) + jf, core)

    def take_s(t):
        z_wait(rel(t) + js)
        z_copy(rel(t) + js, core)
        z_wait(rel(t) + jd)
        z_copy(rel(t) + jd, core)

    def take_core(t):
        for q in range(4):
            z_wait(rel(t) + 2 * q + 1 - c)

    def scores(t, v):
        p = (z + t) % 4

        def body(h, carry):
            zb = zc[pl.ds(p * PLANE + h * 4, 4), v * ROWS:(v + 1) * ROWS, :].reshape(4 * ROWS, DIM)
            n0 = pl.multiple_of(p * 512 + h * 256, 256)
            acc = jnp.zeros((8, 256), F32)
            for kb in range(COLS // MB):
                cs = call[pl.ds(pl.multiple_of(j * COLS + kb * MB, MB), MB), :]
                s = lax.dot_general(cs, zb, NT, preferred_element_type=F32)
                e = jnp.exp2(s * (INV_T * LOG2E))
                e_ref[v, kb * MB:(kb + 1) * MB, pl.ds(n0, 256)] = e
                a_ref[v, kb * MB:(kb + 1) * MB, pl.ds(n0, 256)] = e * e
                acc = acc + jnp.sum(e.reshape(MB // 8, 8, 256), axis=0)
            tot = jnp.sum(acc, axis=0, keepdims=True)
            for b in range(2):
                rbuf[0, j, pl.ds(v * 16 + p * 4 + h * 2 + b, 1), :] = tot[:, b * 128:(b + 1) * 128]
            return carry

        lax.fori_loop(0, 2, body, 0)

    take_f(0)
    take_s(0)
    for t in range(1, 4):
        z_wait(rel(t) + j)
        z_copy(rel(t) + j, first)
        z_copy(rel(t) + j, second)
        z_copy(rel(t) + j, core)
    c_copy.wait()
    take_core(0)
    scores(0, 0)
    take_f(1)
    scores(0, 1)
    take_f(2)
    take_f(3)
    take_s(1)
    take_core(1)
    scores(1, 0)
    take_s(2)
    scores(1, 1)
    take_s(3)
    take_core(2)
    scores(2, 0)
    scores(2, 1)
    take_core(3)
    scores(3, 0)
    scores(3, 1)

    def ar_copies(ph):
        return [remote(rbuf.at[ph, j], rbuf.at[ph, j], ar_send.at[ph, t - 1], ar_recv.at[ph, j],
                       z * PLANE + (j + t) % PLANE) for t in range(1, PLANE)]

    def ar_wait(ph):
        for t in range(1, PLANE):
            o = (j + t) % PLANE
            remote(rbuf.at[ph, o], rbuf.at[ph, o], ar_send.at[ph, 0], ar_recv.at[ph, o], me).wait_recv()

    def ar_sum(ph):
        tot = rbuf[ph, 0]
        for o in range(1, PLANE):
            tot = tot + rbuf[ph, o]
        return tot

    for cp in ar_copies(0):
        cp.start()

    lane = lax.broadcasted_iota(jnp.int32, (1, 128), 1)
    for b in range(16):
        mrow = jnp.where(lane < ROWS, mbuf[2 * b], mbuf[2 * b + 1])
        mden[pl.ds(b, 1), :] = mrow
        mden[pl.ds(16 + b, 1), :] = mrow
    valid = jnp.sum(jnp.sum(mden[0:16, :], axis=0, keepdims=True), axis=1, keepdims=True)

    def spread(dense, slot):
        uden[...] = dense
        for v in range(2):
            for b in range(16):
                ub[slot, v, :, b * 128:(b + 1) * 128] = jnp.broadcast_to(uden[pl.ds(v * 16 + b, 1), :], (8, 128))

    spread(mden[...], 0)

    GRP = 4
    LB = SAMPLES // 128

    def sweep(ph):
        for v in range(2):
            u = [ub[0, v, :, b * 128:(b + 1) * 128] for b in range(LB)]

            def tile(row, b):
                return a_ref[v, pl.ds(row, 8), b * 128:(b + 1) * 128]

            def add_rows(i, acc, vs):
                for g in range(GRP):
                    row = pl.multiple_of((i * GRP + g) * 8, 8)
                    for b in range(LB):
                        acc[b] = acc[b] + tile(row, b) * vs[g]
                return acc

            def body(i, carry):
                acc, vprev = list(carry[:LB]), list(carry[LB:])
                vnew = []
                for g in range(GRP):
                    row = pl.multiple_of((i * GRP + g) * 8, 8)
                    parts = [tile(row, b) * u[b] for b in range(2)]
                    for b in range(2, LB):
                        parts[b % 2] = parts[b % 2] + tile(row, b) * u[b]
                    col = jnp.sum(parts[0] + parts[1], axis=1, keepdims=True)
                    vg = jnp.broadcast_to(1.0 / (PROTOS * col), (8, 128))
                    vbc[v, pl.ds(row, 8), :] = vg
                    vnew.append(vg)
                acc = add_rows(jnp.maximum(i - 1, 0), acc, vprev)
                return tuple(acc) + tuple(vnew)

            zero = jnp.zeros((8, 128), F32)
            steps = COLS // (8 * GRP)
            out = lax.fori_loop(0, steps, body, (zero,) * (LB + GRP))
            acc = add_rows(steps - 1, list(out[:LB]), out[LB:])
            for b in range(LB):
                rbuf[ph, j, pl.ds(v * 16 + b, 1), :] = jnp.sum(acc[b], axis=0, keepdims=True)

    def row_scores(lo, hi):
        def body(i, carry):
            k0 = pl.multiple_of(i * 256, 256)
            rs = lax.dot_general(zc[me], call[pl.ds(k0, 256), :], NT, preferred_element_type=F32)
            q1_ref[:, pl.ds(k0, 256)] = rs[0:ROWS]
            q2_ref[:, pl.ds(k0, 256)] = rs[ROWS:]
            return carry

        lax.fori_loop(lo, hi, body, 0)

    v_copies = []
    u3 = None
    for it in range(ITERS):
        ph = it + 1
        sweep(ph)
        for cp in ar_copies(ph):
            cp.start()
        if it == 0:
            ar_wait(0)
        if it == ITERS - 1:
            diag = (lax.broadcasted_iota(jnp.int32, (128, 128), 0) == lax.broadcasted_iota(jnp.int32, (128, 128), 1))
            for v in range(2):
                for b in range(COLS // 128):
                    blk = vbc[v, b * 128:(b + 1) * 128, :]
                    vall[j, pl.ds(v, 1), b * 128:(b + 1) * 128] = jnp.sum(jnp.where(diag, blk, 0.0), axis=0, keepdims=True)
            v_copies = [remote(vall.at[j], vall.at[j], v_send.at[t - 1], v_recv.at[j],
                               z * PLANE + (j + t) % PLANE) for t in range(1, PLANE)]
            for cp in v_copies:
                cp.start()
        row_scores((0, 11, 22)[it], (11, 22, 32)[it])
        ar_wait(ph)
        u3 = mden[...] / (valid * ar_sum(ph))
        if it < ITERS - 1:
            spread(u3, 0)

    gam = mden[...] / (valid * 0.2)
    soft = ar_sum(0)
    mu = valid * u3
    sub = lax.broadcasted_iota(jnp.int32, (ROWS, 128), 0)
    pick = lax.broadcasted_iota(jnp.int32, (ROWS, 128), 1) == sub + ROWS * (me % 2)

    def own_rows(dense, slot):
        uden[...] = dense
        for v in range(2):
            row = uden[pl.ds(v * 16 + me // 2, 1), :]
            val = jnp.sum(jnp.where(pick, jnp.broadcast_to(row, (ROWS, 128)), 0.0), axis=1, keepdims=True)
            colv[slot, v] = jnp.broadcast_to(val, (ROWS, 128))

    spread(mu * gam, 0)
    spread(gam / soft, 1)

    def unit_of(w):
        return w + par * (UNITS - 1 - 2 * w)

    def unit_ref(q, u):
        return dc_ref.at[pl.ds(pl.multiple_of(q * COLS + u * UNIT, UNIT), UNIT), :]

    def d_copy(q, u, ssem, rsem, dev):
        return remote(unit_ref(q, u), unit_ref(q, u), ssem, rsem, dev)

    def d_core(q, s, u):
        return d_copy(q, u, d_sc.at[s, u], dcore_recv.at[q // 2, u], core)

    def d_wait(q, s, u):
        d_copy(q, u, d_sf.at[0], d_recv.at[s, u], me).wait_recv()

    def own_block(b):
        blk = b + par * (COLS // 128 - 1 - 2 * b)
        k0 = pl.multiple_of(blk * 128, 128)

        def body(i, acc):
            n0 = pl.multiple_of(i * 256, 256)
            e1 = e_ref[0, pl.ds(k0, 128), pl.ds(n0, 256)].reshape(16, 8, 256)
            e2 = e_ref[1, pl.ds(k0, 128), pl.ds(n0, 256)].reshape(16, 8, 256)
            va = jnp.concatenate([vbc[0, pl.ds(k0, 128), :]] * 2, axis=1).reshape(16, 8, 256)
            vb = jnp.concatenate([vbc[1, pl.ds(k0, 128), :]] * 2, axis=1).reshape(16, 8, 256)
            g1 = e1 * ub[1, 0, :, pl.ds(n0, 256)][None] - (e2 * e2 * vb) * ub[0, 1, :, pl.ds(n0, 256)][None]
            g2 = e2 * ub[1, 1, :, pl.ds(n0, 256)][None] - (e1 * e1 * va) * ub[0, 0, :, pl.ds(n0, 256)][None]
            z1 = zc[pl.ds(i * 4, 4), 0:ROWS, :].reshape(256, DIM)
            z2 = zc[pl.ds(i * 4, 4), ROWS:2 * ROWS, :].reshape(256, DIM)
            acc = acc + jnp.dot(g1.reshape(128, 256).astype(BF16), z1, preferred_element_type=F32)
            return acc + jnp.dot(g2.reshape(128, 256).astype(BF16), z2, preferred_element_type=F32)

        acc = lax.fori_loop(0, SAMPLES // 256, body, jnp.zeros((128, DIM), F32))
        dc_ref[pl.ds(pl.multiple_of(j * COLS + blk * 128, 128), 128), :] = acc

    def send_own(w):
        u = unit_of(w)
        if w < DIRECT:
            d_copy(j, u, d_sf.at[u], d_recv.at[0, u], first).start()
        d_core(j, 0, u).start()

    def send_second(w):
        u = unit_of(w)
        d_copy(j, u, d_ss.at[u], d_recv.at[1, u], second).start()

    def take_first(w):
        u = unit_of(w)
        d_wait(jf, 0, u)
        d_copy(jf, u, d_fs.at[u], d_recv.at[2, u], second).start()
        if w < UNITS - DIRECT:
            d_copy(jf, u, d_sz.at[0, u], d_recv.at[0, u], zpart).start()
        d_core(jf, 1, u).start()

    def take_second(w):
        u = unit_of(w)
        d_wait(js, 1, u)
        if w < UNITS - DIRECT:
            d_copy(js, u, d_sz.at[1, u], d_recv.at[1, u], zpart).start()
        d_core(js, 2, u).start()

    def take_diag(w):
        u = unit_of(w)
        d_wait(jd, 2, u)
        if w < UNITS - DIRECT:
            d_copy(jd, u, d_sz.at[2, u], d_recv.at[2, u], zpart).start()
        d_core(jd, 3, u).start()

    def step(w):
        take_first(w)
        if w + 3 < DIRECT:
            send_second(w + 3)
        take_second(w)
        if w >= 3:
            take_diag(w - 3)

    for b in range(UNITS // 2):
        own_block(b)
        send_own(2 * b)
        send_own(2 * b + 1)
        if b < 2:
            send_second(2 * b)
        if b == 0:
            send_second(1)
        if b >= 2:
            step(b - 2)

    own_rows(mu, 0)
    own_rows(gam, 1)
    own_rows(soft, 2)
    for t in range(1, PLANE):
        o = (j + t) % PLANE
        remote(vall.at[o], vall.at[o], v_send.at[0], v_recv.at[o], me).wait_recv()

    mu1, mu2 = colv[0, 0][:, 0:1], colv[0, 1][:, 0:1]
    gm = colv[1, 0][:, 0:1]
    p1, p2 = colv[2, 0][:, 0:1], colv[2, 1][:, 0:1]
    ip1, ip2 = 1.0 / p1, 1.0 / p2
    lp1, lp2 = jnp.log(p1), jnp.log(p2)

    def row_body(i, carry):
        dz, lacc = carry
        k0 = pl.multiple_of(i * 256, 256)
        l0 = pl.multiple_of((i % 4) * 256, 256)
        cb = call[pl.ds(k0, 256), :]
        s1 = q1_ref[:, pl.ds(k0, 256)] * INV_T
        s2 = q2_ref[:, pl.ds(k0, 256)] * INV_T
        e1 = jnp.exp2(s1 * LOG2E)
        e2 = jnp.exp2(s2 * LOG2E)
        q1 = (e1 * e1) * mu1 * vall[i // 4, 0:1, pl.ds(l0, 256)]
        q2 = (e2 * e2) * mu2 * vall[i // 4, 1:2, pl.ds(l0, 256)]
        q1_ref[:, pl.ds(k0, 256)] = q1
        q2_ref[:, pl.ds(k0, 256)] = q2
        lsum = q2 * (s1 - lp1) + q1 * (s2 - lp2)
        lacc = lacc + jnp.sum(lsum.reshape(ROWS // 8, 8, 256), axis=0)
        g = jnp.concatenate([(e1 * ip1 - q2) * gm, (e2 * ip2 - q1) * gm], axis=0).astype(BF16)
        return dz + jnp.dot(g, cb, preferred_element_type=F32), lacc

    carry = (jnp.zeros((2 * ROWS, DIM), F32), jnp.zeros((8, 256), F32))
    cuts = (0, 7, 14, 20, 26, 32)
    for i in range(5):
        carry = lax.fori_loop(cuts[i], cuts[i + 1], row_body, carry)
        step(UNITS // 2 - 2 + i)
    dz, lacc = carry
    dz1_ref[...] = dz[0:ROWS]
    dz2_ref[...] = dz[ROWS:]
    lpart = jnp.sum(jnp.sum(lacc, axis=0, keepdims=True), axis=1, keepdims=True)
    lbuf[j] = jnp.broadcast_to(lpart, (8, 128))
    l_copies = [remote(lbuf.at[j], lbuf.at[j], l_send.at[t - 1], l_recv.at[j],
                       z * PLANE + (j + t) % PLANE) for t in range(1, PLANE)]
    for cp in l_copies:
        cp.start()

    for w in range(DIRECT - 3, DIRECT):
        take_diag(w)

    for t in range(1, PLANE):
        o = (j + t) % PLANE
        remote(lbuf.at[o], lbuf.at[o], l_send.at[0], l_recv.at[o], me).wait_recv()
    lsum = lbuf[0]
    for o in range(1, PLANE):
        lsum = lsum + lbuf[o]
    lzbuf[z] = lsum
    lz_copies = [remote(lzbuf.at[z], lzbuf.at[z], lz_send.at[t - 1], lz_recv.at[z],
                        ((z + t) % 4) * PLANE + j) for t in range(1, 4)]
    for cp in lz_copies:
        cp.start()

    for w in reversed(range(DIRECT, UNITS)):
        u = unit_of(w)
        for s, q in ((0, jf), (1, js), (2, jd)):
            d_wait(q, s, u)
            d_core(q, s + 1, u).start()

    for t in range(1, 4):
        o = (z + t) % 4
        remote(lzbuf.at[o], lzbuf.at[o], lz_send.at[0], lz_recv.at[o], me).wait_recv()
    loss = -(((lzbuf[0] + lzbuf[1]) + lzbuf[2]) + lzbuf[3]) / (2.0 * valid)
    loss_ref[...] = loss[0:1, 0:1]

    @pl.loop(0, UNITS)
    def _(u):
        for q in range(4):
            d_copy(2 * q + 1 - c, u, d_sf.at[0], dcore_recv.at[q, u], me).wait_recv()

    for cp in pending + v_copies + l_copies + lz_copies:
        cp.wait_send()
    for ph in range(ITERS + 1):
        for cp in ar_copies(ph):
            cp.wait_send()
    for w in range(UNITS):
        u = unit_of(w)
        for s in range(4):
            d_copy(j, u, d_sc.at[s, u], dcore_recv.at[0, u], core).wait_send()
        if w < DIRECT:
            d_copy(j, u, d_sf.at[u], d_recv.at[0, u], first).wait_send()
            d_copy(j, u, d_ss.at[u], d_recv.at[1, u], second).wait_send()
            d_copy(jf, u, d_fs.at[u], d_recv.at[2, u], second).wait_send()
        if w < UNITS - DIRECT:
            for s in range(3):
                d_copy(j, u, d_sz.at[s, u], d_recv.at[s, u], zpart).wait_send()


def store_kernel(*refs):
    srcs, dsts, sem = refs[:6], refs[6:12], refs[12]
    copies = [pltpu.make_async_copy(s, d, sem.at[i]) for i, (s, d) in enumerate(zip(srcs, dsts))]
    for cp in copies:
        cp.start()
    for cp in copies:
        cp.wait()


def solution(mesh):
    def local_step(view_one, view_two, protos, valid_mask):
        dma = pltpu.SemaphoreType.DMA
        outs = pl.pallas_call(
            kernel,
            out_shape=[
                pltpu.VMEM((ROWS, PROTOS), F32),
                pltpu.VMEM((ROWS, PROTOS), F32),
                pltpu.VMEM((1, 1), F32),
                pltpu.VMEM((ROWS, DIM), F32),
                pltpu.VMEM((ROWS, DIM), F32),
                pltpu.VMEM((PROTOS, DIM), F32),
            ],
            in_specs=[pl.BlockSpec(memory_space=pl.ANY)] * 4,
            out_specs=[pl.BlockSpec(memory_space=pltpu.VMEM)] * 6,
            scratch_shapes=[
                pltpu.VMEM((DEVS, SLAB, DIM), BF16),
                pltpu.VMEM((1, ROWS), jnp.int32),
                pltpu.VMEM((DEVS, 1, 128), F32),
                pltpu.VMEM((PROTOS, DIM), BF16),
                pltpu.VMEM((2, COLS, SAMPLES), F32),
                pltpu.VMEM((2, COLS, SAMPLES), F32),
                pltpu.VMEM((2, COLS, 128), F32),
                pltpu.VMEM((32, 128), F32),
                pltpu.VMEM((32, 128), F32),
                pltpu.VMEM((2, 2, 8, SAMPLES), F32),
                pltpu.VMEM((ITERS + 1, PLANE, 32, 128), F32),
                pltpu.VMEM((PLANE, 2, COLS), F32),
                pltpu.VMEM((PLANE, 8, 128), F32),
                pltpu.VMEM((4, 8, 128), F32),
                pltpu.VMEM((3, 2, ROWS, 128), F32),
                dma((4,)), dma((31,)), dma((DEVS,)), dma((31,)), dma((DEVS,)),
                dma((ITERS + 1, PLANE - 1)), dma((ITERS + 1, PLANE)),
                dma((PLANE - 1,)), dma((PLANE,)),
                dma((PLANE - 1,)), dma((PLANE,)), dma((3,)), dma((4,)),
                dma((3, UNITS)), dma((4, UNITS)), dma((UNITS,)), dma((UNITS,)), dma((4, UNITS)),
                dma((UNITS,)), dma((3, UNITS)),
            ],
            compiler_params=pltpu.CompilerParams(
                collective_id=0, has_side_effects=True, vmem_limit_bytes=48 << 20),
        )(view_one, view_two, valid_mask.reshape(1, ROWS), protos)
        outs = pl.pallas_call(
            store_kernel,
            out_shape=[jax.ShapeDtypeStruct(o.shape, o.dtype) for o in outs],
            in_specs=[pl.BlockSpec(memory_space=pltpu.VMEM)] * 6,
            out_specs=[pl.BlockSpec(memory_space=pl.ANY)] * 6,
            scratch_shapes=[dma((6,))],
            compiler_params=pltpu.CompilerParams(vmem_limit_bytes=4 << 20),
        )(*[pltpu.with_memory_space_constraint(o, pltpu.VMEM) for o in outs])
        q1, q2, loss, dz1, dz2, dc = outs
        return q1, q2, loss.reshape(()), dz1, dz2, dc

    return jax.shard_map(
        local_step,
        mesh=mesh,
        in_specs=(P("data", None), P("data", None), P(None, None), P("data")),
        out_specs=(P("data", None), P("data", None), P(), P("data", None), P("data", None), P(None, None)),
        check_vma=False,
    )
```

```python
import jax
import jax.numpy as jnp
from jax import lax
from jax.experimental import pallas as pl
from jax.experimental.pallas import tpu as pltpu
from jax.sharding import PartitionSpec as P

MESH = pl.DeviceIdType.MESH
F32 = jnp.float32
BF16 = jnp.bfloat16

ROWS = 64
SLAB = 2 * ROWS
DEVS = 32
PLANE = 8
SAMPLES = ROWS * DEVS
MB = 256
PROTOS = 8192
DIM = 256
COLS = PROTOS // PLANE
ITERS = 3
LANES = 128
PLANES = DEVS // PLANE
PEERS = range(1, PLANE)
BLK = 2 * LANES
DENSE = SAMPLES // LANES
INV_T = 10.0
UNIT = 64
UNITS = COLS // UNIT
BLOCKS = COLS // LANES
DIRECT = 11
GRP = 32
LOG2E = 1.4426950408889634
ROW_CUTS = (5, 11, 17, 32)
NT = (((1,), (1,)), ((), ()))


def kernel(v1_hbm, v2_hbm, mk_hbm, c_hbm,
           q1_ref, q2_ref, loss_ref, dz1_ref, dz2_ref, dc_ref,
           zc, mi, mbuf, call, e_ref, a_ref, vbc, mden, uden, ub, rbuf, vall, lbuf, lzbuf,
           lsem, z_send, z_recv, m_send, m_recv, ar_send, ar_recv, v_send, v_recv,
           l_send, l_recv, lz_send, lz_recv,
           d_recv, dcore_recv, d_sf, d_ss, d_sc, d_fs, d_sz):
    me = lax.axis_index("data")
    z = me // PLANE
    j = me % PLANE
    c = j % 2
    x = (j // 2) % 2
    y = j // 4
    jx = j + 2 - 4 * x
    jy = j + 4 - 8 * y
    jd = (6 - 2 * (j // 2)) + c
    jf = jx + c * (jy - jx)
    js = jy + c * (jx - jy)
    core = me + 1 - 2 * c
    first = z * PLANE + jf
    second = z * PLANE + js
    par = z % 2
    planes = (z, z + 1 - 2 * par, z + 2 - PLANES * (z // 2), PLANES - 1 - z)
    zpart = planes[1] * PLANE + j
    peers = [z * PLANE + (j + t) % PLANE for t in PEERS]
    slots = [(j + t) % PLANE for t in PEERS]
    zpeers = [p * PLANE + j for p in planes[1:]]

    barrier = pltpu.get_barrier_semaphore()
    for dev in peers + zpeers:
        pl.semaphore_signal(barrier, inc=1, device_id=(dev,), device_id_type=MESH)

    own = [
        pltpu.make_async_copy(v1_hbm, zc.at[me, pl.ds(0, ROWS), :], lsem.at[0]),
        pltpu.make_async_copy(v2_hbm, zc.at[me, pl.ds(ROWS, ROWS), :], lsem.at[1]),
        pltpu.make_async_copy(mk_hbm, mi, lsem.at[2]),
    ]
    for cp in own:
        cp.start()
    c_copy = pltpu.make_async_copy(c_hbm, call, lsem.at[3])
    c_copy.start()
    for cp in own:
        cp.wait()
    mrow = mi[...].astype(F32)
    mbuf[me] = jnp.concatenate([mrow, mrow], axis=1)
    pl.semaphore_wait(barrier, len(peers + zpeers))

    def remote(src, dst, ssem, rsem, dev):
        return pltpu.make_async_remote_copy(src_ref=src, dst_ref=dst, send_sem=ssem, recv_sem=rsem,
                                            device_id=(dev,), device_id_type=MESH)

    pending = []

    def z_copy(i, dev):
        k = len(pending) // 2
        for cp in (remote(zc.at[i], zc.at[i], z_send.at[k], z_recv.at[i], dev),
                   remote(mbuf.at[i], mbuf.at[i], m_send.at[k], m_recv.at[i], dev)):
            pending.append(cp)
            cp.start()

    def z_wait(i):
        remote(zc.at[i], zc.at[i], z_send.at[0], z_recv.at[i], me).wait_recv()
        remote(mbuf.at[i], mbuf.at[i], m_send.at[0], m_recv.at[i], me).wait_recv()

    def rel(t):
        return planes[t] * PLANE

    def row_scores(lo, hi):
        def body(i, carry):
            k0 = pl.multiple_of(i * BLK, BLK)
            rs = lax.dot_general(zc[me], call[pl.ds(k0, BLK), :], NT, preferred_element_type=F32)
            q1_ref[:, pl.ds(k0, BLK)] = rs[:ROWS]
            q2_ref[:, pl.ds(k0, BLK)] = rs[ROWS:]
            return carry

        lax.fori_loop(lo, hi, body, 0)

    z_copy(me, first)
    z_copy(me, second)
    for dev in zpeers:
        z_copy(me, dev)
    z_copy(me, core)
    c_copy.wait()
    row_scores(0, ROW_CUTS[0])

    def take_z(t):
        z_wait(rel(t) + j)
        z_copy(rel(t) + j, first)
        if t != 1:
            z_copy(rel(t) + j, second)
        z_copy(rel(t) + j, core)

    def take_f(t):
        z_wait(rel(t) + jf)
        if t != 1:
            z_copy(rel(t) + jf, second)
        z_copy(rel(t) + jf, core)

    def take_s(t):
        z_wait(rel(t) + js)
        if t == 0:
            z_copy(rel(t) + js, zpart)
        z_copy(rel(t) + js, core)

    def take_d(t):
        z_wait(rel(t) + jd)
        if t == 0:
            z_copy(rel(t) + jd, zpart)
        z_copy(rel(t) + jd, core)

    def take_core(t):
        for q in range(4):
            z_wait(rel(t) + 2 * q + 1 - c)

    def scores(t, v):
        def body(h, carry):
            d0 = rel(t) + h * 4
            zb = zc[pl.ds(d0, 4), v * ROWS:(v + 1) * ROWS, :].reshape(BLK, DIM)
            n0 = pl.multiple_of(d0 * ROWS, BLK)
            acc = jnp.zeros((8, BLK), F32)
            for k0 in range(0, COLS, MB):
                cs = call[pl.ds(pl.multiple_of(j * COLS + k0, MB), MB), :]
                e = jnp.exp2(lax.dot_general(cs, zb, NT, preferred_element_type=F32) * (INV_T * LOG2E))
                e_ref[v, k0:k0 + MB, pl.ds(n0, BLK)] = e
                a_ref[v, k0:k0 + MB, pl.ds(n0, BLK)] = e * e
                acc = acc + jnp.sum(e.reshape(MB // 8, 8, BLK), axis=0)
            tot = jnp.sum(acc, axis=0, keepdims=True)
            for b in range(2):
                rbuf[0, v, j, pl.ds(d0 // 2 + b, 1), :] = tot[:, b * LANES:(b + 1) * LANES]
            return carry

        lax.fori_loop(0, 2, body, 0)

    take_f(0)
    take_s(0)
    take_z(1)
    take_z(2)
    take_d(0)
    take_z(3)
    take_f(1)
    take_s(1)
    take_core(0)
    scores(0, 0)
    take_f(2)
    take_s(2)
    take_d(1)
    scores(0, 1)
    take_f(3)
    take_s(3)
    take_core(1)
    scores(1, 0)
    take_d(2)
    scores(1, 1)
    take_d(3)
    take_core(2)
    scores(2, 0)
    scores(2, 1)
    take_core(3)
    scores(3, 0)
    scores(3, 1)

    def ar_copies(ph, v):
        buf = rbuf.at[ph, v, j]
        return [remote(buf, buf, ar_send.at[2 * ph + v, t], ar_recv.at[2 * ph + v, j], dev)
                for t, dev in enumerate(peers)]

    def ar_start(ph, v):
        for cp in ar_copies(ph, v):
            cp.start()

    def ar_wait(ph, v):
        for o in slots:
            buf = rbuf.at[ph, v, o]
            remote(buf, buf, ar_send.at[0, 0], ar_recv.at[2 * ph + v, o], me).wait_recv()
        tot = rbuf[ph, v, 0]
        for o in PEERS:
            tot = tot + rbuf[ph, v, o]
        return tot

    ar_start(0, 0)
    ar_start(0, 1)

    lane = lax.broadcasted_iota(jnp.int32, (1, LANES), 1)
    for b in range(DENSE):
        mden[pl.ds(b, 1), :] = jnp.where(lane < ROWS, mbuf[2 * b], mbuf[2 * b + 1])
    mask = mden[...]
    valid = jnp.sum(jnp.sum(mask, axis=0, keepdims=True), axis=1, keepdims=True)

    def spread(dense, slot, v):
        uden[...] = dense
        for b in range(DENSE):
            ub[slot, v, :, b * LANES:(b + 1) * LANES] = jnp.broadcast_to(uden[pl.ds(b, 1), :], (8, LANES))

    spread(mask, 0, 0)
    spread(mask, 0, 1)

    def sweep(ph, v):
        u = ub[0, v]

        def body(i, acc):
            rows = [pl.multiple_of((i * GRP + g) * 8, 8) for g in range(GRP)]
            for row in rows:
                col = jnp.sum(a_ref[v, pl.ds(row, 8), :] * u, axis=1, keepdims=True)
                vbc[v, pl.ds(row, 8), :] = jnp.broadcast_to(1.0 / (PROTOS * col), (8, LANES))
            for row in rows:
                vg = jnp.concatenate([vbc[v, pl.ds(row, 8), :]] * DENSE, axis=1)
                acc = acc + a_ref[v, pl.ds(row, 8), :] * vg
            return acc

        acc = lax.fori_loop(0, COLS // (8 * GRP), body, jnp.zeros((8, SAMPLES), F32))
        tot = jnp.sum(acc, axis=0, keepdims=True)
        for b in range(DENSE):
            rbuf[ph, v, j, pl.ds(b, 1), :] = tot[:, b * LANES:(b + 1) * LANES]

    def v_copies(v):
        buf = vall.at[v, j]
        return [remote(buf, buf, v_send.at[v, t], v_recv.at[v, j], dev) for t, dev in enumerate(peers)]

    def send_v(v):
        diag = (lax.broadcasted_iota(jnp.int32, (LANES, LANES), 0) == lax.broadcasted_iota(jnp.int32, (LANES, LANES), 1))
        for b in range(BLOCKS):
            blk = vbc[v, b * LANES:(b + 1) * LANES, :]
            vall[v, j, :, b * LANES:(b + 1) * LANES] = jnp.sum(jnp.where(diag, blk, 0.0), axis=0, keepdims=True)
        for cp in v_copies(v):
            cp.start()

    for it in range(ITERS):
        for v in range(2):
            if it > 0:
                spread(mask / (valid * ar_wait(it, v)), 0, v)
            sweep(it + 1, v)
            ar_start(it + 1, v)
            if it == ITERS - 1:
                send_v(v)
        row_scores(ROW_CUTS[it], ROW_CUTS[it + 1])
    mu = [mask / ar_wait(ITERS, v) for v in range(2)]

    gam = mask / (valid * 0.2)
    soft = [ar_wait(0, v) for v in range(2)]
    for v in range(2):
        spread(mu[v] * gam, 0, v)
        spread(gam / soft[v], 1, v)

    def unit_of(w):
        return w + par * (UNITS - 1 - 2 * w)

    def unit_ref(q, u):
        return dc_ref.at[pl.ds(pl.multiple_of(q * COLS + u * UNIT, UNIT), UNIT), :]

    def d_copy(q, u, ssem, rsem, dev):
        return remote(unit_ref(q, u), unit_ref(q, u), ssem, rsem, dev)

    def d_core(q, s, u):
        return d_copy(q, u, d_sc.at[s, u], dcore_recv.at[q // 2, u], core)

    def d_wait(q, s, u):
        d_copy(q, u, d_sf.at[0], d_recv.at[s, u], me).wait_recv()

    def own_block(k0, size):
        k0 = pl.multiple_of(k0, size)

        def body(i, acc):
            n0 = pl.multiple_of(i * BLK, BLK)
            es, vs = [], []
            for v in range(2):
                es.append(e_ref[v, pl.ds(k0, size), pl.ds(n0, BLK)].reshape(size // 8, 8, BLK))
                vs.append(jnp.concatenate([vbc[v, pl.ds(k0, size), :]] * 2, axis=1).reshape(size // 8, 8, BLK))
            for v in range(2):
                o = 1 - v
                g = (es[v] * ub[1, v, :, pl.ds(n0, BLK)][None]
                     - (es[o] * es[o] * vs[o]) * ub[0, o, :, pl.ds(n0, BLK)][None])
                zb = zc[pl.ds(i * 4, 4), v * ROWS:(v + 1) * ROWS, :].reshape(BLK, DIM)
                acc = acc + jnp.dot(g.reshape(size, BLK).astype(BF16), zb, preferred_element_type=F32)
            return acc

        acc = lax.fori_loop(0, SAMPLES // BLK, body, jnp.zeros((size, DIM), F32))
        dc_ref[pl.ds(pl.multiple_of(j * COLS + k0, size), size), :] = acc

    def send_own(w):
        u = unit_of(w)
        if w < DIRECT:
            d_copy(j, u, d_sf.at[u], d_recv.at[0, u], first).start()
        d_core(j, 0, u).start()

    def send_second(w):
        u = unit_of(w)
        d_copy(j, u, d_ss.at[u], d_recv.at[1, u], second).start()

    def take_first(w):
        u = unit_of(w)
        d_wait(jf, 0, u)
        d_copy(jf, u, d_fs.at[u], d_recv.at[2, u], second).start()
        if w < UNITS - DIRECT:
            d_copy(jf, u, d_sz.at[0, u], d_recv.at[0, u], zpart).start()
        d_core(jf, 1, u).start()

    def take_second(w):
        u = unit_of(w)
        d_wait(js, 1, u)
        if w < UNITS - DIRECT:
            d_copy(js, u, d_sz.at[1, u], d_recv.at[1, u], zpart).start()
        d_core(js, 2, u).start()

    def take_diag(w):
        u = unit_of(w)
        d_wait(jd, 2, u)
        if w < UNITS - DIRECT:
            d_copy(jd, u, d_sz.at[2, u], d_recv.at[2, u], zpart).start()
        d_core(jd, 3, u).start()

    LAG = 3

    def step(w):
        take_first(w)
        if w + LAG < DIRECT:
            send_second(w + LAG)
        take_second(w)
        if w >= LAG:
            take_diag(w - LAG)

    def own_units(b):
        own_block((b + par * (BLOCKS - 1 - 2 * b)) * LANES, LANES)
        send_own(2 * b)
        send_own(2 * b + 1)

    for w in range(2):
        own_block(unit_of(w) * UNIT, UNIT)
        send_own(w)
        send_second(w)
    own_units(1)
    send_second(2)
    early = DIRECT // 2 + 1
    for b in range(2, early):
        own_units(b)
        step(b - 2)

    sub = lax.broadcasted_iota(jnp.int32, (ROWS, LANES), 0)
    pick = lax.broadcasted_iota(jnp.int32, (ROWS, LANES), 1) == sub + ROWS * (me % 2)

    def own_rows(dense):
        uden[...] = dense
        row = jnp.broadcast_to(uden[pl.ds(me // 2, 1), :], (ROWS, LANES))
        return jnp.sum(jnp.where(pick, row, 0.0), axis=1, keepdims=True)

    gm = own_rows(gam)
    mus = [own_rows(mu[v]) for v in range(2)]
    ps = [own_rows(soft[v]) for v in range(2)]
    ips = [1.0 / p for p in ps]
    lps = [jnp.log(p) for p in ps]
    for v in range(2):
        for o in slots:
            buf = vall.at[v, o]
            remote(buf, buf, v_send.at[0, 0], v_recv.at[v, o], me).wait_recv()
    q_refs = (q1_ref, q2_ref)
    chunks = COLS // BLK

    def row_body(i, carry):
        dz, lacc = carry
        k0 = pl.multiple_of(i * BLK, BLK)
        l0 = pl.multiple_of((i % chunks) * BLK, BLK)
        ss, es, qs, gs = [], [], [], []
        for v in range(2):
            ss.append(q_refs[v][:, pl.ds(k0, BLK)] * INV_T)
            es.append(jnp.exp2(ss[v] * LOG2E))
            qs.append((es[v] * es[v]) * mus[v] * vall[v, i // chunks, :, pl.ds(l0, BLK)])
            q_refs[v][:, pl.ds(k0, BLK)] = qs[v]
        for v in range(2):
            lsum = qs[1 - v] * (ss[v] - lps[v])
            lacc = lacc + jnp.sum(lsum.reshape(ROWS // 8, 8, BLK), axis=0)
            gs.append((es[v] * ips[v] - qs[1 - v]) * gm)
        g = jnp.concatenate(gs, axis=0).astype(BF16)
        return dz + jnp.dot(g, call[pl.ds(k0, BLK), :], preferred_element_type=F32), lacc

    carry = (jnp.zeros((SLAB, DIM), F32), jnp.zeros((8, BLK), F32))
    cuts = (0, 7, 14, 20, 26, PROTOS // BLK)
    for i, (lo, hi) in enumerate(zip(cuts[:-1], cuts[1:])):
        carry = lax.fori_loop(lo, hi, row_body, carry)
        step(early - 2 + i)
    dz, lacc = carry
    dz1_ref[...] = dz[:ROWS]
    dz2_ref[...] = dz[ROWS:]
    lpart = jnp.sum(jnp.sum(lacc, axis=0, keepdims=True), axis=1, keepdims=True)
    lbuf[j] = jnp.broadcast_to(lpart, (8, LANES))
    l_copies = [remote(lbuf.at[j], lbuf.at[j], l_send.at[t], l_recv.at[j], dev) for t, dev in enumerate(peers)]
    for cp in l_copies:
        cp.start()

    for b in range(early, BLOCKS):
        own_units(b)
        step(b + len(cuts) - LAG)

    for o in slots:
        remote(lbuf.at[o], lbuf.at[o], l_send.at[0], l_recv.at[o], me).wait_recv()
    lsum = lbuf[0]
    for o in PEERS:
        lsum = lsum + lbuf[o]
    lzbuf[z] = lsum
    lz_copies = [remote(lzbuf.at[z], lzbuf.at[z], lz_send.at[t], lz_recv.at[z], dev) for t, dev in enumerate(zpeers)]
    for cp in lz_copies:
        cp.start()

    for w in range(DIRECT - LAG, DIRECT):
        take_diag(w)

    for w in reversed(range(DIRECT, UNITS)):
        u = unit_of(w)
        for s, q in ((0, jf), (1, js), (2, jd)):
            d_wait(q, s, u)
            d_core(q, s + 1, u).start()

    for o in planes[1:]:
        remote(lzbuf.at[o], lzbuf.at[o], lz_send.at[0], lz_recv.at[o], me).wait_recv()
    loss = lzbuf[0]
    for o in range(1, PLANES):
        loss = loss + lzbuf[o]
    loss_ref[...] = (-loss / (2.0 * valid))[:1, :1]

    @pl.loop(0, UNITS)
    def _(u):
        for q in range(4):
            d_copy(2 * q + 1 - c, u, d_sf.at[0], dcore_recv.at[q, u], me).wait_recv()

    for v in range(2):
        for ph in range(ITERS + 1):
            pending += ar_copies(ph, v)
        pending += v_copies(v)
    for cp in pending + l_copies + lz_copies:
        cp.wait_send()
    for w in range(UNITS):
        u = unit_of(w)
        for s in range(4):
            d_copy(j, u, d_sc.at[s, u], dcore_recv.at[0, u], core).wait_send()
        if w < DIRECT:
            d_copy(j, u, d_sf.at[u], d_recv.at[0, u], first).wait_send()
            d_copy(j, u, d_ss.at[u], d_recv.at[1, u], second).wait_send()
            d_copy(jf, u, d_fs.at[u], d_recv.at[2, u], second).wait_send()
        if w < UNITS - DIRECT:
            for s in range(3):
                d_copy(j, u, d_sz.at[s, u], d_recv.at[s, u], zpart).wait_send()


STORE = (4, 4, 1, 1, 1, 8)


def store_kernel(*refs):
    results = len(STORE)
    sem = refs[2 * results]
    copies = []
    for i, pieces in enumerate(STORE):
        src, dst = refs[i], refs[results + i]
        rows = src.shape[0] // pieces
        for p in range(pieces):
            part = pl.ds(p * rows, rows)
            copies.append(pltpu.make_async_copy(src.at[part, :], dst.at[part, :], sem.at[len(copies)]))
            copies[-1].start()
    for cp in copies:
        cp.wait()


def solution(mesh):
    def local_step(view_one, view_two, protos, valid_mask):
        dma = pltpu.SemaphoreType.DMA
        outs = pl.pallas_call(
            kernel,
            out_shape=[
                pltpu.VMEM((ROWS, PROTOS), F32),
                pltpu.VMEM((ROWS, PROTOS), F32),
                pltpu.VMEM((1, 1), F32),
                pltpu.VMEM((ROWS, DIM), F32),
                pltpu.VMEM((ROWS, DIM), F32),
                pltpu.VMEM((PROTOS, DIM), F32),
            ],
            in_specs=[pl.BlockSpec(memory_space=pl.ANY)] * 4,
            out_specs=[pl.BlockSpec(memory_space=pltpu.VMEM)] * 6,
            scratch_shapes=[
                pltpu.VMEM((DEVS, SLAB, DIM), BF16),
                pltpu.VMEM((1, ROWS), jnp.int32),
                pltpu.VMEM((DEVS, 1, LANES), F32),
                pltpu.VMEM((PROTOS, DIM), BF16),
                pltpu.VMEM((2, COLS, SAMPLES), F32),
                pltpu.VMEM((2, COLS, SAMPLES), F32),
                pltpu.VMEM((2, COLS, LANES), F32),
                pltpu.VMEM((DENSE, LANES), F32),
                pltpu.VMEM((DENSE, LANES), F32),
                pltpu.VMEM((2, 2, 8, SAMPLES), F32),
                pltpu.VMEM((ITERS + 1, 2, PLANE, DENSE, LANES), F32),
                pltpu.VMEM((2, PLANE, 1, COLS), F32),
                pltpu.VMEM((PLANE, 8, LANES), F32),
                pltpu.VMEM((PLANES, 8, LANES), F32),
                dma((4,)), dma((DEVS - 1,)), dma((DEVS,)), dma((DEVS - 1,)), dma((DEVS,)),
                dma((2 * ITERS + 2, PLANE - 1)), dma((2 * ITERS + 2, PLANE)),
                dma((2, PLANE - 1)), dma((2, PLANE)),
                dma((PLANE - 1,)), dma((PLANE,)), dma((PLANES - 1,)), dma((PLANES,)),
                dma((3, UNITS)), dma((4, UNITS)), dma((UNITS,)), dma((UNITS,)), dma((4, UNITS)),
                dma((UNITS,)), dma((3, UNITS)),
            ],
            compiler_params=pltpu.CompilerParams(
                collective_id=0, has_side_effects=True, vmem_limit_bytes=48 << 20),
        )(view_one, view_two, valid_mask.reshape(1, ROWS), protos)
        outs = pl.pallas_call(
            store_kernel,
            out_shape=[jax.ShapeDtypeStruct(o.shape, o.dtype) for o in outs],
            in_specs=[pl.BlockSpec(memory_space=pltpu.VMEM)] * len(STORE),
            out_specs=[pl.BlockSpec(memory_space=pl.ANY)] * len(STORE),
            scratch_shapes=[dma((sum(STORE),))],
            compiler_params=pltpu.CompilerParams(vmem_limit_bytes=4 << 20),
        )(*[pltpu.with_memory_space_constraint(o, pltpu.VMEM) for o in outs])
        q1, q2, loss, dz1, dz2, dc = outs
        return q1, q2, loss.reshape(()), dz1, dz2, dc

    return jax.shard_map(
        local_step,
        mesh=mesh,
        in_specs=(P("data", None), P("data", None), P(None, None), P("data")),
        out_specs=(P("data", None), P("data", None), P(), P("data", None), P("data", None), P(None, None)),
        check_vma=False,
    )
```

```python
import jax
import jax.numpy as jnp
from jax import lax
from jax.experimental import pallas as pl
from jax.experimental.pallas import tpu as pltpu
from jax.sharding import PartitionSpec as P

MESH = pl.DeviceIdType.MESH
F32 = jnp.float32
BF16 = jnp.bfloat16

ROWS = 64
SLAB = 2 * ROWS
DEVS = 32
PLANE = 8
SAMPLES = ROWS * DEVS
MB = 256
PROTOS = 8192
DIM = 256
COLS = PROTOS // PLANE
ITERS = 3
LANES = 128
PLANES = DEVS // PLANE
CHIPS = PLANE // 2
PEERS = range(1, PLANE)
BLK = 2 * LANES
DENSE = SAMPLES // LANES
INV_T = 10.0
UNIT = 64
UNITS = COLS // UNIT
BLOCKS = COLS // LANES
DIRECT = 11
KDEPTH = 1024
RCOLS = 1024
LAG = 3
QCOLS = 512
GRP = 32
LOG2E = 1.4426950408889634
ROW_CUTS = (1, 3, 5, 7, 8)
NT = (((1,), (1,)), ((), ()))


def kernel(v1_hbm, v2_hbm, mk_hbm, c_hbm,
           q1_ref, q2_ref, loss_ref, dz1_ref, dz2_ref, dc_ref,
           zc, mi, mbuf, call, a_ref, vbc, mden, uden, ub, rbuf, vall, lbuf, lzbuf,
           lsem, z_send, z_recv, m_send, m_recv, ar_send, ar_recv, v_send, v_recv,
           l_send, l_recv, lz_send, lz_recv,
           d_recv, dcore_recv, d_sf, d_ss, d_sc, d_fs, d_sz):
    me = lax.axis_index("data")
    z = me // PLANE
    j = me % PLANE
    c = j % 2
    x = (j // 2) % 2
    y = j // 4
    jx = j + 2 - 4 * x
    jy = j + 4 - 8 * y
    jd = (6 - 2 * (j // 2)) + c
    jf = jx + c * (jy - jx)
    js = jy + c * (jx - jy)
    core = me + 1 - 2 * c
    own_slot = z * PLANE + c * CHIPS + j // 2
    first = z * PLANE + jf
    second = z * PLANE + js
    par = z % 2
    planes = (z, z + 1 - 2 * par, z + 2 - PLANES * (z // 2), PLANES - 1 - z)
    zpart = planes[1] * PLANE + j
    peers = [z * PLANE + (j + t) % PLANE for t in PEERS]
    slots = [(j + t) % PLANE for t in PEERS]
    zpeers = [p * PLANE + j for p in planes[1:]]

    barrier = pltpu.get_barrier_semaphore()
    for dev in peers + zpeers:
        pl.semaphore_signal(barrier, inc=1, device_id=(dev,), device_id_type=MESH)

    own = [
        pltpu.make_async_copy(v1_hbm, zc.at[own_slot, pl.ds(0, ROWS), :], lsem.at[0]),
        pltpu.make_async_copy(v2_hbm, zc.at[own_slot, pl.ds(ROWS, ROWS), :], lsem.at[1]),
        pltpu.make_async_copy(mk_hbm, mi, lsem.at[2]),
    ]
    for cp in own:
        cp.start()
    c_copy = pltpu.make_async_copy(c_hbm, call, lsem.at[3])
    c_copy.start()
    for cp in own:
        cp.wait()
    mrow = mi[...].astype(F32)
    mbuf[own_slot] = jnp.concatenate([mrow, mrow], axis=1)
    pl.semaphore_wait(barrier, len(peers + zpeers))

    def remote(src, dst, ssem, rsem, dev):
        return pltpu.make_async_remote_copy(src_ref=src, dst_ref=dst, send_sem=ssem, recv_sem=rsem,
                                            device_id=(dev,), device_id_type=MESH)

    pending = []

    def z_copy(i, dev):
        k = len(pending) // 2
        for cp in (remote(zc.at[i], zc.at[i], z_send.at[k], z_recv.at[i], dev),
                   remote(mbuf.at[i], mbuf.at[i], m_send.at[k], m_recv.at[i], dev)):
            pending.append(cp)
            cp.start()

    def z_wait(i):
        remote(zc.at[i], zc.at[i], z_send.at[0], z_recv.at[i], me).wait_recv()
        remote(mbuf.at[i], mbuf.at[i], m_send.at[0], m_recv.at[i], me).wait_recv()

    def row_scores(lo, hi):
        def body(i, carry):
            k0 = pl.multiple_of(i * RCOLS, RCOLS)
            rs = lax.dot_general(zc[own_slot], call[pl.ds(k0, RCOLS), :], NT, preferred_element_type=F32)
            q1_ref[:, pl.ds(k0, RCOLS)] = rs[:ROWS]
            q2_ref[:, pl.ds(k0, RCOLS)] = rs[ROWS:]
            return carry

        lax.fori_loop(lo, hi, body, 0)

    z_copy(own_slot, first)
    z_copy(own_slot, second)
    for dev in zpeers:
        z_copy(own_slot, dev)
    z_copy(own_slot, core)
    c_copy.wait()
    row_scores(0, ROW_CUTS[0])

    def take(t, k, *devs):
        i = planes[t] * PLANE + c * CHIPS + k // 2
        z_wait(i)
        for dev in devs + (core,):
            z_copy(i, dev)

    def take_z(t):
        take(t, j, *((first,) if t == 1 else (first, second)))

    def take_f(t):
        take(t, jf, *(() if t == 1 else (second,)))

    def take_s(t):
        take(t, js, *((zpart,) if t == 0 else ()))

    def take_d(t):
        take(t, jd, *((zpart,) if t == 0 else ()))

    def take_core(t):
        for q in range(CHIPS):
            z_wait(planes[t] * PLANE + (1 - c) * CHIPS + q)

    def scores(t, k):
        d0 = planes[t] * PLANE + k * CHIPS
        n0 = pl.multiple_of(d0 * ROWS, BLK)

        for v in range(2):
            zb = zc[pl.ds(d0, CHIPS), v * ROWS:(v + 1) * ROWS, :].reshape(BLK, DIM)
            acc = jnp.zeros((8, BLK), F32)
            for k0 in range(0, COLS, MB):
                cs = call[pl.ds(pl.multiple_of(j * COLS + k0, MB), MB), :]
                e = jnp.exp2(lax.dot_general(cs, zb, NT, preferred_element_type=F32) * (INV_T * LOG2E))
                a_ref[v, k0:k0 + MB, pl.ds(n0, BLK)] = e * e
                acc = acc + jnp.sum(e.reshape(MB // 8, 8, BLK), axis=0)
            tot = jnp.sum(acc, axis=0, keepdims=True)
            for b in range(2):
                rbuf[0, v, j, pl.ds(d0 // 2 + b, 1), :] = tot[:, b * LANES:(b + 1) * LANES]

    def own_scores(t):
        scores(t, c)

    def other_scores(t):
        take_core(t)
        scores(t, 1 - c)

    take_f(0)
    take_s(0)
    take_z(1)
    row_scores(ROW_CUTS[0], ROW_CUTS[1])
    take_z(2)
    take_d(0)
    take_z(3)
    take_f(1)
    take_s(1)
    own_scores(0)
    take_f(2)
    take_s(2)
    take_d(1)
    own_scores(1)
    other_scores(0)
    take_f(3)
    take_s(3)
    take_d(2)
    own_scores(2)
    other_scores(1)
    take_d(3)
    own_scores(3)
    other_scores(2)
    other_scores(3)

    def ar_copies(ph, v):
        buf = rbuf.at[ph, v, j]
        return [remote(buf, buf, ar_send.at[2 * ph + v, t], ar_recv.at[2 * ph + v, j], dev)
                for t, dev in enumerate(peers)]

    def ar_start(ph, v):
        for cp in ar_copies(ph, v):
            cp.start()

    def ar_wait(ph, v):
        for o in slots:
            buf = rbuf.at[ph, v, o]
            remote(buf, buf, ar_send.at[0, 0], ar_recv.at[2 * ph + v, o], me).wait_recv()
        tot = rbuf[ph, v, 0]
        for o in PEERS:
            tot = tot + rbuf[ph, v, o]
        return tot

    ar_start(0, 0)
    ar_start(0, 1)

    lane = lax.broadcasted_iota(jnp.int32, (1, LANES), 1)
    for b in range(DENSE):
        mden[pl.ds(b, 1), :] = jnp.where(lane < ROWS, mbuf[2 * b], mbuf[2 * b + 1])
    mask = mden[...]
    valid = jnp.sum(jnp.sum(mask, axis=0, keepdims=True), axis=1, keepdims=True)

    def spread(dense, slot, v):
        uden[...] = dense
        for b in range(DENSE):
            ub[slot, v, :, b * LANES:(b + 1) * LANES] = jnp.broadcast_to(uden[pl.ds(b, 1), :], (8, LANES))

    spread(mask, 0, 0)
    spread(mask, 0, 1)

    def sweep(ph, v):
        u = ub[0, v]

        def body(i, acc):
            rows = [pl.multiple_of((i * GRP + g) * 8, 8) for g in range(GRP)]
            for row in rows:
                col = jnp.sum(a_ref[v, pl.ds(row, 8), :] * u, axis=1, keepdims=True)
                vbc[v, pl.ds(row, 8), :] = jnp.broadcast_to(1.0 / (PROTOS * col), (8, LANES))
            for row in rows:
                vg = jnp.concatenate([vbc[v, pl.ds(row, 8), :]] * DENSE, axis=1)
                acc = acc + a_ref[v, pl.ds(row, 8), :] * vg
            return acc

        acc = lax.fori_loop(0, COLS // (8 * GRP), body, jnp.zeros((8, SAMPLES), F32))
        tot = jnp.sum(acc, axis=0, keepdims=True)
        for b in range(DENSE):
            rbuf[ph, v, j, pl.ds(b, 1), :] = tot[:, b * LANES:(b + 1) * LANES]

    def v_copies(v):
        buf = vall.at[v, j]
        return [remote(buf, buf, v_send.at[v, t], v_recv.at[v, j], dev) for t, dev in enumerate(peers)]

    def send_v(v):
        diag = (lax.broadcasted_iota(jnp.int32, (LANES, LANES), 0) == lax.broadcasted_iota(jnp.int32, (LANES, LANES), 1))
        for b in range(BLOCKS):
            blk = vbc[v, b * LANES:(b + 1) * LANES, :]
            vall[v, j, :, b * LANES:(b + 1) * LANES] = jnp.sum(jnp.where(diag, blk, 0.0), axis=0, keepdims=True)
        for cp in v_copies(v):
            cp.start()

    for it in range(ITERS):
        for v in range(2):
            if it > 0:
                spread(mask / (valid * ar_wait(it, v)), 0, v)
            sweep(it + 1, v)
            ar_start(it + 1, v)
            if it == ITERS - 1:
                send_v(v)
        row_scores(ROW_CUTS[it + 1], ROW_CUTS[it + 2])

    gam = mask / (valid * 0.2)
    soft = [ar_wait(0, v) for v in range(2)]
    for v in range(2):
        spread(gam / soft[v], 1, v)

    def unit_of(w):
        return w + par * (UNITS - 1 - 2 * w)

    def unit_ref(q, u):
        return dc_ref.at[pl.ds(pl.multiple_of(q * COLS + u * UNIT, UNIT), UNIT), :]

    def d_copy(q, u, ssem, rsem, dev):
        return remote(unit_ref(q, u), unit_ref(q, u), ssem, rsem, dev)

    def d_core(q, s, u):
        return d_copy(q, u, d_sc.at[s, u], dcore_recv.at[q // 2, u], core)

    def d_wait(q, s, u):
        d_copy(q, u, d_sf.at[0], d_recv.at[s, u], me).wait_recv()

    def grad_part(k0, size, v, acc):
        k0 = pl.multiple_of(k0, size)
        o = 1 - v

        wide = KDEPTH // BLK
        devs = KDEPTH // ROWS

        def body(i, acc):
            n0 = pl.multiple_of(i * KDEPTH, KDEPTH)
            a = a_ref[v, pl.ds(k0, size), pl.ds(n0, KDEPTH)].reshape(size // 8, 8, KDEPTH)
            ao = a_ref[o, pl.ds(k0, size), pl.ds(n0, KDEPTH)].reshape(size // 8, 8, KDEPTH)
            vo = jnp.concatenate([vbc[o, pl.ds(k0, size), :]] * (2 * wide), axis=1).reshape(size // 8, 8, KDEPTH)
            g = (a * lax.rsqrt(a)) * ub[1, v, :, pl.ds(n0, KDEPTH)][None] - (ao * vo) * ub[0, o, :, pl.ds(n0, KDEPTH)][None]
            zb = zc[pl.ds(i * devs, devs), v * ROWS:(v + 1) * ROWS, :].reshape(KDEPTH, DIM)
            return acc + jnp.dot(g.reshape(size, KDEPTH).astype(BF16), zb, preferred_element_type=F32)

        return lax.fori_loop(0, SAMPLES // KDEPTH, body, acc)

    def grad_first(k0, size):
        return grad_part(k0, size, 1, jnp.zeros((size, DIM), F32))

    def grad_rest(k0, size, acc):
        dc_ref[pl.ds(pl.multiple_of(j * COLS + k0, size), size), :] = grad_part(k0, size, 0, acc)

    def send_own(w):
        u = unit_of(w)
        if w < DIRECT:
            d_copy(j, u, d_sf.at[u], d_recv.at[0, u], first).start()
        d_core(j, 0, u).start()

    def send_second(w):
        u = unit_of(w)
        d_copy(j, u, d_ss.at[u], d_recv.at[1, u], second).start()

    def take_first(w):
        u = unit_of(w)
        d_wait(jf, 0, u)
        d_copy(jf, u, d_fs.at[u], d_recv.at[2, u], second).start()
        if w < UNITS - DIRECT:
            d_copy(jf, u, d_sz.at[0, u], d_recv.at[0, u], zpart).start()
        d_core(jf, 1, u).start()
        if w + LAG < DIRECT:
            send_second(w + LAG)

    def take_second(w):
        u = unit_of(w)
        d_wait(js, 1, u)
        if w < UNITS - DIRECT:
            d_copy(js, u, d_sz.at[1, u], d_recv.at[1, u], zpart).start()
        d_core(js, 2, u).start()

    def take_diag(w):
        u = unit_of(w)
        d_wait(jd, 2, u)
        if w < UNITS - DIRECT:
            d_copy(jd, u, d_sz.at[2, u], d_recv.at[2, u], zpart).start()
        d_core(jd, 3, u).start()

    def own_units(b):
        k0 = (b + par * (BLOCKS - 1 - 2 * b)) * LANES
        grad_rest(k0, LANES, grad_first(k0, LANES))
        send_own(2 * b)
        send_own(2 * b + 1)

    mu = [mask / ar_wait(ITERS, 0)]
    spread(mu[0] * gam, 0, 0)
    parts = [grad_first(unit_of(w) * UNIT, UNIT) for w in range(2)]
    mu.append(mask / ar_wait(ITERS, 1))
    spread(mu[1] * gam, 0, 1)
    for w in range(2):
        grad_rest(unit_of(w) * UNIT, UNIT, parts[w])
        send_own(w)
        send_second(w)
    own_units(1)
    send_second(2)
    own_units(2)

    sub = lax.broadcasted_iota(jnp.int32, (ROWS, LANES), 0)
    pick = lax.broadcasted_iota(jnp.int32, (ROWS, LANES), 1) == sub + ROWS * (own_slot % 2)

    def own_rows(dense):
        uden[...] = dense
        row = jnp.broadcast_to(uden[pl.ds(own_slot // 2, 1), :], (ROWS, LANES))
        return jnp.sum(jnp.where(pick, row, 0.0), axis=1, keepdims=True)

    gm = own_rows(gam)
    mus = [own_rows(mu[v]) for v in range(2)]
    ps = [own_rows(soft[v]) for v in range(2)]
    ips = [1.0 / p for p in ps]
    lps = [jnp.log(p) for p in ps]
    for v in range(2):
        for o in slots:
            buf = vall.at[v, o]
            remote(buf, buf, v_send.at[0, 0], v_recv.at[v, o], me).wait_recv()
    q_refs = (q1_ref, q2_ref)
    chunks = COLS // QCOLS

    def row_body(i, carry):
        dz, lacc = carry
        k0 = pl.multiple_of(i * QCOLS, QCOLS)
        l0 = pl.multiple_of((i % chunks) * QCOLS, QCOLS)
        ss, es, qs, gs = [], [], [], []
        for v in range(2):
            ss.append(q_refs[v][:, pl.ds(k0, QCOLS)] * INV_T)
            es.append(jnp.exp2(ss[v] * LOG2E))
            qs.append((es[v] * es[v]) * mus[v] * vall[v, i // chunks, :, pl.ds(l0, QCOLS)])
            q_refs[v][:, pl.ds(k0, QCOLS)] = qs[v]
        for v in range(2):
            lsum = qs[1 - v] * (ss[v] - lps[v])
            lacc = lacc + jnp.sum(lsum.reshape(ROWS // 8, 8, QCOLS), axis=0)
            gs.append((es[v] * ips[v] - qs[1 - v]) * gm)
        g = jnp.concatenate(gs, axis=0).astype(BF16)
        return dz + jnp.dot(g, call[pl.ds(k0, QCOLS), :], preferred_element_type=F32), lacc

    carry = (jnp.zeros((SLAB, DIM), F32), jnp.zeros((8, QCOLS), F32))
    cuts = (0, 4, 7, 10, 13, PROTOS // QCOLS)

    def row_part(i, carry):
        return lax.fori_loop(cuts[i], cuts[i + 1], row_body, carry)

    carry = row_part(0, carry)
    take_first(0)
    take_second(0)
    carry = row_part(1, carry)
    take_first(1)
    take_second(1)
    own_units(3)
    take_first(2)
    take_second(2)
    carry = row_part(2, carry)
    take_first(3)
    take_diag(0)
    carry = row_part(3, carry)
    take_first(4)
    take_second(3)
    dz, lacc = row_part(4, carry)
    dz1_ref[...] = dz[:ROWS]
    dz2_ref[...] = dz[ROWS:]
    lpart = jnp.sum(jnp.sum(lacc, axis=0, keepdims=True), axis=1, keepdims=True)
    lbuf[j] = jnp.broadcast_to(lpart, (8, LANES))
    l_copies = [remote(lbuf.at[j], lbuf.at[j], l_send.at[t], l_recv.at[j], dev) for t, dev in enumerate(peers)]
    for cp in l_copies:
        cp.start()
    own_units(4)
    take_first(5)
    take_diag(1)
    take_first(6)
    take_second(4)
    own_units(5)
    take_first(7)
    take_diag(2)
    take_first(8)
    take_second(5)
    own_units(6)
    take_first(9)
    take_diag(3)
    take_first(10)
    take_second(6)
    take_diag(4)

    for o in slots:
        remote(lbuf.at[o], lbuf.at[o], l_send.at[0], l_recv.at[o], me).wait_recv()
    lsum = lbuf[0]
    for o in PEERS:
        lsum = lsum + lbuf[o]
    lzbuf[z] = lsum
    lz_copies = [remote(lzbuf.at[z], lzbuf.at[z], lz_send.at[t], lz_recv.at[z], dev) for t, dev in enumerate(zpeers)]
    for cp in lz_copies:
        cp.start()

    own_units(7)
    for w in range(7, DIRECT):
        take_second(w)
        take_diag(w - 2)
    take_diag(DIRECT - 2)
    take_diag(DIRECT - 1)

    for w in reversed(range(DIRECT, UNITS)):
        u = unit_of(w)
        for s, q in ((0, jf), (1, js), (2, jd)):
            d_wait(q, s, u)
            d_core(q, s + 1, u).start()

    for o in planes[1:]:
        remote(lzbuf.at[o], lzbuf.at[o], lz_send.at[0], lz_recv.at[o], me).wait_recv()
    loss = lzbuf[0]
    for o in range(1, PLANES):
        loss = loss + lzbuf[o]
    loss_ref[...] = (-loss / (2.0 * valid))[:1, :1]

    @pl.loop(0, UNITS)
    def _(u):
        for q in range(4):
            d_copy(2 * q + 1 - c, u, d_sf.at[0], dcore_recv.at[q, u], me).wait_recv()

    for v in range(2):
        for ph in range(ITERS + 1):
            pending += ar_copies(ph, v)
        pending += v_copies(v)
    for cp in pending + l_copies + lz_copies:
        cp.wait_send()
    for w in range(UNITS):
        u = unit_of(w)
        for s in range(4):
            d_copy(j, u, d_sc.at[s, u], dcore_recv.at[0, u], core).wait_send()
        if w < DIRECT:
            d_copy(j, u, d_sf.at[u], d_recv.at[0, u], first).wait_send()
            d_copy(j, u, d_ss.at[u], d_recv.at[1, u], second).wait_send()
            d_copy(jf, u, d_fs.at[u], d_recv.at[2, u], second).wait_send()
        if w < UNITS - DIRECT:
            for s in range(3):
                d_copy(j, u, d_sz.at[s, u], d_recv.at[s, u], zpart).wait_send()


STORE = (4, 4, 1, 1, 1, 8)


def store_kernel(*refs):
    results = len(STORE)
    sem = refs[2 * results]
    copies = []
    for i, pieces in enumerate(STORE):
        src, dst = refs[i], refs[results + i]
        rows = src.shape[0] // pieces
        for p in range(pieces):
            part = pl.ds(p * rows, rows)
            copies.append(pltpu.make_async_copy(src.at[part, :], dst.at[part, :], sem.at[len(copies)]))
            copies[-1].start()
    for cp in copies:
        cp.wait()


def solution(mesh):
    def local_step(view_one, view_two, protos, valid_mask):
        dma = pltpu.SemaphoreType.DMA
        outs = pl.pallas_call(
            kernel,
            out_shape=[
                pltpu.VMEM((ROWS, PROTOS), F32),
                pltpu.VMEM((ROWS, PROTOS), F32),
                pltpu.VMEM((1, 1), F32),
                pltpu.VMEM((ROWS, DIM), F32),
                pltpu.VMEM((ROWS, DIM), F32),
                pltpu.VMEM((PROTOS, DIM), F32),
            ],
            in_specs=[pl.BlockSpec(memory_space=pl.ANY)] * 4,
            out_specs=[pl.BlockSpec(memory_space=pltpu.VMEM)] * 6,
            scratch_shapes=[
                pltpu.VMEM((DEVS, SLAB, DIM), BF16),
                pltpu.VMEM((1, ROWS), jnp.int32),
                pltpu.VMEM((DEVS, 1, LANES), F32),
                pltpu.VMEM((PROTOS, DIM), BF16),
                pltpu.VMEM((2, COLS, SAMPLES), F32),
                pltpu.VMEM((2, COLS, LANES), F32),
                pltpu.VMEM((DENSE, LANES), F32),
                pltpu.VMEM((DENSE, LANES), F32),
                pltpu.VMEM((2, 2, 8, SAMPLES), F32),
                pltpu.VMEM((ITERS + 1, 2, PLANE, DENSE, LANES), F32),
                pltpu.VMEM((2, PLANE, 1, COLS), F32),
                pltpu.VMEM((PLANE, 8, LANES), F32),
                pltpu.VMEM((PLANES, 8, LANES), F32),
                dma((4,)), dma((DEVS - 1,)), dma((DEVS,)), dma((DEVS - 1,)), dma((DEVS,)),
                dma((2 * ITERS + 2, PLANE - 1)), dma((2 * ITERS + 2, PLANE)),
                dma((2, PLANE - 1)), dma((2, PLANE)),
                dma((PLANE - 1,)), dma((PLANE,)), dma((PLANES - 1,)), dma((PLANES,)),
                dma((3, UNITS)), dma((4, UNITS)), dma((UNITS,)), dma((UNITS,)), dma((4, UNITS)),
                dma((UNITS,)), dma((3, UNITS)),
            ],
            compiler_params=pltpu.CompilerParams(
                collective_id=0, has_side_effects=True, vmem_limit_bytes=48 << 20),
        )(view_one, view_two, valid_mask.reshape(1, ROWS), protos)
        outs = pl.pallas_call(
            store_kernel,
            out_shape=[jax.ShapeDtypeStruct(o.shape, o.dtype) for o in outs],
            in_specs=[pl.BlockSpec(memory_space=pltpu.VMEM)] * len(STORE),
            out_specs=[pl.BlockSpec(memory_space=pl.ANY)] * len(STORE),
            scratch_shapes=[dma((sum(STORE),))],
            compiler_params=pltpu.CompilerParams(vmem_limit_bytes=4 << 20),
        )(*[pltpu.with_memory_space_constraint(o, pltpu.VMEM) for o in outs])
        q1, q2, loss, dz1, dz2, dc = outs
        return q1, q2, loss.reshape(()), dz1, dz2, dc

    return jax.shard_map(
        local_step,
        mesh=mesh,
        in_specs=(P("data", None), P("data", None), P(None, None), P("data")),
        out_specs=(P("data", None), P("data", None), P(), P("data", None), P("data", None), P(None, None)),
        check_vma=False,
    )
```

```python
import jax
import jax.numpy as jnp
from jax import lax
from jax.experimental import pallas as pl
from jax.experimental.pallas import tpu as pltpu
from jax.sharding import PartitionSpec as P

MESH = pl.DeviceIdType.MESH
F32 = jnp.float32
BF16 = jnp.bfloat16

ROWS = 64
SLAB = 2 * ROWS
DEVS = 32
PLANE = 8
SAMPLES = ROWS * DEVS
MB = 256
PROTOS = 8192
DIM = 256
COLS = PROTOS // PLANE
ITERS = 3
LANES = 128
PLANES = DEVS // PLANE
CHIPS = PLANE // 2
PEERS = range(1, PLANE)
BLK = 2 * LANES
DENSE = SAMPLES // LANES
INV_T = 10.0
UNIT = 64
UNITS = COLS // UNIT
BLOCKS = COLS // LANES
FIRST = 12
SECOND = 11
DIAG = 4
LOCAL = COLS - 2 * DIAG * UNIT
KDEPTH = 1024
RCOLS = 1024
LAG = 3
QCOLS = 512
GRP = 32
LOG2E = 1.4426950408889634
ROW_CUTS = (1, 3, 5, 7, 8)
DIAG_CUTS = (0, 4, 5, 8)
NT = (((1,), (1,)), ((), ()))


def kernel(v1_hbm, v2_hbm, mk_hbm, c_hbm,
           q1_ref, q2_ref, loss_ref, dz1_ref, dz2_ref, dc_ref,
           zc, mi, mbuf, call, a_ref, ad_ref, vbc, vd, mden, uden, ub, rbuf, vall, lbuf, lzbuf,
           lsem, z_send, z_recv, zcore_recv, m_recv, mcore_recv, ar_send, ar_recv, v_recv, l_recv, d_recv, d_send):
    me = lax.axis_index("data")
    z = me // PLANE
    j = me % PLANE
    c = j % 2
    x = (j // 2) % 2
    y = j // 4
    jx = j + 2 - 4 * x
    jy = j + 4 - 8 * y
    jd = (6 - 2 * (j // 2)) + c
    jf = jx + c * (jy - jx)
    js = jy + c * (jx - jy)
    core = me + 1 - 2 * c
    own_slot = z * PLANE + c * CHIPS + j // 2
    first = z * PLANE + jf
    second = z * PLANE + js
    par = z % 2
    planes = (z, z + 1 - 2 * par, z + 2 - PLANES * (z // 2), PLANES - 1 - z)
    zpart = planes[1] * PLANE + j
    peers = [z * PLANE + (j + t) % PLANE for t in PEERS]
    zpeers = [p * PLANE + j for p in planes[1:]]

    barrier = pltpu.get_barrier_semaphore()
    for dev in peers + zpeers:
        pl.semaphore_signal(barrier, inc=1, device_id=(dev,), device_id_type=MESH)

    own = [
        pltpu.make_async_copy(v1_hbm, zc.at[own_slot, pl.ds(0, ROWS), :], lsem.at[0]),
        pltpu.make_async_copy(v2_hbm, zc.at[own_slot, pl.ds(ROWS, ROWS), :], lsem.at[1]),
        pltpu.make_async_copy(mk_hbm, mi, lsem.at[2]),
    ]
    for cp in own:
        cp.start()
    c_copy = pltpu.make_async_copy(c_hbm, call, lsem.at[3])
    c_copy.start()
    for cp in own:
        cp.wait()
    mrow = mi[...].astype(F32)
    mbuf[own_slot] = jnp.concatenate([mrow, mrow], axis=1)
    pl.semaphore_wait(barrier, len(peers + zpeers))

    def remote(src, dst, ssem, rsem, dev):
        return pltpu.make_async_remote_copy(src_ref=src, dst_ref=dst, send_sem=ssem, recv_sem=rsem,
                                            device_id=(dev,), device_id_type=MESH)

    def wait_in(buf, rsem):
        remote(buf, buf, lsem.at[0], rsem, me).wait_recv()

    def wait_out(buf, ssem):
        remote(buf, buf, ssem, lsem.at[0], me).wait_send()

    def z_copy(i, dev):
        remote(zc.at[i], zc.at[i], z_send.at[0], z_recv.at[i], dev).start()
        remote(mbuf.at[i], mbuf.at[i], z_send.at[1], m_recv.at[i], dev).start()

    def z_core(i, p):
        remote(zc.at[i], zc.at[i], z_send.at[0], zcore_recv.at[p], core).start()
        remote(mbuf.at[i], mbuf.at[i], z_send.at[1], mcore_recv.at[p], core).start()

    def z_wait(i):
        wait_in(zc.at[i], z_recv.at[i])
        wait_in(mbuf.at[i], m_recv.at[i])

    def row_scores(lo, hi):
        def body(i, carry):
            k0 = pl.multiple_of(i * RCOLS, RCOLS)
            rs = lax.dot_general(zc[own_slot], call[pl.ds(k0, RCOLS), :], NT, preferred_element_type=F32)
            q1_ref[:, pl.ds(k0, RCOLS)] = rs[:ROWS]
            q2_ref[:, pl.ds(k0, RCOLS)] = rs[ROWS:]
            return carry

        lax.fori_loop(lo, hi, body, 0)

    z_copy(own_slot, first)
    z_copy(own_slot, second)
    for dev in zpeers:
        z_copy(own_slot, dev)
    z_core(own_slot, z)
    c_copy.wait()
    row_scores(0, ROW_CUTS[0])

    def take(t, k, *devs):
        i = planes[t] * PLANE + c * CHIPS + k // 2
        z_wait(i)
        for dev in devs:
            z_copy(i, dev)
        z_core(i, planes[t])

    def take_z(t):
        take(t, j, *((first,) if t == 1 else (first, second)))

    def take_f(t):
        take(t, jf, *(() if t == 1 else (second,)))

    def take_s(t):
        take(t, js, *((zpart,) if t == 0 else ()))

    def take_d(t):
        take(t, jd, *((zpart,) if t == 0 else ()))

    def take_core(t):
        part = pl.ds(planes[t] * PLANE + (1 - c) * CHIPS, CHIPS)
        wait_in(zc.at[part], zcore_recv.at[planes[t]])
        wait_in(mbuf.at[part], mcore_recv.at[planes[t]])

    def scores(t, k):
        d0 = planes[t] * PLANE + k * CHIPS
        n0 = pl.multiple_of(d0 * ROWS, BLK)

        for v in range(2):
            zb = zc[pl.ds(d0, CHIPS), v * ROWS:(v + 1) * ROWS, :].reshape(BLK, DIM)
            acc = jnp.zeros((8, BLK), F32)
            for k0 in range(0, COLS, MB):
                cs = call[pl.ds(pl.multiple_of(j * COLS + k0, MB), MB), :]
                e = jnp.exp2(lax.dot_general(cs, zb, NT, preferred_element_type=F32) * (INV_T * LOG2E))
                a_ref[v, k0:k0 + MB, pl.ds(n0, BLK)] = e * e
                acc = acc + jnp.sum(e.reshape(MB // 8, 8, BLK), axis=0)
            tot = jnp.sum(acc, axis=0, keepdims=True)
            for b in range(2):
                rbuf[0, v, j, pl.ds(d0 // 2 + b, 1), :] = tot[:, b * LANES:(b + 1) * LANES]

    def own_scores(t):
        scores(t, c)

    def other_scores(t):
        take_core(t)
        scores(t, 1 - c)

    take_f(0)
    take_s(0)
    take_z(1)
    row_scores(ROW_CUTS[0], ROW_CUTS[1])
    take_z(2)
    take_d(0)
    take_z(3)
    take_f(1)
    take_s(1)
    own_scores(0)
    take_f(2)
    take_s(2)
    take_d(1)
    own_scores(1)
    other_scores(0)
    take_f(3)
    take_s(3)
    take_d(2)
    own_scores(2)
    other_scores(1)
    take_d(3)
    own_scores(3)
    other_scores(2)
    other_scores(3)

    def to_plane(buf, ssem, rsem):
        for dev in peers:
            remote(buf, buf, ssem, rsem, dev).start()

    others = pl.ds(0, PLANE - 1)

    def ar_start(ph, v):
        to_plane(rbuf.at[ph, v, j], ar_send.at[0], ar_recv.at[2 * ph + v])

    def ar_wait(ph, v):
        wait_in(rbuf.at[ph, v, others], ar_recv.at[2 * ph + v])
        tot = rbuf[ph, v, 0]
        for o in PEERS:
            tot = tot + rbuf[ph, v, o]
        return tot

    ar_start(0, 0)
    ar_start(0, 1)

    lane = lax.broadcasted_iota(jnp.int32, (1, LANES), 1)
    for b in range(DENSE):
        mden[pl.ds(b, 1), :] = jnp.where(lane < ROWS, mbuf[2 * b], mbuf[2 * b + 1])
    mask = mden[...]
    valid = jnp.sum(jnp.sum(mask, axis=0, keepdims=True), axis=1, keepdims=True)

    def spread(dense, slot, v):
        uden[...] = dense
        for b in range(DENSE):
            ub[slot, v, :, b * LANES:(b + 1) * LANES] = jnp.broadcast_to(uden[pl.ds(b, 1), :], (8, LANES))

    spread(mask, 0, 0)
    spread(mask, 0, 1)

    def sweep(ph, v):
        u = ub[0, v]

        def body(i, acc):
            rows = [pl.multiple_of((i * GRP + g) * 8, 8) for g in range(GRP)]
            for row in rows:
                col = jnp.sum(a_ref[v, pl.ds(row, 8), :] * u, axis=1, keepdims=True)
                vbc[v, pl.ds(row, 8), :] = jnp.broadcast_to(1.0 / (PROTOS * col), (8, LANES))
            for row in rows:
                vg = jnp.concatenate([vbc[v, pl.ds(row, 8), :]] * DENSE, axis=1)
                acc = acc + a_ref[v, pl.ds(row, 8), :] * vg
            return acc

        acc = lax.fori_loop(0, COLS // (8 * GRP), body, jnp.zeros((8, SAMPLES), F32))
        tot = jnp.sum(acc, axis=0, keepdims=True)
        for b in range(DENSE):
            rbuf[ph, v, j, pl.ds(b, 1), :] = tot[:, b * LANES:(b + 1) * LANES]

    def send_v(v):
        diag = (lax.broadcasted_iota(jnp.int32, (LANES, LANES), 0) == lax.broadcasted_iota(jnp.int32, (LANES, LANES), 1))
        for b in range(BLOCKS):
            blk = vbc[v, b * LANES:(b + 1) * LANES, :]
            vall[v, j, :, b * LANES:(b + 1) * LANES] = jnp.sum(jnp.where(diag, blk, 0.0), axis=0, keepdims=True)
        to_plane(vall.at[v, j], ar_send.at[1], v_recv.at[v])

    def diag_scores(lo, hi):
        def body(i, carry):
            n0 = pl.multiple_of(i * BLK, BLK)
            for v in range(2):
                zb = zc[pl.ds(i * CHIPS, CHIPS), v * ROWS:(v + 1) * ROWS, :].reshape(BLK, DIM)
                for k0 in range(0, LOCAL, MB):
                    cs = call[pl.ds(pl.multiple_of(jd * COLS + DIAG * UNIT + k0, MB), MB), :]
                    e = jnp.exp2(lax.dot_general(cs, zb, NT, preferred_element_type=F32) * (INV_T * LOG2E))
                    ad_ref[v, k0:k0 + MB, pl.ds(n0, BLK)] = e * e
            return carry

        lax.fori_loop(lo, hi, body, 0)

    for it in range(ITERS):
        for v in range(2):
            if it > 0:
                spread(mask / (valid * ar_wait(it, v)), 0, v)
            sweep(it + 1, v)
            ar_start(it + 1, v)
            if it == ITERS - 1:
                send_v(v)
        row_scores(ROW_CUTS[it + 1], ROW_CUTS[it + 2])
        diag_scores(DIAG_CUTS[it], DIAG_CUTS[it + 1])

    gam = mask / (valid * 0.2)
    soft = [ar_wait(0, v) for v in range(2)]
    for v in range(2):
        spread(gam / soft[v], 1, v)

    def unit_of(w):
        return w + par * (UNITS - 1 - 2 * w)

    def unit_ref(q, u):
        return dc_ref.at[pl.ds(pl.multiple_of(q * COLS + u * UNIT, UNIT), UNIT), :]

    def d_copy(q, u, ssem, rsem, dev):
        return remote(unit_ref(q, u), unit_ref(q, u), ssem, rsem, dev)

    def d_core(q, u):
        return d_copy(q, u, d_send.at[0], v_recv.at[2], core)

    def d_wait(q, s, u):
        wait_in(unit_ref(q, u), d_recv.at[s, u])

    def grad_part(a_buf, v_buf, k0, size, v, acc):
        k0 = pl.multiple_of(k0, size)
        o = 1 - v

        wide = KDEPTH // BLK
        devs = KDEPTH // ROWS

        def body(i, acc):
            n0 = pl.multiple_of(i * KDEPTH, KDEPTH)
            a = a_buf[v, pl.ds(k0, size), pl.ds(n0, KDEPTH)].reshape(size // 8, 8, KDEPTH)
            ao = a_buf[o, pl.ds(k0, size), pl.ds(n0, KDEPTH)].reshape(size // 8, 8, KDEPTH)
            vo = jnp.concatenate([v_buf[o, pl.ds(k0, size), :]] * (2 * wide), axis=1).reshape(size // 8, 8, KDEPTH)
            g = (a * lax.rsqrt(a)) * ub[1, v, :, pl.ds(n0, KDEPTH)][None] - (ao * vo) * ub[0, o, :, pl.ds(n0, KDEPTH)][None]
            zb = zc[pl.ds(i * devs, devs), v * ROWS:(v + 1) * ROWS, :].reshape(KDEPTH, DIM)
            return acc + jnp.dot(g.reshape(size, KDEPTH).astype(BF16), zb, preferred_element_type=F32)

        return lax.fori_loop(0, SAMPLES // KDEPTH, body, acc)

    def grad_first(k0, size):
        return grad_part(a_ref, vbc, k0, size, 1, jnp.zeros((size, DIM), F32))

    def grad_rest(k0, size, acc):
        acc = grad_part(a_ref, vbc, k0, size, 0, acc)
        dc_ref[pl.ds(pl.multiple_of(j * COLS + k0, size), size), :] = acc

    def diag_units(b):
        k0 = b * LANES
        acc = jnp.zeros((LANES, DIM), F32)
        for v in (1, 0):
            acc = grad_part(ad_ref, vd, k0, LANES, v, acc)
        dc_ref[pl.ds(pl.multiple_of(jd * COLS + DIAG * UNIT + k0, LANES), LANES), :] = acc
        for u in range(2):
            d_core(jd, DIAG + 2 * b + u).start()

    def send_own(w):
        u = unit_of(w)
        if w < FIRST:
            d_copy(j, u, d_send.at[1], d_recv.at[0, u], first).start()
        d_core(j, u).start()

    def send_second(w):
        u = unit_of(w)
        d_copy(j, u, d_send.at[2], d_recv.at[1, u], second).start()

    def take_unit(q, s, w, direct):
        u = unit_of(w)
        d_wait(q, s, u)
        if s == 0 and w < DIAG:
            d_copy(q, u, d_send.at[3], d_recv.at[2, u], second).start()
        if w < UNITS - direct:
            d_copy(q, u, d_send.at[4], d_recv.at[s, u], zpart).start()
        d_core(q, u).start()

    def take_first(w):
        take_unit(jf, 0, w, FIRST)
        if w + LAG < SECOND:
            send_second(w + LAG)

    def take_second(w):
        take_unit(js, 1, w, SECOND)

    def take_diag(w):
        take_unit(jd, 2, w, UNITS - DIAG)

    def own_units(b):
        k0 = (b + par * (BLOCKS - 1 - 2 * b)) * LANES
        grad_rest(k0, LANES, grad_first(k0, LANES))
        send_own(2 * b)
        send_own(2 * b + 1)

    mu = [mask / ar_wait(ITERS, 0)]
    spread(mu[0] * gam, 0, 0)
    parts = [grad_first(unit_of(w) * UNIT, UNIT) for w in range(2)]
    mu.append(mask / ar_wait(ITERS, 1))
    spread(mu[1] * gam, 0, 1)
    for w in range(2):
        grad_rest(unit_of(w) * UNIT, UNIT, parts[w])
        send_own(w)
        send_second(w)
    own_units(1)
    send_second(2)
    own_units(2)

    sub = lax.broadcasted_iota(jnp.int32, (ROWS, LANES), 0)
    pick = lax.broadcasted_iota(jnp.int32, (ROWS, LANES), 1) == sub + ROWS * (own_slot % 2)

    def own_rows(dense):
        uden[...] = dense
        row = jnp.broadcast_to(uden[pl.ds(own_slot // 2, 1), :], (ROWS, LANES))
        return jnp.sum(jnp.where(pick, row, 0.0), axis=1, keepdims=True)

    gm = own_rows(gam)
    mus = [own_rows(mu[v]) for v in range(2)]
    ps = [own_rows(soft[v]) for v in range(2)]
    ips = [1.0 / p for p in ps]
    lps = [jnp.log(p) for p in ps]
    for v in range(2):
        wait_in(vall.at[v, others], v_recv.at[v])
    eye = lax.broadcasted_iota(jnp.int32, (LANES, LANES), 0) == lax.broadcasted_iota(jnp.int32, (LANES, LANES), 1)
    for v in range(2):
        for k0 in range(0, LOCAL, LANES):
            row = jnp.broadcast_to(vall[v, jd, :, DIAG * UNIT + k0:DIAG * UNIT + k0 + LANES], (LANES, LANES))
            col = jnp.sum(jnp.where(eye, row, 0.0), axis=1, keepdims=True)
            vd[v, k0:k0 + LANES, :] = jnp.broadcast_to(col, (LANES, LANES))
    q_refs = (q1_ref, q2_ref)
    chunks = COLS // QCOLS

    def row_body(i, carry):
        dz, lacc = carry
        k0 = pl.multiple_of(i * QCOLS, QCOLS)
        l0 = pl.multiple_of((i % chunks) * QCOLS, QCOLS)
        ss, es, qs, gs = [], [], [], []
        for v in range(2):
            ss.append(q_refs[v][:, pl.ds(k0, QCOLS)] * INV_T)
            es.append(jnp.exp2(ss[v] * LOG2E))
            qs.append((es[v] * es[v]) * mus[v] * vall[v, i // chunks, :, pl.ds(l0, QCOLS)])
            q_refs[v][:, pl.ds(k0, QCOLS)] = qs[v]
        for v in range(2):
            lsum = qs[1 - v] * (ss[v] - lps[v])
            lacc = lacc + jnp.sum(lsum.reshape(ROWS // 8, 8, QCOLS), axis=0)
            gs.append((es[v] * ips[v] - qs[1 - v]) * gm)
        g = jnp.concatenate(gs, axis=0).astype(BF16)
        return dz + jnp.dot(g, call[pl.ds(k0, QCOLS), :], preferred_element_type=F32), lacc

    carry = (jnp.zeros((SLAB, DIM), F32), jnp.zeros((8, QCOLS), F32))
    cuts = (0, 4, 7, 10, 13, PROTOS // QCOLS)

    def row_part(i, carry):
        return lax.fori_loop(cuts[i], cuts[i + 1], row_body, carry)

    carry = row_part(0, carry)
    take_first(0)
    take_second(0)
    carry = row_part(1, carry)
    take_first(1)
    take_second(1)
    own_units(3)
    take_first(2)
    take_second(2)
    carry = row_part(2, carry)
    take_first(3)
    take_diag(0)
    carry = row_part(3, carry)
    take_first(4)
    take_second(3)
    dz, lacc = row_part(4, carry)
    dz1_ref[...] = dz[:ROWS]
    dz2_ref[...] = dz[ROWS:]
    lpart = jnp.sum(jnp.sum(lacc, axis=0, keepdims=True), axis=1, keepdims=True)
    lbuf[j] = jnp.broadcast_to(lpart, (8, LANES))
    to_plane(lbuf.at[j], ar_send.at[2], l_recv.at[0])
    own_units(4)
    take_first(5)
    take_diag(1)
    take_first(6)
    take_second(4)
    own_units(5)
    take_first(7)
    take_diag(2)
    diag_units(0)
    take_first(8)
    take_second(5)
    diag_units(1)
    take_first(9)
    take_diag(3)
    diag_units(2)
    take_first(10)
    take_second(6)

    wait_in(lbuf.at[others], l_recv.at[0])
    lsum = lbuf[0]
    for o in PEERS:
        lsum = lsum + lbuf[o]
    lzbuf[z] = lsum
    for dev in zpeers:
        remote(lzbuf.at[z], lzbuf.at[z], ar_send.at[3], l_recv.at[1], dev).start()

    diag_units(3)
    take_first(11)
    take_second(7)
    own_units(6)
    take_second(8)
    take_second(9)
    own_units(7)
    take_second(10)
    for w in reversed(range(SECOND, UNITS)):
        for s, q, direct in ((0, jf, FIRST), (1, js, SECOND), (2, jd, UNITS - DIAG)):
            if w >= direct:
                u = unit_of(w)
                d_wait(q, s, u)
                d_core(q, u).start()

    other_planes = pl.ds(0, PLANES - 1)
    wait_in(lzbuf.at[other_planes], l_recv.at[1])
    loss = lzbuf[0]
    for o in range(1, PLANES):
        loss = loss + lzbuf[o]
    loss_ref[...] = (-loss / (2.0 * valid))[:1, :1]

    wait_in(dc_ref.at[pl.ds(0, PROTOS // 2), :], v_recv.at[2])
    sent = pl.ds(0, DEVS - 1)
    wait_out(zc.at[sent], z_send.at[0])
    wait_out(mbuf.at[sent], z_send.at[1])
    wait_out(rbuf.at[:, :, others], ar_send.at[0])
    wait_out(vall.at[:, others], ar_send.at[1])
    wait_out(lbuf.at[others], ar_send.at[2])
    wait_out(lzbuf.at[other_planes], ar_send.at[3])
    counts = (4 * UNITS, FIRST, SECOND, DIAG, 2 * UNITS - FIRST - SECOND + DIAG)
    for k, units in enumerate(counts):
        wait_out(dc_ref.at[pl.ds(0, units * UNIT), :], d_send.at[k])


STORE = (4, 4, 1, 1, 1, 8)


def store_kernel(*refs):
    results = len(STORE)
    sem = refs[2 * results]
    copies = []
    for i, pieces in enumerate(STORE):
        src, dst = refs[i], refs[results + i]
        rows = src.shape[0] // pieces
        for p in range(pieces):
            part = pl.ds(p * rows, rows)
            copies.append(pltpu.make_async_copy(src.at[part, :], dst.at[part, :], sem.at[len(copies)]))
            copies[-1].start()
    for cp in copies:
        cp.wait()


def solution(mesh):
    def local_step(view_one, view_two, protos, valid_mask):
        dma = pltpu.SemaphoreType.DMA
        outs = pl.pallas_call(
            kernel,
            out_shape=[
                pltpu.VMEM((ROWS, PROTOS), F32),
                pltpu.VMEM((ROWS, PROTOS), F32),
                pltpu.VMEM((1, 1), F32),
                pltpu.VMEM((ROWS, DIM), F32),
                pltpu.VMEM((ROWS, DIM), F32),
                pltpu.VMEM((PROTOS, DIM), F32),
            ],
            in_specs=[pl.BlockSpec(memory_space=pl.ANY)] * 4,
            out_specs=[pl.BlockSpec(memory_space=pltpu.VMEM)] * 6,
            scratch_shapes=[
                pltpu.VMEM((DEVS, SLAB, DIM), BF16),
                pltpu.VMEM((1, ROWS), jnp.int32),
                pltpu.VMEM((DEVS, 1, LANES), F32),
                pltpu.VMEM((PROTOS, DIM), BF16),
                pltpu.VMEM((2, COLS, SAMPLES), F32),
                pltpu.VMEM((2, LOCAL, SAMPLES), F32),
                pltpu.VMEM((2, COLS, LANES), F32),
                pltpu.VMEM((2, LOCAL, LANES), F32),
                pltpu.VMEM((DENSE, LANES), F32),
                pltpu.VMEM((DENSE, LANES), F32),
                pltpu.VMEM((2, 2, 8, SAMPLES), F32),
                pltpu.VMEM((ITERS + 1, 2, PLANE, DENSE, LANES), F32),
                pltpu.VMEM((2, PLANE, 1, COLS), F32),
                pltpu.VMEM((PLANE, 8, LANES), F32),
                pltpu.VMEM((PLANES, 8, LANES), F32),
                dma((4,)), dma((2,)), dma((DEVS,)), dma((PLANES,)), dma((DEVS,)), dma((PLANES,)),
                dma((4,)), dma((2 * ITERS + 2,)), dma((3,)), dma((2,)), dma((3, UNITS)), dma((5,)),
            ],
            compiler_params=pltpu.CompilerParams(
                collective_id=0, has_side_effects=True, vmem_limit_bytes=48 << 20),
        )(view_one, view_two, valid_mask.reshape(1, ROWS), protos)
        outs = pl.pallas_call(
            store_kernel,
            out_shape=[jax.ShapeDtypeStruct(o.shape, o.dtype) for o in outs],
            in_specs=[pl.BlockSpec(memory_space=pltpu.VMEM)] * len(STORE),
            out_specs=[pl.BlockSpec(memory_space=pl.ANY)] * len(STORE),
            scratch_shapes=[dma((sum(STORE),))],
            compiler_params=pltpu.CompilerParams(vmem_limit_bytes=4 << 20),
        )(*[pltpu.with_memory_space_constraint(o, pltpu.VMEM) for o in outs])
        q1, q2, loss, dz1, dz2, dc = outs
        return q1, q2, loss.reshape(()), dz1, dz2, dc

    return jax.shard_map(
        local_step,
        mesh=mesh,
        in_specs=(P("data", None), P("data", None), P(None, None), P("data")),
        out_specs=(P("data", None), P("data", None), P(), P("data", None), P("data", None), P(None, None)),
        check_vma=False,
    )
```

```python
import jax
import jax.numpy as jnp
from jax import lax
from jax.experimental import pallas as pl
from jax.experimental.pallas import tpu as pltpu
from jax.sharding import PartitionSpec as P

MESH = pl.DeviceIdType.MESH
F32 = jnp.float32
BF16 = jnp.bfloat16

ROWS = 64
SLAB = 2 * ROWS
DEVS = 32
PLANE = 8
SAMPLES = ROWS * DEVS
MB = 256
PROTOS = 8192
DIM = 256
COLS = PROTOS // PLANE
ITERS = 3
LANES = 128
PLANES = DEVS // PLANE
CHIPS = PLANE // 2
PEERS = range(1, PLANE)
BLK = 2 * LANES
DENSE = SAMPLES // LANES
INV_T = 10.0
UNIT = 64
UNITS = COLS // UNIT
BLOCKS = COLS // LANES
FIRST = 12
SECOND = 12
DIAG = 4
LOCAL = COLS - 2 * DIAG * UNIT
KDEPTH = 1024
RCOLS = 1024
LAG = 3
QCOLS = 512
GRP = 32
LOG2E = 1.4426950408889634
ROW_CUTS = (1, 3, 5, 7, 8)
DIAG_CUTS = (0, 4, 5, 8)
NT = (((1,), (1,)), ((), ()))


def kernel(v1_hbm, v2_hbm, mk_hbm, c_hbm,
           q1_ref, q2_ref, loss_ref, dz1_ref, dz2_ref, dc_ref,
           zc, mi, mbuf, call, a_ref, ad_ref, vbc, vd, mden, uden, ub, rbuf, vall, lbuf, lzbuf,
           lsem, z_send, z_recv, zcore_recv, m_recv, mcore_recv, ar_send, ar_recv, v_recv, l_recv, d_recv, d_send):
    me = lax.axis_index("data")
    z = me // PLANE
    j = me % PLANE
    c = j % 2
    x = (j // 2) % 2
    y = j // 4
    jx = j + 2 - 4 * x
    jy = j + 4 - 8 * y
    jd = (6 - 2 * (j // 2)) + c
    jf = jx + c * (jy - jx)
    js = jy + c * (jx - jy)
    core = me + 1 - 2 * c
    own_slot = z * PLANE + c * CHIPS + j // 2
    first = z * PLANE + jf
    second = z * PLANE + js
    par = z % 2
    planes = (z, z + 1 - 2 * par, z + 2 - PLANES * (z // 2), PLANES - 1 - z)
    zpart = planes[1] * PLANE + j
    peers = [z * PLANE + (j + t) % PLANE for t in PEERS]
    zpeers = [p * PLANE + j for p in planes[1:]]

    barrier = pltpu.get_barrier_semaphore()
    for dev in peers + zpeers:
        pl.semaphore_signal(barrier, inc=1, device_id=(dev,), device_id_type=MESH)

    own = [
        pltpu.make_async_copy(v1_hbm, zc.at[own_slot, pl.ds(0, ROWS), :], lsem.at[0]),
        pltpu.make_async_copy(v2_hbm, zc.at[own_slot, pl.ds(ROWS, ROWS), :], lsem.at[1]),
        pltpu.make_async_copy(mk_hbm, mi, lsem.at[2]),
    ]
    for cp in own:
        cp.start()
    c_copy = pltpu.make_async_copy(c_hbm, call, lsem.at[3])
    c_copy.start()
    for cp in own:
        cp.wait()
    mrow = mi[...].astype(F32)
    mbuf[own_slot] = jnp.concatenate([mrow, mrow], axis=1)
    pl.semaphore_wait(barrier, len(peers + zpeers))

    def remote(src, dst, ssem, rsem, dev):
        return pltpu.make_async_remote_copy(src_ref=src, dst_ref=dst, send_sem=ssem, recv_sem=rsem,
                                            device_id=(dev,), device_id_type=MESH)

    def wait_in(buf, rsem):
        remote(buf, buf, lsem.at[0], rsem, me).wait_recv()

    def wait_out(buf, ssem):
        remote(buf, buf, ssem, lsem.at[0], me).wait_send()

    def z_copy(i, dev):
        remote(zc.at[i], zc.at[i], z_send.at[0], z_recv.at[i], dev).start()
        remote(mbuf.at[i], mbuf.at[i], z_send.at[1], m_recv.at[i], dev).start()

    def z_core(i, p):
        remote(zc.at[i], zc.at[i], z_send.at[0], zcore_recv.at[p], core).start()
        remote(mbuf.at[i], mbuf.at[i], z_send.at[1], mcore_recv.at[p], core).start()

    def z_wait(i):
        wait_in(zc.at[i], z_recv.at[i])
        wait_in(mbuf.at[i], m_recv.at[i])

    def row_scores(lo, hi):
        def body(i, carry):
            k0 = pl.multiple_of(i * RCOLS, RCOLS)
            rs = lax.dot_general(zc[own_slot], call[pl.ds(k0, RCOLS), :], NT, preferred_element_type=F32)
            q1_ref[:, pl.ds(k0, RCOLS)] = rs[:ROWS]
            q2_ref[:, pl.ds(k0, RCOLS)] = rs[ROWS:]
            return carry

        lax.fori_loop(lo, hi, body, 0)

    z_copy(own_slot, first)
    z_copy(own_slot, second)
    for dev in zpeers:
        z_copy(own_slot, dev)
    z_core(own_slot, z)
    c_copy.wait()
    row_scores(0, ROW_CUTS[0])

    def take(t, k, *devs):
        i = planes[t] * PLANE + c * CHIPS + k // 2
        z_wait(i)
        for dev in devs:
            z_copy(i, dev)
        z_core(i, planes[t])

    def take_z(t):
        take(t, j, *((first,) if t == 1 else (first, second)))

    def take_f(t):
        take(t, jf, *(() if t == 1 else (second,)))

    def take_s(t):
        take(t, js, *((zpart,) if t == 0 else ()))

    def take_d(t):
        take(t, jd, *((zpart,) if t == 0 else ()))

    def take_core(t):
        part = pl.ds(planes[t] * PLANE + (1 - c) * CHIPS, CHIPS)
        wait_in(zc.at[part], zcore_recv.at[planes[t]])
        wait_in(mbuf.at[part], mcore_recv.at[planes[t]])

    def scores(t, k):
        d0 = planes[t] * PLANE + k * CHIPS
        n0 = pl.multiple_of(d0 * ROWS, BLK)

        for v in range(2):
            zb = zc[pl.ds(d0, CHIPS), v * ROWS:(v + 1) * ROWS, :].reshape(BLK, DIM)
            acc = jnp.zeros((8, BLK), F32)
            for k0 in range(0, COLS, MB):
                cs = call[pl.ds(pl.multiple_of(j * COLS + k0, MB), MB), :]
                e = jnp.exp2(lax.dot_general(cs, zb, NT, preferred_element_type=F32) * (INV_T * LOG2E))
                a_ref[v, k0:k0 + MB, pl.ds(n0, BLK)] = e * e
                acc = acc + jnp.sum(e.reshape(MB // 8, 8, BLK), axis=0)
            tot = jnp.sum(acc, axis=0, keepdims=True)
            for b in range(2):
                rbuf[0, v, j, pl.ds(d0 // 2 + b, 1), :] = tot[:, b * LANES:(b + 1) * LANES]

    def own_scores(t):
        scores(t, c)

    def other_scores(t):
        take_core(t)
        scores(t, 1 - c)

    take_f(0)
    take_s(0)
    take_z(1)
    row_scores(ROW_CUTS[0], ROW_CUTS[1])
    take_z(2)
    take_d(0)
    take_z(3)
    take_f(1)
    take_s(1)
    own_scores(0)
    take_f(2)
    take_s(2)
    take_d(1)
    own_scores(1)
    other_scores(0)
    take_f(3)
    take_s(3)
    take_d(2)
    own_scores(2)
    other_scores(1)
    take_d(3)
    own_scores(3)
    other_scores(2)
    other_scores(3)

    def to_plane(buf, ssem, rsem):
        for dev in peers:
            remote(buf, buf, ssem, rsem, dev).start()

    others = pl.ds(0, PLANE - 1)

    def ar_start(ph, v):
        to_plane(rbuf.at[ph, v, j], ar_send.at[0], ar_recv.at[2 * ph + v])

    def ar_wait(ph, v):
        wait_in(rbuf.at[ph, v, others], ar_recv.at[2 * ph + v])
        tot = rbuf[ph, v, 0]
        for o in PEERS:
            tot = tot + rbuf[ph, v, o]
        return tot

    ar_start(0, 0)
    ar_start(0, 1)

    lane = lax.broadcasted_iota(jnp.int32, (1, LANES), 1)
    for b in range(DENSE):
        mden[pl.ds(b, 1), :] = jnp.where(lane < ROWS, mbuf[2 * b], mbuf[2 * b + 1])
    mask = mden[...]
    valid = jnp.sum(jnp.sum(mask, axis=0, keepdims=True), axis=1, keepdims=True)

    def spread(dense, slot, v):
        uden[...] = dense
        for b in range(DENSE):
            ub[slot, v, :, b * LANES:(b + 1) * LANES] = jnp.broadcast_to(uden[pl.ds(b, 1), :], (8, LANES))

    spread(mask, 0, 0)
    spread(mask, 0, 1)

    def sweep(ph, v):
        u = ub[0, v]

        def body(i, acc):
            rows = [pl.multiple_of((i * GRP + g) * 8, 8) for g in range(GRP)]
            for row in rows:
                col = jnp.sum(a_ref[v, pl.ds(row, 8), :] * u, axis=1, keepdims=True)
                vbc[v, pl.ds(row, 8), :] = jnp.broadcast_to(1.0 / (PROTOS * col), (8, LANES))
            for row in rows:
                vg = jnp.concatenate([vbc[v, pl.ds(row, 8), :]] * DENSE, axis=1)
                acc = acc + a_ref[v, pl.ds(row, 8), :] * vg
            return acc

        acc = lax.fori_loop(0, COLS // (8 * GRP), body, jnp.zeros((8, SAMPLES), F32))
        tot = jnp.sum(acc, axis=0, keepdims=True)
        for b in range(DENSE):
            rbuf[ph, v, j, pl.ds(b, 1), :] = tot[:, b * LANES:(b + 1) * LANES]

    def send_v(v):
        diag = (lax.broadcasted_iota(jnp.int32, (LANES, LANES), 0) == lax.broadcasted_iota(jnp.int32, (LANES, LANES), 1))
        for b in range(BLOCKS):
            blk = vbc[v, b * LANES:(b + 1) * LANES, :]
            vall[v, j, :, b * LANES:(b + 1) * LANES] = jnp.sum(jnp.where(diag, blk, 0.0), axis=0, keepdims=True)
        to_plane(vall.at[v, j], ar_send.at[1], v_recv.at[v])

    def diag_scores(lo, hi):
        def body(i, carry):
            n0 = pl.multiple_of(i * BLK, BLK)
            for v in range(2):
                zb = zc[pl.ds(i * CHIPS, CHIPS), v * ROWS:(v + 1) * ROWS, :].reshape(BLK, DIM)
                for k0 in range(0, LOCAL, MB):
                    cs = call[pl.ds(pl.multiple_of(jd * COLS + DIAG * UNIT + k0, MB), MB), :]
                    e = jnp.exp2(lax.dot_general(cs, zb, NT, preferred_element_type=F32) * (INV_T * LOG2E))
                    ad_ref[v, k0:k0 + MB, pl.ds(n0, BLK)] = e * e
            return carry

        lax.fori_loop(lo, hi, body, 0)

    for it in range(ITERS):
        for v in range(2):
            if it > 0:
                spread(mask / (valid * ar_wait(it, v)), 0, v)
            sweep(it + 1, v)
            ar_start(it + 1, v)
            if it == ITERS - 1:
                send_v(v)
        row_scores(ROW_CUTS[it + 1], ROW_CUTS[it + 2])
        diag_scores(DIAG_CUTS[it], DIAG_CUTS[it + 1])

    gam = mask / (valid * 0.2)
    soft = [ar_wait(0, v) for v in range(2)]
    for v in range(2):
        spread(gam / soft[v], 1, v)

    def unit_of(w):
        return w + par * (UNITS - 1 - 2 * w)

    def unit_ref(q, u):
        return dc_ref.at[pl.ds(pl.multiple_of(q * COLS + u * UNIT, UNIT), UNIT), :]

    def d_copy(q, u, ssem, rsem, dev):
        return remote(unit_ref(q, u), unit_ref(q, u), ssem, rsem, dev)

    def d_core(q, u):
        return d_copy(q, u, d_send.at[0], v_recv.at[2], core)

    def d_wait(q, s, u):
        wait_in(unit_ref(q, u), d_recv.at[s, u])

    def grad_part(a_buf, v_buf, k0, size, v, acc):
        k0 = pl.multiple_of(k0, size)
        o = 1 - v

        wide = KDEPTH // BLK
        devs = KDEPTH // ROWS

        def body(i, acc):
            n0 = pl.multiple_of(i * KDEPTH, KDEPTH)
            a = a_buf[v, pl.ds(k0, size), pl.ds(n0, KDEPTH)].reshape(size // 8, 8, KDEPTH)
            ao = a_buf[o, pl.ds(k0, size), pl.ds(n0, KDEPTH)].reshape(size // 8, 8, KDEPTH)
            vo = jnp.concatenate([v_buf[o, pl.ds(k0, size), :]] * (2 * wide), axis=1).reshape(size // 8, 8, KDEPTH)
            g = (a * lax.rsqrt(a)) * ub[1, v, :, pl.ds(n0, KDEPTH)][None] - (ao * vo) * ub[0, o, :, pl.ds(n0, KDEPTH)][None]
            zb = zc[pl.ds(i * devs, devs), v * ROWS:(v + 1) * ROWS, :].reshape(KDEPTH, DIM)
            return acc + jnp.dot(g.reshape(size, KDEPTH).astype(BF16), zb, preferred_element_type=F32)

        return lax.fori_loop(0, SAMPLES // KDEPTH, body, acc)

    def grad_first(k0, size):
        return grad_part(a_ref, vbc, k0, size, 1, jnp.zeros((size, DIM), F32))

    def grad_rest(k0, size, acc):
        acc = grad_part(a_ref, vbc, k0, size, 0, acc)
        dc_ref[pl.ds(pl.multiple_of(j * COLS + k0, size), size), :] = acc

    def diag_units(k0, size):
        acc = jnp.zeros((size, DIM), F32)
        for v in (1, 0):
            acc = grad_part(ad_ref, vd, k0, size, v, acc)
        dc_ref[pl.ds(pl.multiple_of(jd * COLS + DIAG * UNIT + k0, LANES), size), :] = acc
        for u in range(DIAG + k0 // UNIT, DIAG + (k0 + size) // UNIT):
            d_core(jd, u).start()

    def send_own(w):
        u = unit_of(w)
        if w < FIRST:
            d_copy(j, u, d_send.at[1], d_recv.at[0, u], first).start()
        d_core(j, u).start()

    def send_second(w):
        u = unit_of(w)
        d_copy(j, u, d_send.at[2], d_recv.at[1, u], second).start()

    def take_unit(q, s, w, direct):
        u = unit_of(w)
        d_wait(q, s, u)
        if s == 0 and w < DIAG:
            d_copy(q, u, d_send.at[3], d_recv.at[2, u], second).start()
        if w < UNITS - direct:
            d_copy(q, u, d_send.at[4], d_recv.at[s, u], zpart).start()
        d_core(q, u).start()

    def take_first(w):
        take_unit(jf, 0, w, FIRST)
        if w + LAG < SECOND:
            send_second(w + LAG)

    def take_second(w):
        take_unit(js, 1, w, SECOND)

    def take_diag(w):
        take_unit(jd, 2, w, UNITS - DIAG)

    def own_units(w, units):
        size = units * UNIT
        k0 = (w + par * (UNITS - units - 2 * w)) * UNIT
        grad_rest(k0, size, grad_first(k0, size))
        for i in range(units):
            send_own(w + i)

    mu = [mask / ar_wait(ITERS, 0)]
    spread(mu[0] * gam, 0, 0)
    parts = [grad_first(unit_of(w) * UNIT, UNIT) for w in range(2)]
    mu.append(mask / ar_wait(ITERS, 1))
    spread(mu[1] * gam, 0, 1)
    for w in range(2):
        grad_rest(unit_of(w) * UNIT, UNIT, parts[w])
        send_own(w)
        send_second(w)
    own_units(2, 2)
    send_second(2)
    own_units(4, 2)
    take_first(0)
    take_second(0)

    sub = lax.broadcasted_iota(jnp.int32, (ROWS, LANES), 0)
    pick = lax.broadcasted_iota(jnp.int32, (ROWS, LANES), 1) == sub + ROWS * (own_slot % 2)

    def own_rows(dense):
        uden[...] = dense
        row = jnp.broadcast_to(uden[pl.ds(own_slot // 2, 1), :], (ROWS, LANES))
        return jnp.sum(jnp.where(pick, row, 0.0), axis=1, keepdims=True)

    gm = own_rows(gam)
    mus = [own_rows(mu[v]) for v in range(2)]
    ps = [own_rows(soft[v]) for v in range(2)]
    ips = [1.0 / p for p in ps]
    lps = [jnp.log(p) for p in ps]
    for v in range(2):
        wait_in(vall.at[v, others], v_recv.at[v])
    eye = lax.broadcasted_iota(jnp.int32, (LANES, LANES), 0) == lax.broadcasted_iota(jnp.int32, (LANES, LANES), 1)
    for v in range(2):
        for k0 in range(0, LOCAL, LANES):
            row = jnp.broadcast_to(vall[v, jd, :, DIAG * UNIT + k0:DIAG * UNIT + k0 + LANES], (LANES, LANES))
            col = jnp.sum(jnp.where(eye, row, 0.0), axis=1, keepdims=True)
            vd[v, k0:k0 + LANES, :] = jnp.broadcast_to(col, (LANES, LANES))
    q_refs = (q1_ref, q2_ref)
    chunks = COLS // QCOLS

    def row_body(i, carry):
        dz, lacc = carry
        k0 = pl.multiple_of(i * QCOLS, QCOLS)
        l0 = pl.multiple_of((i % chunks) * QCOLS, QCOLS)
        ss, es, qs, gs = [], [], [], []
        for v in range(2):
            ss.append(q_refs[v][:, pl.ds(k0, QCOLS)] * INV_T)
            es.append(jnp.exp2(ss[v] * LOG2E))
            qs.append((es[v] * es[v]) * mus[v] * vall[v, i // chunks, :, pl.ds(l0, QCOLS)])
            q_refs[v][:, pl.ds(k0, QCOLS)] = qs[v]
        for v in range(2):
            lsum = qs[1 - v] * (ss[v] - lps[v])
            lacc = lacc + jnp.sum(lsum.reshape(ROWS // 8, 8, QCOLS), axis=0)
            gs.append((es[v] * ips[v] - qs[1 - v]) * gm)
        g = jnp.concatenate(gs, axis=0).astype(BF16)
        return dz + jnp.dot(g, call[pl.ds(k0, QCOLS), :], preferred_element_type=F32), lacc

    carry = (jnp.zeros((SLAB, DIM), F32), jnp.zeros((8, QCOLS), F32))
    cuts = (0, 4, 7, 10, 13, PROTOS // QCOLS)

    def row_part(i, carry):
        return lax.fori_loop(cuts[i], cuts[i + 1], row_body, carry)

    carry = row_part(0, carry)
    carry = row_part(1, carry)
    take_first(1)
    take_second(1)
    own_units(6, 2)
    take_first(2)
    take_second(2)
    carry = row_part(2, carry)
    take_first(3)
    take_diag(0)
    carry = row_part(3, carry)
    take_first(4)
    take_second(3)
    dz, lacc = row_part(4, carry)
    dz1_ref[...] = dz[:ROWS]
    dz2_ref[...] = dz[ROWS:]
    lpart = jnp.sum(jnp.sum(lacc, axis=0, keepdims=True), axis=1, keepdims=True)
    lbuf[j] = jnp.broadcast_to(lpart, (8, LANES))
    to_plane(lbuf.at[j], ar_send.at[2], l_recv.at[0])
    own_units(8, 2)
    take_first(5)
    take_diag(1)
    take_first(6)
    take_second(4)
    own_units(10, 2)
    take_first(7)
    take_diag(2)
    diag_units(0, LOCAL // 2)
    take_first(8)
    take_second(5)
    take_first(9)
    take_diag(3)
    diag_units(LOCAL // 2, LOCAL // 2)
    take_first(10)
    take_second(6)
    take_first(11)
    take_second(7)

    wait_in(lbuf.at[others], l_recv.at[0])
    lsum = lbuf[0]
    for o in PEERS:
        lsum = lsum + lbuf[o]
    lzbuf[z] = lsum
    for dev in zpeers:
        remote(lzbuf.at[z], lzbuf.at[z], ar_send.at[3], l_recv.at[1], dev).start()

    own_units(12, 4)
    take_second(8)
    take_second(9)
    take_second(10)
    take_second(11)
    for w in reversed(range(SECOND, UNITS)):
        for s, q, direct in ((0, jf, FIRST), (1, js, SECOND), (2, jd, UNITS - DIAG)):
            if w >= direct:
                u = unit_of(w)
                d_wait(q, s, u)
                d_core(q, u).start()

    other_planes = pl.ds(0, PLANES - 1)
    wait_in(lzbuf.at[other_planes], l_recv.at[1])
    loss = lzbuf[0]
    for o in range(1, PLANES):
        loss = loss + lzbuf[o]
    loss_ref[...] = -loss / (2.0 * valid)

    wait_in(dc_ref.at[pl.ds(0, PROTOS // 2), :], v_recv.at[2])
    sent = pl.ds(0, DEVS - 1)
    wait_out(zc.at[sent], z_send.at[0])
    wait_out(mbuf.at[sent], z_send.at[1])
    wait_out(rbuf.at[:, :, others], ar_send.at[0])
    wait_out(vall.at[:, others], ar_send.at[1])
    wait_out(lbuf.at[others], ar_send.at[2])
    wait_out(lzbuf.at[other_planes], ar_send.at[3])
    counts = (4 * UNITS, FIRST, SECOND, DIAG, 2 * UNITS - FIRST - SECOND + DIAG)
    for k, units in enumerate(counts):
        wait_out(dc_ref.at[pl.ds(0, units * UNIT), :], d_send.at[k])


STORE = (4, 4, 1, 1, 1, 8)


def store_kernel(*refs):
    results = len(STORE)
    one, sem = refs[2 * results:]
    copies = []
    for i, pieces in enumerate(STORE):
        src, dst = refs[i], refs[results + i]
        if dst.shape == one.shape:
            one[...] = src[:1, :1]
            src = one
        rows = src.shape[0] // pieces
        for p in range(pieces):
            part = pl.ds(p * rows, rows)
            copies.append(pltpu.make_async_copy(src.at[part, :], dst.at[part, :], sem.at[len(copies)]))
            copies[-1].start()
    for cp in copies:
        cp.wait()


def solution(mesh):
    def local_step(view_one, view_two, protos, valid_mask):
        dma = pltpu.SemaphoreType.DMA
        outs = pl.pallas_call(
            kernel,
            out_shape=[
                pltpu.VMEM((ROWS, PROTOS), F32),
                pltpu.VMEM((ROWS, PROTOS), F32),
                pltpu.VMEM((8, LANES), F32),
                pltpu.VMEM((ROWS, DIM), F32),
                pltpu.VMEM((ROWS, DIM), F32),
                pltpu.VMEM((PROTOS, DIM), F32),
            ],
            in_specs=[pl.BlockSpec(memory_space=pl.ANY)] * 4,
            out_specs=[pl.BlockSpec(memory_space=pltpu.VMEM)] * 6,
            scratch_shapes=[
                pltpu.VMEM((DEVS, SLAB, DIM), BF16),
                pltpu.VMEM((1, ROWS), jnp.int32),
                pltpu.VMEM((DEVS, 1, LANES), F32),
                pltpu.VMEM((PROTOS, DIM), BF16),
                pltpu.VMEM((2, COLS, SAMPLES), F32),
                pltpu.VMEM((2, LOCAL, SAMPLES), F32),
                pltpu.VMEM((2, COLS, LANES), F32),
                pltpu.VMEM((2, LOCAL, LANES), F32),
                pltpu.VMEM((DENSE, LANES), F32),
                pltpu.VMEM((DENSE, LANES), F32),
                pltpu.VMEM((2, 2, 8, SAMPLES), F32),
                pltpu.VMEM((ITERS + 1, 2, PLANE, DENSE, LANES), F32),
                pltpu.VMEM((2, PLANE, 1, COLS), F32),
                pltpu.VMEM((PLANE, 8, LANES), F32),
                pltpu.VMEM((PLANES, 8, LANES), F32),
                dma((4,)), dma((2,)), dma((DEVS,)), dma((PLANES,)), dma((DEVS,)), dma((PLANES,)),
                dma((4,)), dma((2 * ITERS + 2,)), dma((3,)), dma((2,)), dma((3, UNITS)), dma((5,)),
            ],
            compiler_params=pltpu.CompilerParams(
                collective_id=0, has_side_effects=True, vmem_limit_bytes=48 << 20),
        )(view_one, view_two, valid_mask.reshape(1, ROWS), protos)
        outs = pl.pallas_call(
            store_kernel,
            out_shape=[jax.ShapeDtypeStruct((1, 1) if o.shape == (8, LANES) else o.shape, F32) for o in outs],
            in_specs=[pl.BlockSpec(memory_space=pltpu.VMEM)] * len(STORE),
            out_specs=[pl.BlockSpec(memory_space=pl.ANY)] * len(STORE),
            scratch_shapes=[pltpu.VMEM((1, 1), F32), dma((sum(STORE),))],
            compiler_params=pltpu.CompilerParams(vmem_limit_bytes=4 << 20),
        )(*[pltpu.with_memory_space_constraint(o, pltpu.VMEM) for o in outs])
        q1, q2, loss, dz1, dz2, dc = outs
        return q1, q2, loss.reshape(()), dz1, dz2, dc

    return jax.shard_map(
        local_step,
        mesh=mesh,
        in_specs=(P("data", None), P("data", None), P(None, None), P("data")),
        out_specs=(P("data", None), P("data", None), P(), P("data", None), P("data", None), P(None, None)),
        check_vma=False,
    )
```

```python
import jax
import jax.numpy as jnp
from jax import lax
from jax.experimental import pallas as pl
from jax.experimental.pallas import tpu as pltpu
from jax.sharding import PartitionSpec as P

MESH = pl.DeviceIdType.MESH
F32 = jnp.float32
BF16 = jnp.bfloat16

ROWS = 64
SLAB = 2 * ROWS
DEVS = 32
PLANE = 8
SAMPLES = ROWS * DEVS
MB = 256
PROTOS = 8192
DIM = 256
COLS = PROTOS // PLANE
ITERS = 3
LANES = 128
PLANES = DEVS // PLANE
CHIPS = PLANE // 2
PEERS = range(1, PLANE)
BLK = 2 * LANES
DENSE = SAMPLES // LANES
INV_T = 10.0
UNIT = 64
UNITS = COLS // UNIT
BLOCKS = COLS // LANES
FIRST = 12
SECOND = 12
DIAG = 4
LOCAL = COLS - 2 * DIAG * UNIT
KDEPTH = 1024
RCOLS = 1024
QCOLS = 512
GRP = 32
LOG2E = 1.4426950408889634
ROW_CUTS = (1, 3, 5, 7, 8)
DIAG_CUTS = (0, 4, 5, 8)
NT = (((1,), (1,)), ((), ()))


def kernel(v1_hbm, v2_hbm, mk_hbm, c_hbm,
           q1_ref, q2_ref, loss_ref, dz1_ref, dz2_ref, dc_ref,
           zc, mi, mbuf, call, a_ref, ad_ref, vbc, vd, mden, uden, ub, rbuf, vall, lbuf, lzbuf,
           lsem, z_send, z_recv, zcore_recv, m_send, m_recv, ar_send, ar_recv, v_recv, l_recv, d_recv, d_send):
    me = lax.axis_index("data")
    z = me // PLANE
    j = me % PLANE
    c = j % 2
    x = (j // 2) % 2
    y = j // 4
    jx = j + 2 - 4 * x
    jy = j + 4 - 8 * y
    jd = (6 - 2 * (j // 2)) + c
    jf = jx + c * (jy - jx)
    js = jy + c * (jx - jy)
    core = me + 1 - 2 * c
    own_slot = z * PLANE + c * CHIPS + j // 2
    first = z * PLANE + jf
    second = z * PLANE + js
    par = z % 2
    planes = (z, z + 1 - 2 * par, z + 2 - PLANES * (z // 2), PLANES - 1 - z)
    zpart = planes[1] * PLANE + j
    peers = [z * PLANE + (j + t) % PLANE for t in PEERS]
    zpeers = [p * PLANE + j for p in planes[1:]]

    barrier = pltpu.get_barrier_semaphore()
    for dev in peers + zpeers:
        pl.semaphore_signal(barrier, inc=1, device_id=(dev,), device_id_type=MESH)

    own = [
        pltpu.make_async_copy(v1_hbm, zc.at[own_slot, pl.ds(0, ROWS), :], lsem.at[0]),
        pltpu.make_async_copy(v2_hbm, zc.at[own_slot, pl.ds(ROWS, ROWS), :], lsem.at[1]),
        pltpu.make_async_copy(mk_hbm, mi, lsem.at[2]),
    ]
    for cp in own:
        cp.start()
    c_copy = pltpu.make_async_copy(c_hbm, call, lsem.at[3])
    c_copy.start()
    for cp in own:
        cp.wait()
    mrow = mi[...].astype(F32)
    mbuf[own_slot] = jnp.concatenate([mrow, mrow], axis=1)
    pl.semaphore_wait(barrier, len(peers + zpeers))

    def remote(src, dst, ssem, rsem, dev):
        return pltpu.make_async_remote_copy(src_ref=src, dst_ref=dst, send_sem=ssem, recv_sem=rsem,
                                            device_id=(dev,), device_id_type=MESH)

    def wait_in(buf, rsem):
        remote(buf, buf, lsem.at[0], rsem, me).wait_recv()

    def wait_out(buf, ssem):
        remote(buf, buf, ssem, lsem.at[0], me).wait_send()

    def to_plane(buf, ssem, rsem):
        for dev in peers:
            remote(buf, buf, ssem, rsem, dev).start()

    others = pl.ds(0, PLANE - 1)

    def z_slot(p, q):
        return zc.at[p * PLANE + c * CHIPS + q]

    def z_copy(p, q, dev):
        remote(z_slot(p, q), z_slot(p, q), z_send.at[0], z_recv.at[p * CHIPS + q], dev).start()

    def z_core(p, q):
        remote(z_slot(p, q), z_slot(p, q), z_send.at[0], zcore_recv.at[p], core).start()

    def row_scores(lo, hi):
        def body(i, carry):
            k0 = pl.multiple_of(i * RCOLS, RCOLS)
            rs = lax.dot_general(zc[own_slot], call[pl.ds(k0, RCOLS), :], NT, preferred_element_type=F32)
            q1_ref[:, pl.ds(k0, RCOLS)] = rs[:ROWS]
            q2_ref[:, pl.ds(k0, RCOLS)] = rs[ROWS:]
            return carry

        lax.fori_loop(lo, hi, body, 0)

    chip = j // 2
    for dev in (first, second, *zpeers):
        z_copy(z, chip, dev)
    z_core(z, chip)
    to_plane(mbuf.at[own_slot], m_send.at[0], m_recv.at[0])
    c_copy.wait()
    row_scores(0, ROW_CUTS[0])

    def take(t, k, *devs):
        p, q = planes[t], k // 2
        wait_in(z_slot(p, q), z_recv.at[p * CHIPS + q])
        for dev in devs:
            z_copy(p, q, dev)
        z_core(p, q)

    def take_z(t):
        take(t, j, *((first,) if t == 1 else (first, second)))

    def take_f(t):
        take(t, jf, *((second,) if t != 1 else ()))

    def take_s(t):
        take(t, js, *((zpart,) if t == 0 else ()))

    def take_d(t):
        take(t, jd, *((zpart,) if t == 0 else ()))

    def take_core(t):
        part = pl.ds(planes[t] * PLANE + (1 - c) * CHIPS, CHIPS)
        wait_in(zc.at[part], zcore_recv.at[planes[t]])

    def scores(t, k):
        d0 = planes[t] * PLANE + k * CHIPS
        n0 = pl.multiple_of(d0 * ROWS, BLK)

        for v in range(2):
            zb = zc[pl.ds(d0, CHIPS), v * ROWS:(v + 1) * ROWS, :].reshape(BLK, DIM)
            acc = jnp.zeros((8, BLK), F32)
            for k0 in range(0, COLS, MB):
                cs = call[pl.ds(pl.multiple_of(j * COLS + k0, MB), MB), :]
                e = jnp.exp2(lax.dot_general(cs, zb, NT, preferred_element_type=F32) * (INV_T * LOG2E))
                a_ref[v, k0:k0 + MB, pl.ds(n0, BLK)] = e * e
                acc = acc + jnp.sum(e.reshape(MB // 8, 8, BLK), axis=0)
            tot = jnp.sum(acc, axis=0, keepdims=True)
            for b in range(2):
                rbuf[0, v, j, pl.ds(d0 // 2 + b, 1), :] = tot[:, b * LANES:(b + 1) * LANES]

    def own_scores(t):
        scores(t, c)

    def other_scores(t):
        take_core(t)
        scores(t, 1 - c)

    take_f(0)
    take_s(0)
    take_z(1)
    row_scores(ROW_CUTS[0], ROW_CUTS[1])
    take_z(2)
    take_d(0)
    take_z(3)
    take_f(1)
    take_s(1)
    wait_in(mbuf.at[others], m_recv.at[0])
    block = mbuf.at[pl.ds(z * PLANE, PLANE)]
    for dev in zpeers:
        remote(block, block, m_send.at[1], m_recv.at[1], dev).start()
    own_scores(0)
    take_f(2)
    take_s(2)
    take_d(1)
    own_scores(1)
    other_scores(0)
    take_f(3)
    take_s(3)
    take_d(2)
    own_scores(2)
    other_scores(1)
    take_d(3)
    own_scores(3)
    other_scores(2)
    other_scores(3)

    def ar_start(ph, v):
        to_plane(rbuf.at[ph, v, j], ar_send.at[0], ar_recv.at[2 * ph + v])

    def ar_wait(ph, v):
        wait_in(rbuf.at[ph, v, others], ar_recv.at[2 * ph + v])
        tot = rbuf[ph, v, 0]
        for o in PEERS:
            tot = tot + rbuf[ph, v, o]
        return tot

    ar_start(0, 0)
    ar_start(0, 1)

    far = pl.ds(0, DEVS - PLANE)
    wait_in(mbuf.at[far], m_recv.at[1])
    lane = lax.broadcasted_iota(jnp.int32, (1, LANES), 1)
    for b in range(DENSE):
        mden[pl.ds(b, 1), :] = jnp.where(lane < ROWS, mbuf[2 * b], mbuf[2 * b + 1])
    mask = mden[...]
    valid = jnp.sum(jnp.sum(mask, axis=0, keepdims=True), axis=1, keepdims=True)

    def spread(dense, slot, v):
        uden[...] = dense
        for b in range(DENSE):
            ub[slot, v, :, b * LANES:(b + 1) * LANES] = jnp.broadcast_to(uden[pl.ds(b, 1), :], (8, LANES))

    spread(mask, 0, 0)
    spread(mask, 0, 1)

    def sweep(ph, v):
        u = ub[0, v]

        def body(i, acc):
            rows = [pl.multiple_of((i * GRP + g) * 8, 8) for g in range(GRP)]
            for row in rows:
                col = jnp.sum(a_ref[v, pl.ds(row, 8), :] * u, axis=1, keepdims=True)
                vbc[v, pl.ds(row, 8), :] = jnp.broadcast_to(1.0 / (PROTOS * col), (8, LANES))
            for row in rows:
                vg = jnp.concatenate([vbc[v, pl.ds(row, 8), :]] * DENSE, axis=1)
                acc = acc + a_ref[v, pl.ds(row, 8), :] * vg
            return acc

        acc = lax.fori_loop(0, COLS // (8 * GRP), body, jnp.zeros((8, SAMPLES), F32))
        tot = jnp.sum(acc, axis=0, keepdims=True)
        for b in range(DENSE):
            rbuf[ph, v, j, pl.ds(b, 1), :] = tot[:, b * LANES:(b + 1) * LANES]

    def send_v(v):
        diag = (lax.broadcasted_iota(jnp.int32, (LANES, LANES), 0) == lax.broadcasted_iota(jnp.int32, (LANES, LANES), 1))
        for b in range(BLOCKS):
            blk = vbc[v, b * LANES:(b + 1) * LANES, :]
            vall[v, j, :, b * LANES:(b + 1) * LANES] = jnp.sum(jnp.where(diag, blk, 0.0), axis=0, keepdims=True)
        to_plane(vall.at[v, j], ar_send.at[1], v_recv.at[v])

    def diag_scores(lo, hi):
        def body(i, carry):
            n0 = pl.multiple_of(i * BLK, BLK)
            for v in range(2):
                zb = zc[pl.ds(i * CHIPS, CHIPS), v * ROWS:(v + 1) * ROWS, :].reshape(BLK, DIM)
                for k0 in range(0, LOCAL, MB):
                    cs = call[pl.ds(pl.multiple_of(jd * COLS + DIAG * UNIT + k0, MB), MB), :]
                    e = jnp.exp2(lax.dot_general(cs, zb, NT, preferred_element_type=F32) * (INV_T * LOG2E))
                    ad_ref[v, k0:k0 + MB, pl.ds(n0, BLK)] = e * e
            return carry

        lax.fori_loop(lo, hi, body, 0)

    for it in range(ITERS):
        for v in range(2):
            if it > 0:
                spread(mask / (valid * ar_wait(it, v)), 0, v)
            sweep(it + 1, v)
            ar_start(it + 1, v)
            if it == ITERS - 1:
                send_v(v)
        row_scores(ROW_CUTS[it + 1], ROW_CUTS[it + 2])
        diag_scores(DIAG_CUTS[it], DIAG_CUTS[it + 1])

    gam = mask / (valid * 0.2)
    soft = [ar_wait(0, v) for v in range(2)]
    for v in range(2):
        spread(gam / soft[v], 1, v)

    def unit_of(w):
        return w + par * (UNITS - 1 - 2 * w)

    def unit_ref(q, u):
        return dc_ref.at[pl.ds(pl.multiple_of(q * COLS + u * UNIT, UNIT), UNIT), :]

    def d_copy(q, u, ssem, rsem, dev):
        return remote(unit_ref(q, u), unit_ref(q, u), ssem, rsem, dev)

    def d_core(q, u):
        return d_copy(q, u, d_send.at[0], v_recv.at[2], core)

    def d_wait(q, s, u):
        wait_in(unit_ref(q, u), d_recv.at[s, u])

    def grad_part(a_buf, v_buf, k0, size, v, acc):
        k0 = pl.multiple_of(k0, size)
        o = 1 - v

        wide = KDEPTH // BLK
        devs = KDEPTH // ROWS

        def body(i, acc):
            n0 = pl.multiple_of(i * KDEPTH, KDEPTH)
            a = a_buf[v, pl.ds(k0, size), pl.ds(n0, KDEPTH)].reshape(size // 8, 8, KDEPTH)
            ao = a_buf[o, pl.ds(k0, size), pl.ds(n0, KDEPTH)].reshape(size // 8, 8, KDEPTH)
            vo = jnp.concatenate([v_buf[o, pl.ds(k0, size), :]] * (2 * wide), axis=1).reshape(size // 8, 8, KDEPTH)
            g = (a * lax.rsqrt(a)) * ub[1, v, :, pl.ds(n0, KDEPTH)][None] - (ao * vo) * ub[0, o, :, pl.ds(n0, KDEPTH)][None]
            zb = zc[pl.ds(i * devs, devs), v * ROWS:(v + 1) * ROWS, :].reshape(KDEPTH, DIM)
            return acc + jnp.dot(g.reshape(size, KDEPTH).astype(BF16), zb, preferred_element_type=F32)

        return lax.fori_loop(0, SAMPLES // KDEPTH, body, acc)

    def grad_first(k0, size):
        return grad_part(a_ref, vbc, k0, size, 1, jnp.zeros((size, DIM), F32))

    def grad_rest(k0, size, acc):
        acc = grad_part(a_ref, vbc, k0, size, 0, acc)
        dc_ref[pl.ds(pl.multiple_of(j * COLS + k0, size), size), :] = acc

    def diag_units(k0, size):
        acc = jnp.zeros((size, DIM), F32)
        for v in (1, 0):
            acc = grad_part(ad_ref, vd, k0, size, v, acc)
        dc_ref[pl.ds(pl.multiple_of(jd * COLS + DIAG * UNIT + k0, LANES), size), :] = acc
        for u in range(DIAG + k0 // UNIT, DIAG + (k0 + size) // UNIT):
            d_core(jd, u).start()

    def send_own(w):
        u = unit_of(w)
        if w < FIRST:
            d_copy(j, u, d_send.at[1], d_recv.at[0, u], first).start()
        d_core(j, u).start()

    def send_second(w):
        u = unit_of(w)
        d_copy(j, u, d_send.at[2], d_recv.at[1, u], second).start()

    def take_unit(q, s, w, direct):
        u = unit_of(w)
        d_wait(q, s, u)
        if s == 0 and w < DIAG:
            d_copy(q, u, d_send.at[3], d_recv.at[2, u], second).start()
        if w < UNITS - direct:
            d_copy(q, u, d_send.at[4], d_recv.at[s, u], zpart).start()
        d_core(q, u).start()

    def take_first(w):
        take_unit(jf, 0, w, FIRST)
        for own in (range(w + 1, w + 2) if w <= DIAG else range(2 * w - DIAG, 2 * w - DIAG + 2)):
            if own < SECOND:
                send_second(own)

    def take_second(w):
        take_unit(js, 1, w, SECOND)

    def take_far(s, w):
        u = unit_of(w)
        d_wait((jf, js, jd)[s], s, u)
        d_core((jf, js, jd)[s], u).start()

    def take_diag(w):
        take_unit(jd, 2, w, UNITS - DIAG)

    def own_units(w, units):
        size = units * UNIT
        k0 = (w + par * (UNITS - units - 2 * w)) * UNIT
        grad_rest(k0, size, grad_first(k0, size))
        for i in range(units):
            send_own(w + i)

    mu = [mask / ar_wait(ITERS, 0)]
    spread(mu[0] * gam, 0, 0)
    parts = [grad_first(unit_of(w) * UNIT, UNIT) for w in range(2)]
    mu.append(mask / ar_wait(ITERS, 1))
    spread(mu[1] * gam, 0, 1)
    for w in range(2):
        grad_rest(unit_of(w) * UNIT, UNIT, parts[w])
        send_own(w)
        if w == 0:
            send_second(w)
    own_units(2, 2)
    own_units(4, 2)
    take_first(0)
    take_second(0)

    sub = lax.broadcasted_iota(jnp.int32, (ROWS, LANES), 0)
    pick = lax.broadcasted_iota(jnp.int32, (ROWS, LANES), 1) == sub + ROWS * (own_slot % 2)

    def own_rows(dense):
        uden[...] = dense
        row = jnp.broadcast_to(uden[pl.ds(own_slot // 2, 1), :], (ROWS, LANES))
        return jnp.sum(jnp.where(pick, row, 0.0), axis=1, keepdims=True)

    gm = own_rows(gam)
    mus = [own_rows(mu[v]) for v in range(2)]
    ps = [own_rows(soft[v]) for v in range(2)]
    ips = [1.0 / p for p in ps]
    lps = [jnp.log(p) for p in ps]
    for v in range(2):
        wait_in(vall.at[v, others], v_recv.at[v])
    eye = lax.broadcasted_iota(jnp.int32, (LANES, LANES), 0) == lax.broadcasted_iota(jnp.int32, (LANES, LANES), 1)
    for v in range(2):
        for k0 in range(0, LOCAL, LANES):
            row = jnp.broadcast_to(vall[v, jd, :, DIAG * UNIT + k0:DIAG * UNIT + k0 + LANES], (LANES, LANES))
            col = jnp.sum(jnp.where(eye, row, 0.0), axis=1, keepdims=True)
            vd[v, k0:k0 + LANES, :] = jnp.broadcast_to(col, (LANES, LANES))
    q_refs = (q1_ref, q2_ref)
    chunks = COLS // QCOLS

    def row_body(i, carry):
        dz, lacc = carry
        k0 = pl.multiple_of(i * QCOLS, QCOLS)
        l0 = pl.multiple_of((i % chunks) * QCOLS, QCOLS)
        ss, es, qs, gs = [], [], [], []
        for v in range(2):
            ss.append(q_refs[v][:, pl.ds(k0, QCOLS)] * INV_T)
            es.append(jnp.exp2(ss[v] * LOG2E))
            qs.append((es[v] * es[v]) * mus[v] * vall[v, i // chunks, :, pl.ds(l0, QCOLS)])
            q_refs[v][:, pl.ds(k0, QCOLS)] = qs[v]
        for v in range(2):
            lsum = qs[1 - v] * (ss[v] - lps[v])
            lacc = lacc + jnp.sum(lsum.reshape(ROWS // 8, 8, QCOLS), axis=0)
            gs.append((es[v] * ips[v] - qs[1 - v]) * gm)
        g = jnp.concatenate(gs, axis=0).astype(BF16)
        return dz + jnp.dot(g, call[pl.ds(k0, QCOLS), :], preferred_element_type=F32), lacc

    carry = (jnp.zeros((SLAB, DIM), F32), jnp.zeros((8, QCOLS), F32))
    cuts = (0, 4, 7, 10, 13, PROTOS // QCOLS)

    def row_part(i, carry):
        return lax.fori_loop(cuts[i], cuts[i + 1], row_body, carry)

    carry = row_part(0, carry)
    carry = row_part(1, carry)
    take_first(1)
    take_diag(0)
    own_units(6, 2)
    take_first(2)
    take_second(1)
    carry = row_part(2, carry)
    take_first(3)
    take_diag(1)
    carry = row_part(3, carry)
    take_first(4)
    take_second(2)
    dz, lacc = row_part(4, carry)
    dz1_ref[...] = dz[:ROWS]
    dz2_ref[...] = dz[ROWS:]
    lpart = jnp.sum(jnp.sum(lacc, axis=0, keepdims=True), axis=1, keepdims=True)
    lbuf[j] = jnp.broadcast_to(lpart, (8, LANES))
    to_plane(lbuf.at[j], ar_send.at[2], l_recv.at[0])
    own_units(8, 2)
    take_first(5)
    take_diag(2)
    take_first(6)
    take_second(3)
    own_units(10, 2)
    take_first(7)
    take_diag(3)
    for w in (15, 14):
        take_far(0, w)
        take_far(1, w)
    diag_units(0, LOCAL // 2)
    take_first(8)
    take_second(4)
    own_units(12, 4)
    take_first(9)
    take_second(5)
    take_far(0, 13)
    take_far(2, 15)

    wait_in(lbuf.at[others], l_recv.at[0])
    lsum = lbuf[0]
    for o in PEERS:
        lsum = lsum + lbuf[o]
    lzbuf[z] = lsum
    for dev in zpeers:
        remote(lzbuf.at[z], lzbuf.at[z], ar_send.at[3], l_recv.at[1], dev).start()

    diag_units(LOCAL // 2, LOCAL // 2)
    take_first(10)
    take_second(6)

    take_first(11)
    take_second(7)
    take_far(1, 13)
    take_far(2, 14)
    take_far(0, 12)
    for w in (8, 9, 10, 11):
        take_second(w)
    take_far(2, 13)
    take_far(1, 12)
    take_far(2, 12)

    other_planes = pl.ds(0, PLANES - 1)
    wait_in(lzbuf.at[other_planes], l_recv.at[1])
    loss = lzbuf[0]
    for o in range(1, PLANES):
        loss = loss + lzbuf[o]
    loss_ref[...] = -loss / (2.0 * valid)

    wait_in(dc_ref.at[pl.ds(0, PROTOS // 2), :], v_recv.at[2])
    sent = pl.ds(0, DEVS - 1)
    wait_out(zc.at[sent], z_send.at[0])
    wait_out(mbuf.at[others], m_send.at[0])
    wait_out(mbuf.at[far], m_send.at[1])
    wait_out(rbuf.at[:, :, others], ar_send.at[0])
    wait_out(vall.at[:, others], ar_send.at[1])
    wait_out(lbuf.at[others], ar_send.at[2])
    wait_out(lzbuf.at[other_planes], ar_send.at[3])
    counts = (4 * UNITS, FIRST, SECOND, DIAG, 2 * UNITS - FIRST - SECOND + DIAG)
    for k, units in enumerate(counts):
        wait_out(dc_ref.at[pl.ds(0, units * UNIT), :], d_send.at[k])


STORE = (1, 1, 1, 1, 1, 2)


def store_kernel(*refs):
    results = len(STORE)
    one, sem = refs[2 * results:]
    copies = []
    for i, pieces in enumerate(STORE):
        src, dst = refs[i], refs[results + i]
        if dst.shape == one.shape:
            one[...] = src[:1, :1]
            src = one
        rows = src.shape[0] // pieces
        for p in range(pieces):
            part = pl.ds(p * rows, rows)
            copies.append(pltpu.make_async_copy(src.at[part, :], dst.at[part, :], sem.at[len(copies)]))
            copies[-1].start()
    for cp in copies:
        cp.wait()


def solution(mesh):
    def local_step(view_one, view_two, protos, valid_mask):
        dma = pltpu.SemaphoreType.DMA
        outs = pl.pallas_call(
            kernel,
            out_shape=[
                pltpu.VMEM((ROWS, PROTOS), F32),
                pltpu.VMEM((ROWS, PROTOS), F32),
                pltpu.VMEM((8, LANES), F32),
                pltpu.VMEM((ROWS, DIM), F32),
                pltpu.VMEM((ROWS, DIM), F32),
                pltpu.VMEM((PROTOS, DIM), F32),
            ],
            in_specs=[pl.BlockSpec(memory_space=pl.ANY)] * 4,
            out_specs=[pl.BlockSpec(memory_space=pltpu.VMEM)] * 6,
            scratch_shapes=[
                pltpu.VMEM((DEVS, SLAB, DIM), BF16),
                pltpu.VMEM((1, ROWS), jnp.int32),
                pltpu.VMEM((DEVS, 1, LANES), F32),
                pltpu.VMEM((PROTOS, DIM), BF16),
                pltpu.VMEM((2, COLS, SAMPLES), F32),
                pltpu.VMEM((2, LOCAL, SAMPLES), F32),
                pltpu.VMEM((2, COLS, LANES), F32),
                pltpu.VMEM((2, LOCAL, LANES), F32),
                pltpu.VMEM((DENSE, LANES), F32),
                pltpu.VMEM((DENSE, LANES), F32),
                pltpu.VMEM((2, 2, 8, SAMPLES), F32),
                pltpu.VMEM((ITERS + 1, 2, PLANE, DENSE, LANES), F32),
                pltpu.VMEM((2, PLANE, 1, COLS), F32),
                pltpu.VMEM((PLANE, 8, LANES), F32),
                pltpu.VMEM((PLANES, 8, LANES), F32),
                dma((4,)), dma((1,)), dma((DEVS // 2,)), dma((PLANES,)), dma((2,)), dma((2,)),
                dma((4,)), dma((2 * ITERS + 2,)), dma((3,)), dma((2,)), dma((3, UNITS)), dma((5,)),
            ],
            compiler_params=pltpu.CompilerParams(
                collective_id=0, has_side_effects=True, vmem_limit_bytes=48 << 20),
        )(view_one, view_two, valid_mask.reshape(1, ROWS), protos)
        outs = pl.pallas_call(
            store_kernel,
            out_shape=[jax.ShapeDtypeStruct((1, 1) if o.shape == (8, LANES) else o.shape, F32) for o in outs],
            in_specs=[pl.BlockSpec(memory_space=pltpu.VMEM)] * len(STORE),
            out_specs=[pl.BlockSpec(memory_space=pl.ANY)] * len(STORE),
            scratch_shapes=[pltpu.VMEM((1, 1), F32), dma((sum(STORE),))],
            compiler_params=pltpu.CompilerParams(vmem_limit_bytes=4 << 20),
        )(*[pltpu.with_memory_space_constraint(o, pltpu.VMEM) for o in outs])
        q1, q2, loss, dz1, dz2, dc = outs
        return q1, q2, loss.reshape(()), dz1, dz2, dc

    return jax.shard_map(
        local_step,
        mesh=mesh,
        in_specs=(P("data", None), P("data", None), P(None, None), P("data")),
        out_specs=(P("data", None), P("data", None), P(), P("data", None), P("data", None), P(None, None)),
        check_vma=False,
    )
```

```python
import jax
import jax.numpy as jnp
from jax import lax
from jax.experimental import pallas as pl
from jax.experimental.pallas import tpu as pltpu
from jax.sharding import PartitionSpec as P

MESH = pl.DeviceIdType.MESH
F32 = jnp.float32
BF16 = jnp.bfloat16

ROWS = 64
SLAB = 2 * ROWS
DEVS = 32
PLANE = 8
SAMPLES = ROWS * DEVS
MB = 256
PROTOS = 8192
DIM = 256
COLS = PROTOS // PLANE
ITERS = 3
LANES = 128
PLANES = DEVS // PLANE
CHIPS = PLANE // 2
PEERS = range(1, PLANE)
BLK = 2 * LANES
DENSE = SAMPLES // LANES
INV_T = 10.0
UNIT = 64
UNITS = COLS // UNIT
BLOCKS = COLS // LANES
FIRST = 12
SECOND = 12
DIAG = 4
LOCAL = COLS - 2 * DIAG * UNIT
KDEPTH = 1024
RCOLS = 1024
QCOLS = 512
GRP = 32
LOG2E = 1.4426950408889634
ROW_CUTS = (1, 3, 5, 8, 8)
DIAG_CUTS = (0, 4, 6, 8)
NT = (((1,), (1,)), ((), ()))


def kernel(v1_hbm, v2_hbm, mk_hbm, c_hbm,
           q1_ref, q2_ref, loss_ref, dz1_ref, dz2_ref, dc_ref,
           zc, mi, mbuf, call, a_ref, ad_ref, vbc, vd, mden, uden, ub, rbuf, vall, lbuf, lzbuf,
           lsem, z_send, z_recv, zcore_recv, m_send, m_recv, ar_send, ar_recv, v_recv, l_recv, d_recv, d_send):
    me = lax.axis_index("data")
    z = me // PLANE
    j = me % PLANE
    c = j % 2
    x = (j // 2) % 2
    y = j // 4
    jx = j + 2 - 4 * x
    jy = j + 4 - 8 * y
    jd = (6 - 2 * (j // 2)) + c
    jf = jx + c * (jy - jx)
    js = jy + c * (jx - jy)
    core = me + 1 - 2 * c
    own_slot = z * PLANE + c * CHIPS + j // 2
    first = z * PLANE + jf
    second = z * PLANE + js
    par = z % 2
    planes = (z, z + 1 - 2 * par, z + 2 - PLANES * (z // 2), PLANES - 1 - z)
    zpart = planes[1] * PLANE + j
    peers = [z * PLANE + (j + t) % PLANE for t in PEERS]
    zpeers = [p * PLANE + j for p in planes[1:]]

    barrier = pltpu.get_barrier_semaphore()
    for dev in peers + zpeers:
        pl.semaphore_signal(barrier, inc=1, device_id=(dev,), device_id_type=MESH)

    own = [
        pltpu.make_async_copy(v1_hbm, zc.at[own_slot, pl.ds(0, ROWS), :], lsem.at[0]),
        pltpu.make_async_copy(v2_hbm, zc.at[own_slot, pl.ds(ROWS, ROWS), :], lsem.at[1]),
        pltpu.make_async_copy(mk_hbm, mi, lsem.at[2]),
    ]
    for cp in own:
        cp.start()
    c_copy = pltpu.make_async_copy(c_hbm, call, lsem.at[3])
    c_copy.start()
    for cp in own:
        cp.wait()
    mrow = mi[...].astype(F32)
    mbuf[own_slot] = jnp.concatenate([mrow, mrow], axis=1)
    pl.semaphore_wait(barrier, len(peers + zpeers))

    def remote(src, dst, ssem, rsem, dev):
        return pltpu.make_async_remote_copy(src_ref=src, dst_ref=dst, send_sem=ssem, recv_sem=rsem,
                                            device_id=(dev,), device_id_type=MESH)

    def wait_in(buf, rsem):
        remote(buf, buf, lsem.at[0], rsem, me).wait_recv()

    def wait_out(buf, ssem):
        remote(buf, buf, ssem, lsem.at[0], me).wait_send()

    def to_plane(buf, ssem, rsem):
        for dev in peers:
            remote(buf, buf, ssem, rsem, dev).start()

    others = pl.ds(0, PLANE - 1)

    def z_slot(p, q):
        return zc.at[p * PLANE + c * CHIPS + q]

    def z_copy(p, q, dev):
        remote(z_slot(p, q), z_slot(p, q), z_send.at[0], z_recv.at[p * CHIPS + q], dev).start()

    def z_core(p, q):
        remote(z_slot(p, q), z_slot(p, q), z_send.at[0], zcore_recv.at[p], core).start()

    def row_scores(lo, hi):
        def body(i, carry):
            k0 = pl.multiple_of(i * RCOLS, RCOLS)
            rs = lax.dot_general(zc[own_slot], call[pl.ds(k0, RCOLS), :], NT, preferred_element_type=F32)
            q1_ref[:, pl.ds(k0, RCOLS)] = rs[:ROWS]
            q2_ref[:, pl.ds(k0, RCOLS)] = rs[ROWS:]
            return carry

        lax.fori_loop(lo, hi, body, 0)

    chip = j // 2
    for dev in (first, second, *zpeers):
        z_copy(z, chip, dev)
    z_core(z, chip)
    to_plane(mbuf.at[own_slot], m_send.at[0], m_recv.at[0])
    c_copy.wait()
    row_scores(0, ROW_CUTS[0])

    def take(t, k, *devs):
        p, q = planes[t], k // 2
        wait_in(z_slot(p, q), z_recv.at[p * CHIPS + q])
        for dev in devs:
            z_copy(p, q, dev)
        z_core(p, q)

    def take_z(t):
        take(t, j, *((first,) if t == 1 else (first, second)))

    def take_f(t):
        take(t, jf, *((second,) if t != 1 else ()))

    def take_s(t):
        take(t, js, *((zpart,) if t == 0 else ()))

    def take_d(t):
        take(t, jd, *((zpart,) if t == 0 else ()))

    def take_core(t):
        part = pl.ds(planes[t] * PLANE + (1 - c) * CHIPS, CHIPS)
        wait_in(zc.at[part], zcore_recv.at[planes[t]])

    def scores(t, k):
        d0 = planes[t] * PLANE + k * CHIPS
        n0 = pl.multiple_of(d0 * ROWS, BLK)

        for v in range(2):
            zb = zc[pl.ds(d0, CHIPS), v * ROWS:(v + 1) * ROWS, :].reshape(BLK, DIM)
            acc = jnp.zeros((8, BLK), F32)
            for k0 in range(0, COLS, MB):
                cs = call[pl.ds(pl.multiple_of(j * COLS + k0, MB), MB), :]
                e = jnp.exp2(lax.dot_general(cs, zb, NT, preferred_element_type=F32) * (INV_T * LOG2E))
                a_ref[v, k0:k0 + MB, pl.ds(n0, BLK)] = e * e
                acc = acc + jnp.sum(e.reshape(MB // 8, 8, BLK), axis=0)
            tot = jnp.sum(acc, axis=0, keepdims=True)
            for b in range(2):
                rbuf[0, v, j, pl.ds(d0 // 2 + b, 1), :] = tot[:, b * LANES:(b + 1) * LANES]

    def own_scores(t):
        scores(t, c)

    def other_scores(t):
        take_core(t)
        scores(t, 1 - c)

    take_f(0)
    take_s(0)
    take_z(1)
    row_scores(ROW_CUTS[0], ROW_CUTS[1])
    take_z(2)
    take_d(0)
    take_z(3)
    take_f(1)
    take_s(1)
    wait_in(mbuf.at[others], m_recv.at[0])
    block = mbuf.at[pl.ds(z * PLANE, PLANE)]
    for dev in zpeers:
        remote(block, block, m_send.at[1], m_recv.at[1], dev).start()
    own_scores(0)
    take_f(2)
    take_s(2)
    take_d(1)
    own_scores(1)
    other_scores(0)
    take_f(3)
    take_s(3)
    take_d(2)
    own_scores(2)
    other_scores(1)
    take_d(3)
    own_scores(3)
    other_scores(2)
    other_scores(3)

    def ar_start(ph, v):
        to_plane(rbuf.at[ph, v, j], ar_send.at[0], ar_recv.at[2 * ph + v])

    def ar_wait(ph, v):
        wait_in(rbuf.at[ph, v, others], ar_recv.at[2 * ph + v])
        tot = rbuf[ph, v, 0]
        for o in PEERS:
            tot = tot + rbuf[ph, v, o]
        return tot

    ar_start(0, 0)
    ar_start(0, 1)

    far = pl.ds(0, DEVS - PLANE)
    wait_in(mbuf.at[far], m_recv.at[1])
    lane = lax.broadcasted_iota(jnp.int32, (1, LANES), 1)
    for b in range(DENSE):
        mden[pl.ds(b, 1), :] = jnp.where(lane < ROWS, mbuf[2 * b], mbuf[2 * b + 1])
    mask = mden[...]
    valid = jnp.sum(jnp.sum(mask, axis=0, keepdims=True), axis=1, keepdims=True)

    def spread(dense, slot, v):
        uden[...] = dense
        for b in range(DENSE):
            ub[slot, v, :, b * LANES:(b + 1) * LANES] = jnp.broadcast_to(uden[pl.ds(b, 1), :], (8, LANES))

    spread(mask, 0, 0)
    spread(mask, 0, 1)

    def sweep(ph, v):
        u = ub[0, v]

        def body(i, acc):
            rows = [pl.multiple_of((i * GRP + g) * 8, 8) for g in range(GRP)]
            for row in rows:
                col = jnp.sum(a_ref[v, pl.ds(row, 8), :] * u, axis=1, keepdims=True)
                vbc[v, pl.ds(row, 8), :] = jnp.broadcast_to(1.0 / (PROTOS * col), (8, LANES))
            for row in rows:
                vg = jnp.concatenate([vbc[v, pl.ds(row, 8), :]] * DENSE, axis=1)
                acc = acc + a_ref[v, pl.ds(row, 8), :] * vg
            return acc

        acc = lax.fori_loop(0, COLS // (8 * GRP), body, jnp.zeros((8, SAMPLES), F32))
        tot = jnp.sum(acc, axis=0, keepdims=True)
        for b in range(DENSE):
            rbuf[ph, v, j, pl.ds(b, 1), :] = tot[:, b * LANES:(b + 1) * LANES]

    def send_v(v):
        diag = (lax.broadcasted_iota(jnp.int32, (LANES, LANES), 0) == lax.broadcasted_iota(jnp.int32, (LANES, LANES), 1))
        for b in range(BLOCKS):
            blk = vbc[v, b * LANES:(b + 1) * LANES, :]
            vall[v, j, :, b * LANES:(b + 1) * LANES] = jnp.sum(jnp.where(diag, blk, 0.0), axis=0, keepdims=True)
        to_plane(vall.at[v, j], ar_send.at[1], v_recv.at[v])

    def diag_scores(lo, hi):
        def body(i, carry):
            n0 = pl.multiple_of(i * BLK, BLK)
            for v in range(2):
                zb = zc[pl.ds(i * CHIPS, CHIPS), v * ROWS:(v + 1) * ROWS, :].reshape(BLK, DIM)
                for k0 in range(0, LOCAL, MB):
                    cs = call[pl.ds(pl.multiple_of(jd * COLS + DIAG * UNIT + k0, MB), MB), :]
                    e = jnp.exp2(lax.dot_general(cs, zb, NT, preferred_element_type=F32) * (INV_T * LOG2E))
                    ad_ref[v, k0:k0 + MB, pl.ds(n0, BLK)] = e * e
            return carry

        lax.fori_loop(lo, hi, body, 0)

    for it in range(ITERS):
        for v in range(2):
            if it > 0:
                spread(mask / (valid * ar_wait(it, v)), 0, v)
            sweep(it + 1, v)
            ar_start(it + 1, v)
            if it == ITERS - 1:
                send_v(v)
        row_scores(ROW_CUTS[it + 1], ROW_CUTS[it + 2])
        diag_scores(DIAG_CUTS[it], DIAG_CUTS[it + 1])

    gam = mask / (valid * 0.2)
    soft = [ar_wait(0, v) for v in range(2)]
    for v in range(2):
        spread(gam / soft[v], 1, v)

    def unit_of(w):
        return w + par * (UNITS - 1 - 2 * w)

    def unit_ref(q, u):
        return dc_ref.at[pl.ds(pl.multiple_of(q * COLS + u * UNIT, UNIT), UNIT), :]

    def d_copy(q, u, ssem, rsem, dev):
        return remote(unit_ref(q, u), unit_ref(q, u), ssem, rsem, dev)

    def d_core(q, u):
        return d_copy(q, u, d_send.at[0], v_recv.at[2], core)

    def d_wait(q, s, u):
        wait_in(unit_ref(q, u), d_recv.at[s, u])

    def grad_part(a_buf, v_buf, k0, size, v, acc):
        k0 = pl.multiple_of(k0, size)
        o = 1 - v

        wide = KDEPTH // BLK
        devs = KDEPTH // ROWS

        def body(i, acc):
            n0 = pl.multiple_of(i * KDEPTH, KDEPTH)
            a = a_buf[v, pl.ds(k0, size), pl.ds(n0, KDEPTH)].reshape(size // 8, 8, KDEPTH)
            ao = a_buf[o, pl.ds(k0, size), pl.ds(n0, KDEPTH)].reshape(size // 8, 8, KDEPTH)
            vo = jnp.concatenate([v_buf[o, pl.ds(k0, size), :]] * (2 * wide), axis=1).reshape(size // 8, 8, KDEPTH)
            g = (a * lax.rsqrt(a)) * ub[1, v, :, pl.ds(n0, KDEPTH)][None] - (ao * vo) * ub[0, o, :, pl.ds(n0, KDEPTH)][None]
            zb = zc[pl.ds(i * devs, devs), v * ROWS:(v + 1) * ROWS, :].reshape(KDEPTH, DIM)
            return acc + jnp.dot(g.reshape(size, KDEPTH).astype(BF16), zb, preferred_element_type=F32)

        return lax.fori_loop(0, SAMPLES // KDEPTH, body, acc)

    def grad_first(k0, size):
        return grad_part(a_ref, vbc, k0, size, 1, jnp.zeros((size, DIM), F32))

    def grad_rest(k0, size, acc):
        acc = grad_part(a_ref, vbc, k0, size, 0, acc)
        dc_ref[pl.ds(pl.multiple_of(j * COLS + k0, size), size), :] = acc

    def diag_units(k0, size):
        acc = jnp.zeros((size, DIM), F32)
        for v in (1, 0):
            acc = grad_part(ad_ref, vd, k0, size, v, acc)
        dc_ref[pl.ds(pl.multiple_of(jd * COLS + DIAG * UNIT + k0, LANES), size), :] = acc
        for u in range(DIAG + k0 // UNIT, DIAG + (k0 + size) // UNIT):
            d_core(jd, u).start()

    def send_own(w):
        u = unit_of(w)
        if w < FIRST:
            d_copy(j, u, d_send.at[1], d_recv.at[0, u], first).start()
        d_core(j, u).start()

    def send_second(w):
        u = unit_of(w)
        d_copy(j, u, d_send.at[2], d_recv.at[1, u], second).start()

    def take_unit(q, s, w, direct):
        u = unit_of(w)
        d_wait(q, s, u)
        if s == 0 and w < DIAG:
            d_copy(q, u, d_send.at[3], d_recv.at[2, u], second).start()
        if w < UNITS - direct:
            d_copy(q, u, d_send.at[4], d_recv.at[s, u], zpart).start()
        d_core(q, u).start()

    def take_first(w):
        take_unit(jf, 0, w, FIRST)
        for own in (range(w + 1, w + 2) if w <= DIAG else range(2 * w - DIAG, 2 * w - DIAG + 2)):
            if own < SECOND:
                send_second(own)

    def take_second(w):
        take_unit(js, 1, w, SECOND)

    def take_far(s, w):
        u = unit_of(w)
        d_wait((jf, js, jd)[s], s, u)
        d_core((jf, js, jd)[s], u).start()

    def take_diag(w):
        take_unit(jd, 2, w, UNITS - DIAG)

    def own_units(w, units):
        size = units * UNIT
        k0 = (w + par * (UNITS - units - 2 * w)) * UNIT
        grad_rest(k0, size, grad_first(k0, size))
        for i in range(units):
            send_own(w + i)

    mu = [mask / ar_wait(ITERS, 0)]
    spread(mu[0] * gam, 0, 0)
    parts = [grad_first(unit_of(w) * UNIT, UNIT) for w in range(2)]
    mu.append(mask / ar_wait(ITERS, 1))
    spread(mu[1] * gam, 0, 1)
    for w in range(2):
        grad_rest(unit_of(w) * UNIT, UNIT, parts[w])
        send_own(w)
        if w == 0:
            send_second(w)
    own_units(2, 2)
    own_units(4, 2)
    take_first(0)
    take_second(0)

    sub = lax.broadcasted_iota(jnp.int32, (ROWS, LANES), 0)
    pick = lax.broadcasted_iota(jnp.int32, (ROWS, LANES), 1) == sub + ROWS * (own_slot % 2)

    def own_rows(dense):
        uden[...] = dense
        row = jnp.broadcast_to(uden[pl.ds(own_slot // 2, 1), :], (ROWS, LANES))
        return jnp.sum(jnp.where(pick, row, 0.0), axis=1, keepdims=True)

    gm = own_rows(gam)
    mus = [own_rows(mu[v]) for v in range(2)]
    ps = [own_rows(soft[v]) for v in range(2)]
    ips = [1.0 / p for p in ps]
    lps = [jnp.log(p) for p in ps]
    for v in range(2):
        wait_in(vall.at[v, others], v_recv.at[v])
    eye = lax.broadcasted_iota(jnp.int32, (LANES, LANES), 0) == lax.broadcasted_iota(jnp.int32, (LANES, LANES), 1)
    for v in range(2):
        for k0 in range(0, LOCAL, LANES):
            row = jnp.broadcast_to(vall[v, jd, :, DIAG * UNIT + k0:DIAG * UNIT + k0 + LANES], (LANES, LANES))
            col = jnp.sum(jnp.where(eye, row, 0.0), axis=1, keepdims=True)
            vd[v, k0:k0 + LANES, :] = jnp.broadcast_to(col, (LANES, LANES))
    q_refs = (q1_ref, q2_ref)
    chunks = COLS // QCOLS

    def row_body(i, carry):
        dz, lacc = carry
        k0 = pl.multiple_of(i * QCOLS, QCOLS)
        l0 = pl.multiple_of((i % chunks) * QCOLS, QCOLS)
        ss, es, qs, gs = [], [], [], []
        for v in range(2):
            ss.append(q_refs[v][:, pl.ds(k0, QCOLS)] * INV_T)
            es.append(jnp.exp2(ss[v] * LOG2E))
            qs.append((es[v] * es[v]) * mus[v] * vall[v, i // chunks, :, pl.ds(l0, QCOLS)])
            q_refs[v][:, pl.ds(k0, QCOLS)] = qs[v]
        for v in range(2):
            lsum = qs[1 - v] * (ss[v] - lps[v])
            lacc = lacc + jnp.sum(lsum.reshape(ROWS // 8, 8, QCOLS), axis=0)
            gs.append((es[v] * ips[v] - qs[1 - v]) * gm)
        g = jnp.concatenate(gs, axis=0).astype(BF16)
        return dz + jnp.dot(g, call[pl.ds(k0, QCOLS), :], preferred_element_type=F32), lacc

    carry = (jnp.zeros((SLAB, DIM), F32), jnp.zeros((8, QCOLS), F32))
    cuts = (0, 4, 7, 10, 13, PROTOS // QCOLS)

    def row_part(i, carry):
        return lax.fori_loop(cuts[i], cuts[i + 1], row_body, carry)

    carry = row_part(0, carry)
    carry = row_part(1, carry)
    take_first(1)
    take_diag(0)
    own_units(6, 2)
    take_first(2)
    take_second(1)
    carry = row_part(2, carry)
    take_first(3)
    take_diag(1)
    carry = row_part(3, carry)
    take_first(4)
    take_second(2)
    dz, lacc = row_part(4, carry)
    dz1_ref[...] = dz[:ROWS]
    dz2_ref[...] = dz[ROWS:]
    lpart = jnp.sum(jnp.sum(lacc, axis=0, keepdims=True), axis=1, keepdims=True)
    lbuf[j] = jnp.broadcast_to(lpart, (8, LANES))
    to_plane(lbuf.at[j], ar_send.at[2], l_recv.at[0])
    own_units(8, 2)
    take_first(5)
    take_diag(2)
    take_first(6)
    take_second(3)
    own_units(10, 2)
    take_first(7)
    take_diag(3)
    for w in (15, 14):
        take_far(0, w)
        take_far(1, w)
    diag_units(0, LOCAL // 2)
    take_first(8)
    take_second(4)
    own_units(12, 4)
    take_first(9)
    take_second(5)
    take_far(0, 13)
    take_far(2, 15)

    wait_in(lbuf.at[others], l_recv.at[0])
    lsum = lbuf[0]
    for o in PEERS:
        lsum = lsum + lbuf[o]
    lzbuf[z] = lsum
    for dev in zpeers:
        remote(lzbuf.at[z], lzbuf.at[z], ar_send.at[3], l_recv.at[1], dev).start()

    diag_units(LOCAL // 2, LOCAL // 2)
    take_first(10)
    take_second(6)

    take_first(11)
    take_second(7)
    take_far(1, 13)
    take_far(2, 14)
    take_far(0, 12)
    for w in (8, 9, 10, 11):
        take_second(w)
    take_far(2, 13)
    take_far(1, 12)
    take_far(2, 12)

    other_planes = pl.ds(0, PLANES - 1)
    wait_in(lzbuf.at[other_planes], l_recv.at[1])
    loss = lzbuf[0]
    for o in range(1, PLANES):
        loss = loss + lzbuf[o]
    loss_ref[...] = -loss / (2.0 * valid)

    wait_in(dc_ref.at[pl.ds(0, PROTOS // 2), :], v_recv.at[2])
    sent = pl.ds(0, DEVS - 1)
    wait_out(zc.at[sent], z_send.at[0])
    wait_out(mbuf.at[others], m_send.at[0])
    wait_out(mbuf.at[far], m_send.at[1])
    wait_out(rbuf.at[:, :, others], ar_send.at[0])
    wait_out(vall.at[:, others], ar_send.at[1])
    wait_out(lbuf.at[others], ar_send.at[2])
    wait_out(lzbuf.at[other_planes], ar_send.at[3])
    counts = (4 * UNITS, FIRST, SECOND, DIAG, 2 * UNITS - FIRST - SECOND + DIAG)
    for k, units in enumerate(counts):
        wait_out(dc_ref.at[pl.ds(0, units * UNIT), :], d_send.at[k])


STORE = (1, 1, 1, 1, 1, 2)


def store_kernel(*refs):
    results = len(STORE)
    one, sem = refs[2 * results:]
    copies = []
    for i, pieces in enumerate(STORE):
        src, dst = refs[i], refs[results + i]
        if dst.shape == one.shape:
            one[...] = src[:1, :1]
            src = one
        rows = src.shape[0] // pieces
        for p in range(pieces):
            part = pl.ds(p * rows, rows)
            copies.append(pltpu.make_async_copy(src.at[part, :], dst.at[part, :], sem.at[len(copies)]))
            copies[-1].start()
    for cp in copies:
        cp.wait()


def solution(mesh):
    def local_step(view_one, view_two, protos, valid_mask):
        dma = pltpu.SemaphoreType.DMA
        outs = pl.pallas_call(
            kernel,
            out_shape=[
                pltpu.VMEM((ROWS, PROTOS), F32),
                pltpu.VMEM((ROWS, PROTOS), F32),
                pltpu.VMEM((8, LANES), F32),
                pltpu.VMEM((ROWS, DIM), F32),
                pltpu.VMEM((ROWS, DIM), F32),
                pltpu.VMEM((PROTOS, DIM), F32),
            ],
            in_specs=[pl.BlockSpec(memory_space=pl.ANY)] * 4,
            out_specs=[pl.BlockSpec(memory_space=pltpu.VMEM)] * 6,
            scratch_shapes=[
                pltpu.VMEM((DEVS, SLAB, DIM), BF16),
                pltpu.VMEM((1, ROWS), jnp.int32),
                pltpu.VMEM((DEVS, 1, LANES), F32),
                pltpu.VMEM((PROTOS, DIM), BF16),
                pltpu.VMEM((2, COLS, SAMPLES), F32),
                pltpu.VMEM((2, LOCAL, SAMPLES), F32),
                pltpu.VMEM((2, COLS, LANES), F32),
                pltpu.VMEM((2, LOCAL, LANES), F32),
                pltpu.VMEM((DENSE, LANES), F32),
                pltpu.VMEM((DENSE, LANES), F32),
                pltpu.VMEM((2, 2, 8, SAMPLES), F32),
                pltpu.VMEM((ITERS + 1, 2, PLANE, DENSE, LANES), F32),
                pltpu.VMEM((2, PLANE, 1, COLS), F32),
                pltpu.VMEM((PLANE, 8, LANES), F32),
                pltpu.VMEM((PLANES, 8, LANES), F32),
                dma((4,)), dma((1,)), dma((DEVS // 2,)), dma((PLANES,)), dma((2,)), dma((2,)),
                dma((4,)), dma((2 * ITERS + 2,)), dma((3,)), dma((2,)), dma((3, UNITS)), dma((5,)),
            ],
            compiler_params=pltpu.CompilerParams(
                collective_id=0, has_side_effects=True, vmem_limit_bytes=48 << 20),
        )(view_one, view_two, valid_mask.reshape(1, ROWS), protos)
        outs = pl.pallas_call(
            store_kernel,
            out_shape=[jax.ShapeDtypeStruct((1, 1) if o.shape == (8, LANES) else o.shape, F32) for o in outs],
            in_specs=[pl.BlockSpec(memory_space=pltpu.VMEM)] * len(STORE),
            out_specs=[pl.BlockSpec(memory_space=pl.ANY)] * len(STORE),
            scratch_shapes=[pltpu.VMEM((1, 1), F32), dma((sum(STORE),))],
            compiler_params=pltpu.CompilerParams(vmem_limit_bytes=4 << 20),
        )(*[pltpu.with_memory_space_constraint(o, pltpu.VMEM) for o in outs])
        q1, q2, loss, dz1, dz2, dc = outs
        return q1, q2, loss.reshape(()), dz1, dz2, dc

    return jax.shard_map(
        local_step,
        mesh=mesh,
        in_specs=(P("data", None), P("data", None), P(None, None), P("data")),
        out_specs=(P("data", None), P("data", None), P(), P("data", None), P("data", None), P(None, None)),
        check_vma=False,
    )
```
